256 devices in a mesh: band: 16 (over y_lo, z), dom: 16 (over x, y_hi, core).
Axes of the slice: x: 4, y: 4 (y_hi: 2, y_lo: 2; y = y_hi * 2 + y_lo), z: 8, core: 2. Of those that a mesh axis runs over, the one named last changes fastest.
Arguments:
- wavefunctions: float32 [1024, 64, 16, 128], P('band', 'dom'), may hold values from -6 to 6
- potential: float32 [64, 16, 128], P('dom'), may hold values from -40 to 40
- projectors: float32 [64, 18, 4, 16, 128], P('dom'), may hold values from -0.0625 to 0.0625
- hamiltonian_correction: float32 [64, 18, 18], P('dom'), may hold values from -0.0390625 to 0.0390625
- delta_s: float32 [64, 18, 18], P('dom'), may hold values from -0.0390625 to 0.0390625
- projector_count: int32 [64], P('dom'), may hold values from 1 to 18
Outputs:
- ham: float32 [1024, 1024], P('band')
- correlation: float32 [1024, 1024], P('band')
The draws below stay inside these ranges and needn't reach their ends.
All inputs are finite; a program needn't handle non-finite values.
Results may differ from the reference program's by a relative error of at most 0.00007.
Values sent between devices are 32-bit elements; how exact they have to be, the bound alone decides.
A program may use at most 192 MiB of HBM per device.

```python
import jax
import jax.numpy as jnp
from jax import lax

BANDS = 1024
NPROJ = 18
A_DEV = 4
CX = 4
NY = 16
NZ = 128
NX = 64
ATOMS = 64
N_DOM = 16


def place_ends(entries, rng, least, largest):
    extent = entries.shape
    index_at = [jax.random.randint(jax.random.fold_in(rng, axis), (), 0, extent[axis]) for axis in range(len(extent))]
    entries = entries.at[tuple(index_at)].set(least)
    longest = extent.index(max(extent))
    index_at[longest] = (index_at[longest] + 1) % extent[longest]
    return entries.at[tuple(index_at)].set(largest)


def block_levels(rng, dims, pieces, least, top_value):
    gain = 1.0
    for axis_at, parts in pieces:
        heights = jax.random.uniform(jax.random.fold_in(jax.random.fold_in(rng, 6), axis_at), (parts,), jnp.float32, least / len(pieces), top_value / len(pieces))
        gain = gain * jnp.repeat(jnp.exp(heights), dims[axis_at] // parts).reshape((-1,) + (1,) * (len(dims) - 1 - axis_at))
    return gain


def centred(stream_key, shape, deviation, reach, cuts=(), kind=jnp.bfloat16):
    result = deviation * jax.random.normal(stream_key, shape, jnp.float32)
    if cuts:
        result = result * block_levels(stream_key, shape, cuts, -0.22, 0.18)
    return jnp.clip(result, -reach, reach).astype(kind)


def setup_inputs(seed: int = 0) -> dict:
    arg_keys = jax.random.split(jax.random.key(seed), 7)
    return {
        "wavefunctions": centred(arg_keys[0], (BANDS, NX, NY, NZ), 1.0, 6.0, ((0, 16), (1, 16)), jnp.float32),
        "potential": jnp.clip(jax.random.uniform(arg_keys[1], (NX, NY, NZ), jnp.float32, -40.0, 40.0) * block_levels(arg_keys[1], (NX, NY, NZ), ((0, 16),), -0.4, 0.0), -40.0, 40.0),
        "projectors": centred(arg_keys[2], (ATOMS, NPROJ, CX, NY, NZ), (CX * NY * NZ) ** -0.5, 0.0625, ((0, 16),), jnp.float32),
        "hamiltonian_correction": centred(arg_keys[3], (ATOMS, NPROJ, NPROJ), (ATOMS * NPROJ * NPROJ) ** -0.5, 0.0390625, ((0, 16),), jnp.float32),
        "delta_s": centred(arg_keys[4], (ATOMS, NPROJ, NPROJ), (ATOMS * NPROJ * NPROJ) ** -0.5, 0.0390625, ((0, 16),), jnp.float32),
        "projector_count": place_ends(jax.random.randint(arg_keys[5], (ATOMS,), 1, NPROJ + 1), jax.random.fold_in(arg_keys[5], 1), 1, NPROJ).astype(jnp.int32),
    }


def rows_product(left, right):
    return lax.dot_general(left, right, (((1,), (1,)), ((), ())), precision=lax.Precision.HIGHEST, preferred_element_type=jnp.float32)


def reference(wavefunctions, potential, projectors, hamiltonian_correction, delta_s, projector_count):
    bands = wavefunctions.shape[0]
    beside = jnp.roll(wavefunctions, 1, 1) + jnp.roll(wavefunctions, -1, 1)
    beside = beside + jnp.roll(wavefunctions, 1, 2) + jnp.roll(wavefunctions, -1, 2)
    beside = beside + jnp.roll(wavefunctions, 1, 3) + jnp.roll(wavefunctions, -1, 3)
    hpsi = 0.5 * (6.0 * wavefunctions - beside) + potential[None] * wavefunctions
    volume = 1.0 / (NX * NY * NZ)
    local_cells = CX * NY * NZ
    split_psi = wavefunctions.reshape(bands, N_DOM, local_cells)
    split_proj = projectors.reshape(N_DOM, A_DEV * NPROJ, local_cells)
    projector_coefficient = jnp.einsum("bdg,dkg->bdk", split_psi, split_proj, precision=lax.Precision.HIGHEST)
    slot_mask = (jnp.arange(NPROJ, dtype=jnp.int32)[None, :] < projector_count[:, None]).astype(jnp.float32)
    projector_coefficient = projector_coefficient.reshape(bands, ATOMS, NPROJ) * slot_mask[None]
    sym_h = 0.5 * (hamiltonian_correction + jnp.swapaxes(hamiltonian_correction, 1, 2))
    sym_s = 0.5 * (delta_s + jnp.swapaxes(delta_s, 1, 2))
    coupled_h = jnp.einsum("bap,apq->baq", projector_coefficient, sym_h, precision=lax.Precision.HIGHEST).reshape(bands, -1)
    coupled_s = jnp.einsum("bap,apq->baq", projector_coefficient, sym_s, precision=lax.Precision.HIGHEST).reshape(bands, -1)
    coef_flat = projector_coefficient.reshape(bands, -1)
    psi_flat = wavefunctions.reshape(bands, -1)
    hpsi_flat = hpsi.reshape(bands, -1)
    ham = volume * rows_product(hpsi_flat, psi_flat) + rows_product(coupled_h, coef_flat)
    correlation = volume * rows_product(psi_flat, psi_flat) + rows_product(coupled_s, coef_flat)
    return ham, correlation
```

```python
import functools

import jax
import jax.numpy as jnp
from jax import lax
from jax.experimental import pallas as pl
from jax.experimental.pallas import tpu as pltpu
from jax.sharding import PartitionSpec as P

MESH = pl.DeviceIdType.MESH
F32 = jnp.float32
BF16 = jnp.bfloat16
NB = 16
ND = 16
CH = 8
RPZ = 32
CHUNK = (CH + 1) * RPZ
VOLUME = 1.0 / 131072.0
OFFSETS = [(0, 1), (0, -1), (1, 1), (1, -1), (0, 2), (0, -2), (1, 2), (1, -2), (1, 0),
           (0, 3), (0, -3), (1, 3), (1, -3), (0, 4), (1, 4)]


def split(x):
    hi = x.astype(BF16)
    return hi, (x - hi.astype(F32)).astype(BF16)


def dot(a, b):
    return lax.dot_general(a, b, (((1,), (0,)), ((), ())), preferred_element_type=F32)


def dot_nt(a, b):
    return lax.dot_general(a, b, (((1,), (1,)), ((), ())), preferred_element_type=F32)


def kernel(psi, pot, proj, ext, out, T, R, RX, CS, CR, VB, AF, AThi, ATlo, Bhi, Blo, ATC, BC,
           ssem, rsem, cssem, crsem, xssem, xrsem):
    g = lax.axis_index("band")
    d = lax.axis_index("dom")
    ylo, z = g // 8, lax.rem(g, 8)
    dprev, dnext = lax.rem(d + ND - 1, ND), lax.rem(d + 1, ND)

    def peer(o):
        dy, dz = OFFSETS[o]
        return lax.rem(ylo + dy, 2) * 8 + lax.rem(z + dz + 8, 8)

    def source(o):
        dy, dz = OFFSETS[o]
        return lax.rem(ylo + dy, 2) * 8 + lax.rem(z - dz + 8, 8)

    barrier = pltpu.get_barrier_semaphore()
    for o in range(NB - 1):
        pl.semaphore_signal(barrier, inc=1, device_id={"band": peer(o)}, device_id_type=MESH)
    pl.semaphore_signal(barrier, inc=1, device_id={"dom": dprev}, device_id_type=MESH)
    pl.semaphore_signal(barrier, inc=1, device_id={"dom": dnext}, device_id_type=MESH)

    for r in range(RPZ):
        xy = (r // 8) * 16 + r % 8
        a = psi[pl.ds(xy, 64, stride=64), :]
        b = psi[pl.ds(xy + 8, 64, stride=64), :]
        T[pl.ds(r, 128, stride=RPZ), :] = jnp.concatenate([a, b], axis=0).T
    T[pl.ds(128 * RPZ, RPZ), :] = T[pl.ds(0, RPZ), :]

    pl.semaphore_wait(barrier, NB + 1)

    def main_copy(o):
        p = peer(o)
        return pltpu.make_async_remote_copy(
            src_ref=T.at[pl.ds(pl.multiple_of(p * (CH * RPZ), CH * RPZ), CHUNK)],
            dst_ref=R.at[g],
            send_sem=ssem.at[o], recv_sem=rsem.at[o],
            device_id={"band": p}, device_id_type=MESH)

    def coef_copy(o):
        p = peer(o)
        return pltpu.make_async_remote_copy(
            src_ref=CS.at[p], dst_ref=CR.at[g],
            send_sem=cssem.at[o], recv_sem=crsem.at[o],
            device_id={"band": p}, device_id_type=MESH)

    def x_copy(o):
        s = source(o) if o < NB - 1 else g
        return pltpu.make_async_remote_copy(
            src_ref=R.at[s].reshape(CH + 1, RPZ, 128).at[pl.ds(0, CH), pl.ds(0, 8)],
            dst_ref=RX.at[s],
            send_sem=xssem.at[o], recv_sem=xrsem.at[o],
            device_id={"dom": dprev}, device_id_type=MESH)

    for o in range(NB - 1):
        main_copy(o).start()

    R[g] = T[pl.ds(pl.multiple_of(g * (CH * RPZ), CH * RPZ), CHUNK), :]

    acc = jnp.zeros((72, 64), F32)
    for r in range(RPZ):
        xy = (r // 8) * 16 + r % 8
        p = jnp.concatenate([psi[pl.ds(xy, 64, stride=64), :], psi[pl.ds(xy + 8, 64, stride=64), :]], axis=1)
        q = jnp.concatenate([proj[pl.ds(xy, 72, stride=64), :], proj[pl.ds(xy + 8, 72, stride=64), :]], axis=1)
        phi, plo = split(p)
        qhi, qlo = split(q)
        acc = acc + dot_nt(qhi, phi) + dot_nt(qhi, plo) + dot_nt(qlo, phi)
    c = jnp.concatenate([acc, jnp.zeros((56, 64), F32)], axis=0)
    chi, clo = split(c)
    ehi, elo = split(ext[...])
    msg = dot(ehi, chi) + dot(ehi, clo) + dot(elo, chi)
    msg = jnp.concatenate([msg, msg], axis=1)
    CS[...] = msg.reshape(NB, 16, 128)
    CR[g] = CS[g]
    for o in range(NB - 1):
        coef_copy(o).start()

    v = 3.0 + pltpu.roll(pot[...], lax.rem(128 - g * CH, 128), 1)
    for zi in range(CH):
        wide = jnp.broadcast_to(v[:, zi:zi + 1], (64, 128))
        for half in range(2):
            for x in range(4):
                VB[zi, half, x * 8:(x + 1) * 8, :] = wide[x * 16 + half * 8:x * 16 + half * 8 + 8]

    x_copy(NB - 1).start()
    for o in range(NB - 1):
        main_copy(o).wait_recv()
        x_copy(o).start()
    for o in range(NB - 1):
        coef_copy(o).wait_recv()
    for o in range(NB):
        x_copy(o).wait_recv()

    low = lax.broadcasted_iota(jnp.int32, (RPZ, 128), 1) < 64
    low8 = lax.broadcasted_iota(jnp.int32, (8, 128), 1) < 64
    low16 = lax.broadcasted_iota(jnp.int32, (16, 128), 1) < 64
    last = lax.broadcasted_iota(jnp.int32, (8, 128), 0) == 7

    def merge(a, b, mask):
        return jnp.where(mask, a, pltpu.roll(b, 64, 1)), jnp.where(mask, pltpu.roll(a, 64, 1), b)

    def assemble(m, _):
        cols = pl.ds(pl.multiple_of(m * 128, 128), 128)
        cols2 = pl.ds(pl.multiple_of(1024 + m * 128, 128), 128)

        def column(zi):
            rows = pl.ds(pl.multiple_of(zi * RPZ, RPZ), RPZ)
            return merge(R[2 * m, rows, :], R[2 * m + 1, rows, :], low)

        now = column(0)
        for zi in range(CH):
            nxt = column(zi + 1)
            halo = merge(RX[2 * m, zi], RX[2 * m + 1, zi], low8)
            turned = []
            for half in range(2):
                turned.append([pltpu.roll(now[half][x * 8:(x + 1) * 8], 7, 0) for x in range(4)])
            for half in range(2):
                a = now[half]
                ax = jnp.concatenate([a[8:], halo[half]], axis=0)
                ay = jnp.concatenate(
                    [jnp.where(last, turned[1 - half][x], turned[half][x]) for x in range(4)], axis=0)
                h = VB[zi, half] * a - ax - ay - nxt[half]
                rows = pl.ds(half * 256 + zi * RPZ, RPZ)
                AF[rows, :] = a
                hi, lo = split(h)
                Bhi[rows, cols] = hi
                Blo[rows, cols] = lo
                hi, lo = split(a)
                Bhi[rows, cols2] = hi
                Blo[rows, cols2] = lo
            now = nxt
        hi, lo = split(AF[...].T)
        AThi[cols, :] = hi
        ATlo[cols, :] = lo
        cc, _ = merge(CR[2 * m], CR[2 * m + 1], low16)
        chi, clo = split(cc)
        c5 = chi.astype(F32)
        zero = jnp.zeros((16, 128), F32)
        row16 = lax.broadcasted_iota(jnp.int32, (16, 128), 0)
        keep = row16 < 5
        ahi = jnp.where(keep, chi.astype(F32), zero)
        alo = jnp.where(keep, clo.astype(F32), zero)
        stack = jnp.concatenate([ahi, ahi, alo, jnp.zeros((80, 128), F32)], axis=0)
        ATC[cols, :] = stack.T.astype(BF16)
        for t, at in ((1, cols), (2, cols2)):
            bhi = jnp.where(keep, pltpu.roll(chi.astype(F32), 16 - 5 * t, 0), zero)
            blo = jnp.where(keep, pltpu.roll(clo.astype(F32), 16 - 5 * t, 0), zero)
            BC[:, at] = jnp.concatenate([bhi, blo, bhi, jnp.zeros((80, 128), F32)], axis=0).astype(BF16)
        return 0

    lax.fori_loop(0, 8, assemble, 0)

    def product(t, _):
        i, j = t // 8, lax.rem(t, 8)
        rows = pl.ds(pl.multiple_of(i * 256, 256), 256)
        cols = pl.ds(pl.multiple_of(j * 256, 256), 256)
        a = AThi[rows, :]
        res = dot(a, Bhi[:, cols]) + dot(a, Blo[:, cols]) + dot(ATlo[rows, :], Bhi[:, cols]) \
            + dot(ATC[rows, :], BC[:, cols])
        res = res * VOLUME
        out[2 * j, rows, :] = res[:, :128]
        out[2 * j + 1, rows, :] = res[:, 128:]
        return 0

    lax.fori_loop(0, 32, product, 0)

    def symmetrize(t, _):
        i, j = t // 8, lax.rem(t, 8)
        ri = pl.ds(pl.multiple_of(i * 128, 128), 128)
        rj = pl.ds(pl.multiple_of(j * 128, 128), 128)

        @pl.when(i <= j)
        def _():
            s = 0.5 * (out[j, ri, :] + out[i, rj, :].T)
            out[j, ri, :] = s
            out[i, rj, :] = s.T
        return 0

    lax.fori_loop(0, 64, symmetrize, 0)

    for o in range(NB - 1):
        main_copy(o).wait_send()
        coef_copy(o).wait_send()
    for o in range(NB):
        x_copy(o).wait_send()


def couple_matrix(hamiltonian_correction, delta_s, projector_count):
    slot = jnp.arange(18, dtype=jnp.int32)
    mask = (slot[None, :] < projector_count[:, None]).astype(F32)
    both = jnp.stack([hamiltonian_correction, delta_s])
    sym = (0.5 / VOLUME) * (both + jnp.swapaxes(both, 2, 3)) * mask[None, :, :, None] * mask[None, :, None, :]
    eye4 = jnp.eye(4, dtype=F32)
    block = (sym[:, :, :, None, :] * eye4[None, :, None, :, None]).reshape(2, 72, 72)
    block = jnp.concatenate([jnp.eye(72, dtype=F32)[None], block])
    block = jnp.pad(block, ((0, 0), (0, 8), (0, 56))).reshape(3, 16, 5, 128)
    rows = jnp.swapaxes(block, 0, 1).reshape(16, 15, 128)
    return jnp.pad(rows, ((0, 0), (0, 1), (0, 0))).reshape(256, 128)


def on_device(wavefunctions, potential, projectors, hamiltonian_correction, delta_s, projector_count):
    psi = wavefunctions.reshape(4096, 128)
    pot = potential.reshape(64, 128)
    proj = projectors.reshape(72 * 64, 128)
    ext = couple_matrix(hamiltonian_correction, delta_s, projector_count)
    vm = pl.BlockSpec(memory_space=pltpu.VMEM)
    part = pl.pallas_call(
        kernel,
        out_shape=jax.ShapeDtypeStruct((16, 1024, 128), F32),
        in_specs=[vm] * 4,
        out_specs=vm,
        scratch_shapes=[
            pltpu.VMEM((129 * RPZ, 128), F32),
            pltpu.VMEM((NB, CHUNK, 128), F32),
            pltpu.VMEM((NB, CH, 8, 128), F32),
            pltpu.VMEM((NB, 16, 128), F32),
            pltpu.VMEM((NB, 16, 128), F32),
            pltpu.VMEM((CH, 2, RPZ, 128), F32),
            pltpu.VMEM((512, 128), F32),
            pltpu.VMEM((1024, 512), BF16),
            pltpu.VMEM((1024, 512), BF16),
            pltpu.VMEM((512, 2048), BF16),
            pltpu.VMEM((512, 2048), BF16),
            pltpu.VMEM((1024, 128), BF16),
            pltpu.VMEM((128, 2048), BF16),
            pltpu.SemaphoreType.DMA((NB,)),
            pltpu.SemaphoreType.DMA((NB,)),
            pltpu.SemaphoreType.DMA((NB,)),
            pltpu.SemaphoreType.DMA((NB,)),
            pltpu.SemaphoreType.DMA((NB,)),
            pltpu.SemaphoreType.DMA((NB,)),
        ],
        compiler_params=pltpu.CompilerParams(
            collective_id=0, has_side_effects=True, vmem_limit_bytes=60 * 1024 * 1024),
    )(psi, pot, proj, ext)
    rows = lax.psum_scatter(part, "band", scatter_dimension=1, tiled=True)
    total = lax.psum(rows, "dom")
    total = jnp.swapaxes(total.reshape(2, 8, 64, 128), 1, 2).reshape(2, 64, 1024)
    return total[0], total[1]


def solution(mesh):
    placed = (
        P("band", "dom", None, None),
        P("dom", None, None),
        P("dom", None, None, None, None),
        P("dom", None, None),
        P("dom", None, None),
        P("dom"),
    )
    return jax.shard_map(
        on_device, mesh=mesh, in_specs=placed,
        out_specs=(P("band", None), P("band", None)), check_vma=False)
```

```python
import functools

import jax
import jax.numpy as jnp
from jax import lax
from jax.experimental import pallas as pl
from jax.experimental.pallas import tpu as pltpu
from jax.sharding import PartitionSpec as P

MESH = pl.DeviceIdType.MESH
F32 = jnp.float32
BF16 = jnp.bfloat16
NB = 16
ND = 16
CH = 8
RPZ = 32
CHUNK = (CH + 1) * RPZ
VOLUME = 1.0 / 131072.0
OFFSETS = [(0, 1), (0, -1), (1, 1), (1, -1), (0, 2), (0, -2), (1, 2), (1, -2), (1, 0),
           (0, 3), (0, -3), (1, 3), (1, -3), (0, 4), (1, 4)]


def split(x):
    hi = x.astype(BF16)
    return hi, (x - hi.astype(F32)).astype(BF16)


def dot(a, b):
    return lax.dot_general(a, b, (((1,), (0,)), ((), ())), preferred_element_type=F32)


def dot_nt(a, b):
    return lax.dot_general(a, b, (((1,), (1,)), ((), ())), preferred_element_type=F32)


def kernel(psi, pot, proj, ext, fin, out, T, R, RX, CS, CR, VB, AF, AThi, ATlo, Bhi, Blo, ATC, BC,
           PB, A1, A2, B1, B2, A3, A4, B3, B4, ZR,
           ssem, rsem, cssem, crsem, xssem, xrsem, pssem, prsem, gssem, grsem, zssem, zrsem, fssem, frsem,
           wssem, wrsem):
    g = lax.axis_index("band")
    d = lax.axis_index("dom")
    ylo, z = g // 8, lax.rem(g, 8)
    xi, yhi, c = d // 4, lax.rem(d // 2, 2), lax.rem(d, 2)
    y = yhi * 2 + ylo
    dprev, dnext = lax.rem(d + ND - 1, ND), lax.rem(d + 1, ND)

    def peer(o):
        dy, dz = OFFSETS[o]
        return lax.rem(ylo + dy, 2) * 8 + lax.rem(z + dz + 8, 8)

    def source(o):
        dy, dz = OFFSETS[o]
        return lax.rem(ylo + dy, 2) * 8 + lax.rem(z - dz + 8, 8)

    barrier = pltpu.get_barrier_semaphore()
    for o in range(NB - 1):
        pl.semaphore_signal(barrier, inc=1, device_id={"band": peer(o)}, device_id_type=MESH)
    for k in range(1, ND):
        pl.semaphore_signal(barrier, inc=1, device_id={"dom": lax.rem(d + k, ND)}, device_id_type=MESH)

    def at_y(q):
        return {"band": lax.rem(q, 2) * 8 + z, "dom": xi * 4 + (q // 2) * 2 + c}

    def at_x(q):
        return {"dom": q * 4 + yhi * 2 + c}

    pl.semaphore_signal(barrier, inc=1, device_id={"band": (1 - ylo) * 8 + z, "dom": xi * 4 + (1 - yhi) * 2 + c},
                        device_id_type=MESH)

    for r in range(RPZ):
        xy = (r // 8) * 16 + r % 8
        a = psi[pl.ds(xy, 64, stride=64), :]
        b = psi[pl.ds(xy + 8, 64, stride=64), :]
        T[pl.ds(r, 128, stride=RPZ), :] = jnp.concatenate([a, b], axis=0).T
    T[pl.ds(128 * RPZ, RPZ), :] = T[pl.ds(0, RPZ), :]

    pl.semaphore_wait(barrier, 31)

    def main_copy(o):
        p = peer(o)
        return pltpu.make_async_remote_copy(
            src_ref=T.at[pl.ds(pl.multiple_of(p * (CH * RPZ), CH * RPZ), CHUNK)],
            dst_ref=R.at[g],
            send_sem=ssem.at[o], recv_sem=rsem.at[o],
            device_id={"band": p}, device_id_type=MESH)

    def coef_copy(o):
        p = peer(o)
        return pltpu.make_async_remote_copy(
            src_ref=CS.at[p], dst_ref=CR.at[g],
            send_sem=cssem.at[o], recv_sem=crsem.at[o],
            device_id={"band": p}, device_id_type=MESH)

    def x_copy(o):
        s = source(o) if o < NB - 1 else g
        return pltpu.make_async_remote_copy(
            src_ref=R.at[s].reshape(CH + 1, RPZ, 128).at[pl.ds(0, CH), pl.ds(0, 8)],
            dst_ref=RX.at[s],
            send_sem=xssem.at[o], recv_sem=xrsem.at[o],
            device_id={"dom": dprev}, device_id_type=MESH)

    for o in range(NB - 1):
        main_copy(o).start()

    R[g] = T[pl.ds(pl.multiple_of(g * (CH * RPZ), CH * RPZ), CHUNK), :]

    acc = jnp.zeros((72, 64), F32)
    for r in range(RPZ):
        xy = (r // 8) * 16 + r % 8
        p = jnp.concatenate([psi[pl.ds(xy, 64, stride=64), :], psi[pl.ds(xy + 8, 64, stride=64), :]], axis=1)
        q = jnp.concatenate([proj[pl.ds(xy, 72, stride=64), :], proj[pl.ds(xy + 8, 72, stride=64), :]], axis=1)
        phi, plo = split(p)
        qhi, qlo = split(q)
        acc = acc + dot_nt(qhi, phi) + dot_nt(qhi, plo) + dot_nt(qlo, phi)
    craw = jnp.concatenate([acc, jnp.zeros((56, 64), F32)], axis=0)
    chi, clo = split(craw)
    ehi, elo = split(ext[...])
    msg = dot(ehi, chi) + dot(ehi, clo) + dot(elo, chi)
    msg = jnp.concatenate([msg, msg], axis=1)
    CS[...] = msg.reshape(NB, 16, 128)
    CR[g] = CS[g]
    for o in range(NB - 1):
        coef_copy(o).start()

    v = 3.0 + pltpu.roll(pot[...], lax.rem(128 - g * CH, 128), 1)
    for zi in range(CH):
        wide = jnp.broadcast_to(v[:, zi:zi + 1], (64, 128))
        for half in range(2):
            for x in range(4):
                VB[zi, half, x * 8:(x + 1) * 8, :] = wide[x * 16 + half * 8:x * 16 + half * 8 + 8]

    x_copy(NB - 1).start()
    for o in range(NB - 1):
        main_copy(o).wait_recv()
        x_copy(o).start()
    for o in range(NB - 1):
        coef_copy(o).wait_recv()
    for o in range(NB):
        x_copy(o).wait_recv()

    low = lax.broadcasted_iota(jnp.int32, (RPZ, 128), 1) < 64
    low8 = lax.broadcasted_iota(jnp.int32, (8, 128), 1) < 64
    low16 = lax.broadcasted_iota(jnp.int32, (16, 128), 1) < 64
    last = lax.broadcasted_iota(jnp.int32, (8, 128), 0) == 7

    def merge(a, b, mask):
        return jnp.where(mask, a, pltpu.roll(b, 64, 1)), jnp.where(mask, pltpu.roll(a, 64, 1), b)

    def assemble(m, _):
        cols = pl.ds(pl.multiple_of(m * 128, 128), 128)
        cols2 = pl.ds(pl.multiple_of(1024 + m * 128, 128), 128)

        def column(zi):
            rows = pl.ds(pl.multiple_of(zi * RPZ, RPZ), RPZ)
            return merge(R[2 * m, rows, :], R[2 * m + 1, rows, :], low)

        now = column(0)
        for zi in range(CH):
            nxt = column(zi + 1)
            halo = merge(RX[2 * m, zi], RX[2 * m + 1, zi], low8)
            turned = []
            for half in range(2):
                turned.append([pltpu.roll(now[half][x * 8:(x + 1) * 8], 7, 0) for x in range(4)])
            for half in range(2):
                a = now[half]
                ax = jnp.concatenate([a[8:], halo[half]], axis=0)
                ay = jnp.concatenate(
                    [jnp.where(last, turned[1 - half][x], turned[half][x]) for x in range(4)], axis=0)
                h = VB[zi, half] * a - ax - ay - nxt[half]
                rows = pl.ds(half * 256 + zi * RPZ, RPZ)
                AF[rows, :] = a
                hi, lo = split(h)
                Bhi[rows, cols] = hi
                Blo[rows, cols] = lo
                hi, lo = split(a)
                Bhi[rows, cols2] = hi
                Blo[rows, cols2] = lo
            now = nxt
        hi, lo = split(AF[...].T)
        AThi[cols, :] = hi
        ATlo[cols, :] = lo
        cc, _ = merge(CR[2 * m], CR[2 * m + 1], low16)
        chi, clo = split(cc)
        c5 = chi.astype(F32)
        zero = jnp.zeros((16, 128), F32)
        row16 = lax.broadcasted_iota(jnp.int32, (16, 128), 0)
        keep = row16 < 5
        ahi = jnp.where(keep, chi.astype(F32), zero)
        alo = jnp.where(keep, clo.astype(F32), zero)
        stack = jnp.concatenate([ahi, ahi, alo, jnp.zeros((80, 128), F32)], axis=0)
        ATC[cols, :] = stack.T.astype(BF16)
        for t, at in ((1, cols), (2, cols2)):
            bhi = jnp.where(keep, pltpu.roll(chi.astype(F32), 16 - 5 * t, 0), zero)
            blo = jnp.where(keep, pltpu.roll(clo.astype(F32), 16 - 5 * t, 0), zero)
            BC[:, at] = jnp.concatenate([bhi, blo, bhi, jnp.zeros((80, 128), F32)], axis=0).astype(BF16)
        return 0

    lax.fori_loop(0, 8, assemble, 0)

    def product(first, t):
        i, j = t // 4, first + lax.rem(t, 4)
        rows = pl.ds(pl.multiple_of(i * 256, 256), 256)
        cols = pl.ds(pl.multiple_of(j * 256, 256), 256)
        a = AThi[rows, :]
        res = dot(a, Bhi[:, cols]) + dot(a, Blo[:, cols]) + dot(ATlo[rows, :], Bhi[:, cols]) \
            + dot(ATC[rows, :], BC[:, cols])
        res = res * VOLUME
        out[2 * j, rows, :] = res[:, :128]
        out[2 * j + 1, rows, :] = res[:, 128:]

    def matrix(first):
        def body(t, _):
            product(first, t)
            return 0
        lax.fori_loop(0, 16, body, 0)

    def symmetrize():
        def body(t, _):
            i, j = t // 8, lax.rem(t, 8)
            ri = pl.ds(pl.multiple_of(i * 128, 128), 128)
            rj = pl.ds(pl.multiple_of(j * 128, 128), 128)

            @pl.when(i <= j)
            def _():
                s = 0.5 * (out[j, ri, :] + out[i, rj, :].T)
                out[j, ri, :] = s
                out[i, rj, :] = s.T
            return 0
        lax.fori_loop(0, 64, body, 0)

    other = d + 1 - 2 * c

    def pair_copy(t):
        return pltpu.make_async_remote_copy(
            src_ref=out.at[(1 - c) * 8 + t], dst_ref=PB.at[t], send_sem=pssem.at[t], recv_sem=prsem.at[t],
            device_id={"dom": other}, device_id_type=MESH)

    matrix((1 - c) * 4)

    @pl.when(c == 1)
    def _():
        symmetrize()

    for t in range(8):
        pair_copy(t).start()
    matrix(c * 4)

    @pl.when(c == 0)
    def _():
        symmetrize()

    base = c * 8
    for t in range(8):
        pair_copy(t).wait_recv()

    def add_pair(tile, ly, part):
        rows = pl.ds(pl.multiple_of(ly * 512 + part * 256, 256), 256)
        out[base + tile, rows, :] = out[base + tile, rows, :] + PB[tile, rows, :]

    def rows_of(ly, at, count):
        return pl.ds(pl.multiple_of(ly * 512 + at, 64), count)

    def remote(src, dst, n, where):
        return pltpu.make_async_remote_copy(
            src_ref=src, dst_ref=dst, send_sem=gssem.at[n], recv_sem=grsem.at[n],
            device_id=where, device_id_type=MESH)

    class Ring:
        def __init__(self, me, at, pieces, first, second, number):
            self.me, self.pieces, self.first, self.second = me, pieces, first, second
            self.plus, self.minus = at(lax.rem(me + 1, 4)), at(lax.rem(me + 3, 4))
            self.number = number

        def views(self, q, h):
            return [out.at[v] for v in self.pieces(q, h)]

        def copies(self, k):
            me = self.me
            q, h, buf, way = (
                (me + 2, 0, self.first.at[0], self.plus),
                (me + 2, 1, self.first.at[1], self.minus),
                (me + 1, 1, self.second.at[0, 1], self.plus),
                (me + 3, 0, self.second.at[1, 0], self.minus),
                (me + 1, 0, self.second.at[0, 0], self.plus),
                (me + 3, 1, self.second.at[1, 1], self.minus),
            )[k]
            views = self.views(lax.rem(q, 4), h)
            return [remote(v, buf.at[i], self.number + 2 * k + i, way) for i, v in enumerate(views)]

        def start(self, k):
            for c_ in self.copies(k):
                c_.start()

        def wait_recv(self, k):
            for c_ in self.copies(k):
                c_.wait_recv()

        def wait_send(self, k):
            for c_ in self.copies(k):
                c_.wait_send()

        def add(self, q, h, *bufs):
            for i, v in enumerate(self.pieces(lax.rem(q, 4), h)):
                total = out[v]
                for b in bufs:
                    total = total + b[i]
                out[v] = total

        def relay(self):
            self.wait_recv(0)
            self.add(self.me + 1, 0, self.first.at[0])
            self.start(4)
            self.wait_recv(1)
            self.add(self.me + 3, 1, self.first.at[1])
            self.start(5)

        def finish(self):
            self.wait_recv(2)
            self.wait_recv(3)
            self.wait_recv(4)
            self.wait_recv(5)
            for h in range(2):
                self.add(self.me, h, self.second.at[0, h], self.second.at[1, h])

    def pieces_ax(q, h):
        return [(base + h * 4 + q, pl.ds(ly * 512, 256), slice(None)) for ly in range(2)]

    def pieces_by(q, h):
        return [(base + (q // 2) * 4 + 2 * h + i, rows_of(lax.rem(q, 2), 256, 256), slice(None)) for i in range(2)]

    def pieces_ay(q, h):
        return [(base + (q // 2) * 4 + xi, rows_of(lax.rem(q, 2), h * 128, 128), slice(None))]

    def pieces_bx(q, h):
        return [(base + yhi * 4 + q, rows_of(ylo, 256 + h * 128, 128), slice(None))]

    ax = Ring(xi, at_x, pieces_ax, A1, A2, 0)
    by = Ring(y, at_y, pieces_by, B1, B2, 12)
    ay = Ring(y, at_y, pieces_ay, A3, A4, 24)
    bx = Ring(xi, at_x, pieces_bx, B3, B4, 36)

    def add_ax(q, h):
        for ly in range(2):
            add_pair(h * 4 + lax.rem(q, 4), ly, 0)

    def add_by(q, h):
        q = lax.rem(q, 4)
        for i in range(2):
            add_pair((q // 2) * 4 + 2 * h + i, lax.rem(q, 2), 1)

    order = ((2, 0, 0), (2, 1, 1), (1, 1, 2), (3, 0, 3))
    for step, h, k in order:
        add_ax(xi + step, h)
        ax.start(k)
        add_by(y + step, h)
        by.start(k)
    for step, h in ((1, 0), (3, 1)):
        add_ax(xi + step, h)
        add_by(y + step, h)
    ax.relay()
    by.relay()
    for h in range(2):
        add_ax(xi, h)
        add_by(y, h)
    ax.finish()
    for k in range(4):
        ay.start(k)
    by.finish()
    for k in range(4):
        bx.start(k)
    ay.relay()
    bx.relay()
    ay.finish()
    bx.finish()

    tile = yhi * 4 + xi

    def z_copy(k):
        q = lax.rem(z + k, 8)
        return pltpu.make_async_remote_copy(
            src_ref=out.at[base + tile, rows_of(ylo, q * 64, 64)], dst_ref=ZR.at[k - 1],
            send_sem=zssem.at[k - 1], recv_sem=zrsem.at[k - 1],
            device_id={"band": ylo * 8 + q}, device_id_type=MESH)

    for k in (4, 3, 5, 2, 6, 1, 7):
        z_copy(k).start()
    total = out[base + tile, rows_of(ylo, z * 64, 64), :]
    for k in range(1, 8):
        z_copy(k).wait_recv()
        total = total + ZR[k - 1]
    at = pl.ds(pl.multiple_of(tile * 128, 128), 128)
    fin[c, :, at] = total

    def column(x_, h_):
        return pl.ds(pl.multiple_of((h_ * 4 + x_) * 128, 128), 128)

    def gather_copy(k):
        px, ph = lax.rem(xi + k // 2, 4), lax.rem(yhi + k, 2)
        return pltpu.make_async_remote_copy(
            src_ref=fin.at[c, :, at], dst_ref=fin.at[c, :, at],
            send_sem=fssem.at[k - 1], recv_sem=frsem.at[k - 1],
            device_id={"dom": px * 4 + ph * 2 + c}, device_id_type=MESH)

    def swap_copy(k):
        px, ph = lax.rem(xi - k // 2 + 4, 4), lax.rem(yhi + k, 2)
        part = fin.at[c, :, column(px, ph)]
        return pltpu.make_async_remote_copy(
            src_ref=part, dst_ref=part, send_sem=wssem.at[k], recv_sem=wrsem.at[k],
            device_id={"dom": other}, device_id_type=MESH)

    for k in range(1, 8):
        gather_copy(k).start()
    swap_copy(0).start()
    for k in range(1, 8):
        gather_copy(k).wait_recv()
        swap_copy(k).start()
    for k in range(8):
        swap_copy(k).wait_recv()

    for t in range(8):
        pair_copy(t).wait_send()
    for ring in (ax, by, ay, bx):
        for k in range(6):
            ring.wait_send(k)
    for k in range(1, 8):
        z_copy(k).wait_send()
        gather_copy(k).wait_send()
    for k in range(8):
        swap_copy(k).wait_send()
    for o in range(NB - 1):
        main_copy(o).wait_send()
        coef_copy(o).wait_send()
    for o in range(NB):
        x_copy(o).wait_send()


def couple_matrix(hamiltonian_correction, delta_s, projector_count):
    slot = jnp.arange(18, dtype=jnp.int32)
    mask = (slot[None, :] < projector_count[:, None]).astype(F32)
    both = jnp.stack([hamiltonian_correction, delta_s])
    sym = (0.5 / VOLUME) * (both + jnp.swapaxes(both, 2, 3)) * mask[None, :, :, None] * mask[None, :, None, :]
    eye4 = jnp.eye(4, dtype=F32)
    block = (sym[:, :, :, None, :] * eye4[None, :, None, :, None]).reshape(2, 72, 72)
    block = jnp.concatenate([jnp.eye(72, dtype=F32)[None], block])
    block = jnp.pad(block, ((0, 0), (0, 8), (0, 56))).reshape(3, 16, 5, 128)
    rows = jnp.swapaxes(block, 0, 1).reshape(16, 15, 128)
    return jnp.pad(rows, ((0, 0), (0, 1), (0, 0))).reshape(256, 128)


def on_device(wavefunctions, potential, projectors, hamiltonian_correction, delta_s, projector_count):
    psi = wavefunctions.reshape(4096, 128)
    pot = potential.reshape(64, 128)
    proj = projectors.reshape(72 * 64, 128)
    ext = couple_matrix(hamiltonian_correction, delta_s, projector_count)
    vm = pl.BlockSpec(memory_space=pltpu.VMEM)
    part = pl.pallas_call(
        kernel,
        out_shape=jax.ShapeDtypeStruct((2, 64, 1024), F32),
        in_specs=[vm] * 4,
        out_specs=vm,
        scratch_shapes=[
            pltpu.VMEM((16, 1024, 128), F32),
            pltpu.VMEM((129 * RPZ, 128), F32),
            pltpu.VMEM((NB, CHUNK, 128), F32),
            pltpu.VMEM((NB, CH, 8, 128), F32),
            pltpu.VMEM((NB, 16, 128), F32),
            pltpu.VMEM((NB, 16, 128), F32),
            pltpu.VMEM((CH, 2, RPZ, 128), F32),
            pltpu.VMEM((512, 128), F32),
            pltpu.VMEM((1024, 512), BF16),
            pltpu.VMEM((1024, 512), BF16),
            pltpu.VMEM((512, 2048), BF16),
            pltpu.VMEM((512, 2048), BF16),
            pltpu.VMEM((1024, 128), BF16),
            pltpu.VMEM((128, 2048), BF16),
            pltpu.VMEM((8, 1024, 128), F32),
            pltpu.VMEM((2, 2, 256, 128), F32),
            pltpu.VMEM((2, 2, 2, 256, 128), F32),
            pltpu.VMEM((2, 2, 256, 128), F32),
            pltpu.VMEM((2, 2, 2, 256, 128), F32),
            pltpu.VMEM((2, 1, 128, 128), F32),
            pltpu.VMEM((2, 2, 1, 128, 128), F32),
            pltpu.VMEM((2, 1, 128, 128), F32),
            pltpu.VMEM((2, 2, 1, 128, 128), F32),
            pltpu.VMEM((7, 64, 128), F32),
            pltpu.SemaphoreType.DMA((NB,)),
            pltpu.SemaphoreType.DMA((NB,)),
            pltpu.SemaphoreType.DMA((NB,)),
            pltpu.SemaphoreType.DMA((NB,)),
            pltpu.SemaphoreType.DMA((NB,)),
            pltpu.SemaphoreType.DMA((NB,)),
            pltpu.SemaphoreType.DMA((8,)),
            pltpu.SemaphoreType.DMA((8,)),
            pltpu.SemaphoreType.DMA((48,)),
            pltpu.SemaphoreType.DMA((48,)),
            pltpu.SemaphoreType.DMA((7,)),
            pltpu.SemaphoreType.DMA((7,)),
            pltpu.SemaphoreType.DMA((7,)),
            pltpu.SemaphoreType.DMA((7,)),
            pltpu.SemaphoreType.DMA((8,)),
            pltpu.SemaphoreType.DMA((8,)),
        ],
        compiler_params=pltpu.CompilerParams(
            collective_id=0, has_side_effects=True, vmem_limit_bytes=60 * 1024 * 1024),
    )(psi, pot, proj, ext)
    return part[0], part[1]


def solution(mesh):
    placed = (
        P("band", "dom", None, None),
        P("dom", None, None),
        P("dom", None, None, None, None),
        P("dom", None, None),
        P("dom", None, None),
        P("dom"),
    )
    return jax.shard_map(
        on_device, mesh=mesh, in_specs=placed,
        out_specs=(P("band", None), P("band", None)), check_vma=False)
```

```python
import jax
import jax.numpy as jnp
from jax import lax
from jax.experimental import pallas as pl
from jax.experimental.pallas import tpu as pltpu
from jax.sharding import PartitionSpec as P

MESH = pl.DeviceIdType.MESH
F32 = jnp.float32
BF16 = jnp.bfloat16
NB = 16
ND = 16
CH = 8
RPZ = 32
CHUNK = (CH + 1) * RPZ
VOLUME = 1.0 / 131072.0
DZ = (0, 1, 7, 2, 6, 3, 5, 4)
OFFSETS = [(1, 0)] + [(dy, (8 - DZ[p]) % 8) for p in range(1, 8) for dy in (0, 1)]
STAGES = ((0, 5), (5, 7), (7, 8))
START = (0, 25, 49, 64)
HALF = (12, 12, 7)


def block_of(row, col):
    top = max(row, col)
    if top < 5:
        return col * 5 + row
    if top < 7:
        return 25 + col * 2 + row - 5 if col < 5 else 35 + (col - 5) * 7 + row
    return 49 + col if col < 7 else 56 + row


def split(x):
    hi = x.astype(BF16)
    return hi, (x - hi.astype(F32)).astype(BF16)


def dot(a, b):
    return lax.dot_general(a, b, (((1,), (0,)), ((), ())), preferred_element_type=F32)


def dot_exact(a, b):
    return lax.dot_general(a, b, (((1,), (0,)), ((), ())), precision=lax.Precision.HIGHEST,
                           preferred_element_type=F32)


def dot_nt(a, b):
    return lax.dot_general(a, b, (((1,), (1,)), ((), ())), preferred_element_type=F32)


def kernel(psi_in, pot, proj_in, hcor, dels, count, ham, corr,
           psi, proj, SP, M, T, R, RX, CS, CR, VB, AF, AThi, ATlo, Bhi, Blo, ATC, BC, PB,
           F1, F2, G1, G2, ZS, ZR, fin,
           lsem, ssem, rsem, cssem, crsem, xssem, xrsem, pssem, prsem, gssem, grsem,
           zssem, zrsem, fssem, frsem, wssem, wrsem):
    g = lax.axis_index("band")
    d = lax.axis_index("dom")
    ylo, z = g // 8, lax.rem(g, 8)
    xi, yhi, c = d // 4, lax.rem(d // 2, 2), lax.rem(d, 2)
    y = yhi * 2 + ylo
    dprev = lax.rem(d + ND - 1, ND)
    other = d + 1 - 2 * c

    def peer(o):
        dy, dz = OFFSETS[o]
        return lax.rem(ylo + dy, 2) * 8 + lax.rem(z + dz, 8)

    def source(o):
        dy, dz = OFFSETS[o]
        return lax.rem(ylo + dy, 2) * 8 + lax.rem(z - dz + 8, 8)

    def at_y(q):
        return {"band": lax.rem(q, 2) * 8 + z, "dom": xi * 4 + (q // 2) * 2 + c}

    def at_x(q):
        return {"dom": q * 4 + yhi * 2 + c}

    load_psi = pltpu.make_async_copy(psi_in, psi, lsem.at[0])
    load_proj = pltpu.make_async_copy(proj_in, proj, lsem.at[1])
    load_psi.start()
    load_proj.start()

    barrier = pltpu.get_barrier_semaphore()
    for o in range(NB - 1):
        pl.semaphore_signal(barrier, inc=1, device_id={"band": peer(o)}, device_id_type=MESH)
    for k in range(1, ND):
        pl.semaphore_signal(barrier, inc=1, device_id={"dom": lax.rem(d + k, ND)}, device_id_type=MESH)
    pl.semaphore_signal(barrier, inc=1, device_id={"band": (1 - ylo) * 8 + z, "dom": xi * 4 + (1 - yhi) * 2 + c},
                        device_id_type=MESH)

    load_psi.wait()
    for r in range(RPZ):
        xy = (r // 8) * 16 + r % 8
        a = psi[pl.ds(xy, 64, stride=64), :]
        b = psi[pl.ds(xy + 8, 64, stride=64), :]
        T[pl.ds(r, 128, stride=RPZ), :] = jnp.concatenate([a, b], axis=0).T
    T[pl.ds(128 * RPZ, RPZ), :] = T[pl.ds(0, RPZ), :]

    pl.semaphore_wait(barrier, 31)

    def main_copy(o):
        p = peer(o)
        return pltpu.make_async_remote_copy(
            src_ref=T.at[pl.ds(pl.multiple_of(p * (CH * RPZ), CH * RPZ), CHUNK)],
            dst_ref=R.at[g],
            send_sem=ssem.at[o], recv_sem=rsem.at[o],
            device_id={"band": p}, device_id_type=MESH)

    def coef_copy(o):
        p = peer(o)
        return pltpu.make_async_remote_copy(
            src_ref=CS.at[p], dst_ref=CR.at[g],
            send_sem=cssem.at[o], recv_sem=crsem.at[o],
            device_id={"band": p}, device_id_type=MESH)

    def x_copy(o):
        s = source(o) if o < NB - 1 else g
        return pltpu.make_async_remote_copy(
            src_ref=R.at[s].reshape(CH + 1, RPZ, 128).at[pl.ds(0, CH), pl.ds(0, 8)],
            dst_ref=RX.at[s],
            send_sem=xssem.at[o], recv_sem=xrsem.at[o],
            device_id={"dom": dprev}, device_id_type=MESH)

    for o in range(NB - 1):
        main_copy(o).start()

    R[g] = T[pl.ds(pl.multiple_of(g * (CH * RPZ), CH * RPZ), CHUNK), :]

    load_proj.wait()
    def project(t, acc):
        for x in range(4):
            xy = x * 16 + t
            p = jnp.concatenate([psi[pl.ds(xy, 64, stride=64), :], psi[pl.ds(xy + 8, 64, stride=64), :]], axis=1)
            q = jnp.concatenate([proj[pl.ds(xy, 72, stride=64), :], proj[pl.ds(xy + 8, 72, stride=64), :]], axis=1)
            phi, plo = split(p)
            qhi, qlo = split(q)
            acc = acc + dot_nt(qhi, phi) + dot_nt(qhi, plo) + dot_nt(qlo, phi)
        return acc

    acc = lax.fori_loop(0, 8, project, jnp.zeros((72, 64), F32))
    craw = jnp.concatenate([acc, jnp.zeros((56, 64), F32)], axis=0)
    x_copy(NB - 1).start()

    line = lax.broadcasted_iota(jnp.int32, (256, 128), 0)
    slot = lax.broadcasted_iota(jnp.int32, (256, 128), 1)
    spot = (line >> 4) * 5 + (line & 15)
    ext = jnp.where((line & 15) < 5, jnp.where(slot == spot, 1.0, 0.0), 0.0)
    srow = lax.broadcasted_iota(jnp.int32, (128, 128), 0)
    scol = lax.broadcasted_iota(jnp.int32, (128, 128), 1)
    SP[...] = jnp.zeros_like(SP)
    for t, ref in ((1, hcor), (2, dels)):
        inside = jnp.where((line & 15) >= 5 * t, jnp.where((line & 15) < 5 * t + 5, 1.0, 0.0), 0.0)

        def couple(a, ext):
            SP[0:18, 0:18] = ref[a]
            s = SP[...]
            s = (0.5 / VOLUME) * (s + s.T)
            used_col = jnp.clip(count[a] - slot, 0, 1).astype(F32)
            used_row = jnp.clip(count[a] - srow, 0, 1).astype(F32)
            left = jnp.where(spot - 5 * t == a * 18 + slot, used_col, 0.0) * inside
            right = jnp.where(scol == a * 18 + srow, used_row, 0.0)
            return ext + dot_exact(dot_exact(left, s), right)

        ext = lax.fori_loop(0, 4, couple, ext)
    chi, clo = split(craw)
    ehi, elo = split(ext)
    msg = dot(ehi, chi) + dot(ehi, clo) + dot(elo, chi)
    msg = jnp.concatenate([msg, msg], axis=1)
    CS[...] = msg.reshape(NB, 16, 128)
    CR[g] = CS[g]
    for o in range(NB - 1):
        coef_copy(o).start()

    v = 3.0 + pltpu.roll(pot[...], lax.rem(128 - g * CH, 128), 1)
    for zi in range(CH):
        wide = jnp.broadcast_to(v[:, zi:zi + 1], (64, 128))
        for half in range(2):
            for x in range(4):
                VB[zi, half, x * 8:(x + 1) * 8, :] = wide[x * 16 + half * 8:x * 16 + half * 8 + 8]

    low = lax.broadcasted_iota(jnp.int32, (RPZ, 128), 1) < 64
    low8 = lax.broadcasted_iota(jnp.int32, (8, 128), 1) < 64
    low16 = lax.broadcasted_iota(jnp.int32, (16, 128), 1) < 64
    last = lax.broadcasted_iota(jnp.int32, (8, 128), 0) == 7
    keep = lax.broadcasted_iota(jnp.int32, (16, 128), 0) < 5

    def merge(a, b, mask):
        return jnp.where(mask, a, pltpu.roll(b, 64, 1)), jnp.where(mask, pltpu.roll(a, 64, 1), b)

    def assemble(m, _):
        odd = lax.rem(m, 2)
        dz = odd * ((m + 1) // 2) + (1 - odd) * (8 - m // 2)
        s0 = lax.rem(z + dz, 8)
        s1 = s0 + 8
        rowsm = pl.ds(pl.multiple_of(m * 128, 128), 128)
        cols = pl.ds(pl.multiple_of(m * 256, 256), 128)
        cols2 = pl.ds(pl.multiple_of(m * 256 + 128, 128), 128)

        def column(zi):
            rows = pl.ds(zi * RPZ, RPZ)
            return merge(R[s0, rows, :], R[s1, rows, :], low)

        now = column(0)
        for zi in range(CH):
            nxt = column(zi + 1)
            halo = merge(RX[s0, zi], RX[s1, zi], low8)
            turned = []
            for half in range(2):
                turned.append([pltpu.roll(now[half][x * 8:(x + 1) * 8], 7, 0) for x in range(4)])
            for half in range(2):
                a = now[half]
                ax = jnp.concatenate([a[8:], halo[half]], axis=0)
                ay = jnp.concatenate(
                    [jnp.where(last, turned[1 - half][x], turned[half][x]) for x in range(4)], axis=0)
                h = VB[zi, half] * a - ax - ay - nxt[half]
                rows = pl.ds(half * 256 + zi * RPZ, RPZ)
                AF[rows, :] = a
                hi, lo = split(h)
                Bhi[rows, cols] = hi
                Blo[rows, cols] = lo
                hi, lo = split(a)
                Bhi[rows, cols2] = hi
                Blo[rows, cols2] = lo
            now = nxt
        hi, lo = split(AF[...].T)
        AThi[rowsm, :] = hi
        ATlo[rowsm, :] = lo
        cc, _ = merge(CR[s0], CR[s1], low16)
        chi, clo = split(cc)
        chi, clo = chi.astype(F32), clo.astype(F32)
        zero = jnp.zeros((16, 128), F32)
        pad = jnp.zeros((80, 128), F32)
        ahi = jnp.where(keep, chi, zero)
        alo = jnp.where(keep, clo, zero)
        ATC[rowsm, :] = jnp.concatenate([ahi, ahi, alo, pad], axis=0).T.astype(BF16)
        for t, at in ((1, cols), (2, cols2)):
            bhi = jnp.where(keep, pltpu.roll(chi, 16 - 5 * t, 0), zero)
            blo = jnp.where(keep, pltpu.roll(clo, 16 - 5 * t, 0), zero)
            BC[:, at] = jnp.concatenate([bhi, blo, bhi, pad], axis=0).astype(BF16)
        return 0

    def product(first, n, col, at):
        rows = pl.ds(pl.multiple_of(first * 128, 128), n * 128)
        cols = pl.ds(pl.multiple_of(col * 256, 256), 256)
        a = AThi[rows, :]
        res = dot(a, Bhi[:, cols]) + dot(a, Blo[:, cols]) + dot(ATlo[rows, :], Bhi[:, cols]) \
            + dot(ATC[rows, :], BC[:, cols])
        res = res * VOLUME
        for r in range(n):
            for mat in range(2):
                M[mat * 64 + at + r] = res[r * 128:(r + 1) * 128, mat * 128:(mat + 1) * 128].reshape(2, 4, 2, 8, 128)

    def loop(count_, body):
        def step(t, _):
            body(t)
            return 0
        lax.fori_loop(0, count_, step, 0)

    def even(k, l):
        s = 0.5 * (M[k].reshape(128, 128) + M[l].reshape(128, 128).T)
        M[k] = s.reshape(2, 4, 2, 8, 128)
        M[l] = s.T.reshape(2, 4, 2, 8, 128)

    def products(stage):
        if stage == 0:
            loop(5, lambda t: product(0, 2, t, t * 5))
            loop(5, lambda t: product(2, 2, t, t * 5 + 2))
            loop(5, lambda t: product(4, 1, t, t * 5 + 4))

            def pair(t):
                i, j = t // 5, lax.rem(t, 5)

                @pl.when(i <= j)
                def _():
                    even(j * 5 + i, i * 5 + j)
            loop(25, pair)
        elif stage == 1:
            loop(5, lambda t: product(5, 2, t, 25 + t * 2))
            for i in range(3):
                loop(2, lambda t: product(2 * i, 2, 5 + t, 35 + t * 7 + 2 * i))
            loop(2, lambda t: product(6, 1, 5 + t, 35 + t * 7 + 6))
            loop(10, lambda t: even(35 + (t // 5) * 7 + lax.rem(t, 5), 25 + lax.rem(t, 5) * 2 + t // 5))
            for i, j in ((5, 5), (5, 6), (6, 6)):
                even(block_of(i, j), block_of(j, i))
        else:
            loop(7, lambda t: product(7, 1, t, 49 + t))
            loop(4, lambda t: product(2 * t, 2, 7, 56 + 2 * t))
            loop(7, lambda t: even(56 + t, 49 + t))
            even(63, 63)

    def pair_copy(stage):
        k0, n = START[stage], START[stage + 1] - START[stage]
        return pltpu.make_async_remote_copy(
            src_ref=M.at[pl.ds((1 - c) * 64 + k0, n)], dst_ref=PB.at[pl.ds(k0, n)],
            send_sem=pssem.at[stage], recv_sem=prsem.at[stage],
            device_id={"dom": other}, device_id_type=MESH)

    base = c * 64

    def add_pair(stage):
        pair_copy(stage).wait_recv()

        def body(t):
            M[base + START[stage] + t] = M[base + START[stage] + t] + PB[START[stage] + t]
        loop(START[stage + 1] - START[stage], body)

    class Ring:
        def __init__(self, me, at, piece, first, second, number):
            self.me, self.piece, self.first, self.second = me, piece, first, second
            self.plus, self.minus = at(lax.rem(me + 1, 4)), at(lax.rem(me + 3, 4))
            self.number = number

        def copy(self, k):
            me = self.me
            q, h, buf, way = (
                (me + 2, 0, self.first(0), self.plus),
                (me + 2, 1, self.first(1), self.minus),
                (me + 1, 1, self.second(0, 1), self.plus),
                (me + 3, 0, self.second(1, 0), self.minus),
                (me + 1, 0, self.second(0, 0), self.plus),
                (me + 3, 1, self.second(1, 1), self.minus),
            )[k]
            return pltpu.make_async_remote_copy(
                src_ref=M.at[self.piece(lax.rem(q, 4), h)], dst_ref=buf,
                send_sem=gssem.at[self.number + k], recv_sem=grsem.at[self.number + k],
                device_id=way, device_id_type=MESH)

        def start(self):
            for k in range(4):
                self.copy(k).start()

        def add(self, q, h, *bufs):
            at = self.piece(lax.rem(q, 4), h)
            total = M[at]
            for b in bufs:
                total = total + b[...]
            M[at] = total

        def relay(self):
            self.copy(0).wait_recv()
            self.add(self.me + 1, 0, self.first(0))
            self.copy(4).start()
            self.copy(1).wait_recv()
            self.add(self.me + 3, 1, self.first(1))
            self.copy(5).start()

        def finish(self):
            for k in range(2, 6):
                self.copy(k).wait_recv()
            for h in range(2):
                self.add(self.me, h, self.second(0, h), self.second(1, h))

        def wait_send(self):
            for k in range(6):
                self.copy(k).wait_send()

    rings = []
    full = slice(None)
    for stage in range(3):
        k0, n = START[stage], START[stage + 1] - START[stage]
        na = HALF[stage]
        nb = n - na
        kb = k0 + na
        ha = (na // 2, na - na // 2)
        hb = (nb // 2, nb - nb // 2)

        def ax_piece(q, h, k0=k0, na=na):
            return (pl.ds(base + k0, na), h, q)

        def by_piece(q, h, kb=kb, nb=nb):
            return (pl.ds(base + kb, nb), lax.rem(q, 2), pl.ds(2 * h, 2), q // 2)

        def ay_piece(q, h, k0=k0, ha=ha):
            return (pl.ds(base + k0 + h * ha[0], ha[h]), lax.rem(q, 2), xi, q // 2)

        def bx_piece(q, h, kb=kb, hb=hb):
            return (pl.ds(base + kb + h * hb[0], hb[h]), ylo, q, yhi)

        def wide_first(k, n):
            return lambda h: F1.at[h, pl.ds(k, n)]

        def wide_second(k, n):
            return lambda w, h: F2.at[w, h, pl.ds(k, n)]

        def thin_first(k, hs):
            return lambda h: G1.at[pl.ds(k + h * hs[0], hs[h])]

        def thin_second(k, hs):
            return lambda w, h: G2.at[w, pl.ds(k + h * hs[0], hs[h])]

        rings.append((
            Ring(xi, at_x, ax_piece, wide_first(k0, na), wide_second(k0, na), stage * 24),
            Ring(y, at_y, by_piece, wide_first(kb, nb), wide_second(kb, nb), stage * 24 + 6),
            Ring(y, at_y, ay_piece, thin_first(k0, ha), thin_second(k0, ha), stage * 24 + 12),
            Ring(xi, at_x, bx_piece, thin_first(kb, hb), thin_second(kb, hb), stage * 24 + 18),
        ))

    def arrive(positions):
        for p in positions:
            for o in ((0,) if p == 0 else (2 * p - 1, 2 * p)):
                main_copy(o).wait_recv()
                x_copy(o).start()

    def ready(positions):
        for p in positions:
            for o in ((0, NB - 1) if p == 0 else (2 * p - 1, 2 * p)):
                x_copy(o).wait_recv()
                if o < NB - 1:
                    coef_copy(o).wait_recv()

    def build(stage):
        first, last_ = STAGES[stage]
        lax.fori_loop(first, last_, assemble, 0)
        products(stage)
        pair_copy(stage).start()

    def wide_start(stage):
        add_pair(stage)
        rings[stage][0].start()
        rings[stage][1].start()

    def wide_relay(stage):
        rings[stage][0].relay()
        rings[stage][1].relay()

    def wide_finish(stage):
        rings[stage][0].finish()
        rings[stage][2].start()
        rings[stage][1].finish()
        rings[stage][3].start()

    def thin_relay(stage):
        rings[stage][2].relay()
        rings[stage][3].relay()

    def thin_finish(stage):
        rings[stage][2].finish()
        rings[stage][3].finish()

    arrive(range(0, 5))
    ready(range(0, 5))
    build(0)
    wide_start(0)
    wide_relay(0)
    arrive(range(5, 7))
    wide_finish(0)
    ready(range(5, 7))
    build(1)
    thin_relay(0)
    wide_start(1)
    thin_finish(0)
    wide_relay(1)
    arrive(range(7, 8))
    wide_finish(1)
    ready(range(7, 8))
    build(2)
    thin_relay(1)
    wide_start(2)
    thin_finish(1)
    wide_relay(2)
    wide_finish(2)
    thin_relay(2)
    thin_finish(2)

    for i in range(8):
        for j in range(8):
            ZS[i, lax.rem(z + DZ[j], 8)] = M[base + block_of(i, j), ylo, xi, yhi]

    def z_copy(i):
        return pltpu.make_async_remote_copy(
            src_ref=ZS.at[i], dst_ref=ZR.at[i - 1],
            send_sem=zssem.at[i - 1], recv_sem=zrsem.at[i - 1],
            device_id={"band": ylo * 8 + lax.rem(z + DZ[i], 8)}, device_id_type=MESH)

    for i in range(7, 0, -1):
        z_copy(i).start()
    total = ZS[0]
    for i in range(1, 8):
        z_copy(i).wait_recv()
        total = total + ZR[i - 1]
    rows = pl.ds(pl.multiple_of(xi * 16 + yhi * 8, 8), 8)
    for j in range(4):
        lo, hi = merge(total[2 * j], total[2 * j + 1], low8)
        fin[c, rows, j * 128:(j + 1) * 128] = lo
        fin[c, rows, 512 + j * 128:512 + (j + 1) * 128] = hi

    def gather_copy(k):
        px, ph = lax.rem(xi + k // 2, 4), lax.rem(yhi + k, 2)
        return pltpu.make_async_remote_copy(
            src_ref=fin.at[c, rows], dst_ref=fin.at[c, rows],
            send_sem=fssem.at[k - 1], recv_sem=frsem.at[k - 1],
            device_id={"dom": px * 4 + ph * 2 + c}, device_id_type=MESH)

    def swap_copy(k):
        px, ph = lax.rem(xi - k // 2 + 4, 4), lax.rem(yhi + k, 2)
        part = fin.at[c, pl.ds(pl.multiple_of(px * 16 + ph * 8, 8), 8)]
        return pltpu.make_async_remote_copy(
            src_ref=part, dst_ref=part, send_sem=wssem.at[k], recv_sem=wrsem.at[k],
            device_id={"dom": other}, device_id_type=MESH)

    for k in (5, 4, 7, 6, 3, 2, 1):
        gather_copy(k).start()
    swap_copy(0).start()
    for k in range(1, 8):
        gather_copy(k).wait_recv()
        swap_copy(k).start()
    for k in range(8):
        swap_copy(k).wait_recv()
    ham[...] = fin[0]
    corr[...] = fin[1]

    for stage in range(3):
        pair_copy(stage).wait_send()
        for ring in rings[stage]:
            ring.wait_send()
    for k in range(1, 8):
        z_copy(k).wait_send()
        gather_copy(k).wait_send()
    for k in range(8):
        swap_copy(k).wait_send()
    for o in range(NB - 1):
        main_copy(o).wait_send()
        coef_copy(o).wait_send()
    for o in range(NB):
        x_copy(o).wait_send()


def on_device(wavefunctions, potential, projectors, hamiltonian_correction, delta_s, projector_count):
    vm = pl.BlockSpec(memory_space=pltpu.VMEM)
    hbm = pl.BlockSpec(memory_space=pl.ANY)
    dma = pltpu.SemaphoreType.DMA
    return pl.pallas_call(
        kernel,
        out_shape=(jax.ShapeDtypeStruct((64, 1024), F32), jax.ShapeDtypeStruct((64, 1024), F32)),
        in_specs=[hbm, vm, hbm, vm, vm, pl.BlockSpec(memory_space=pltpu.SMEM)],
        out_specs=(vm, vm),
        scratch_shapes=[
            pltpu.VMEM((4096, 128), F32),
            pltpu.VMEM((4608, 128), F32),
            pltpu.VMEM((128, 128), F32),
            pltpu.VMEM((128, 2, 4, 2, 8, 128), F32),
            pltpu.VMEM((129 * RPZ, 128), F32),
            pltpu.VMEM((NB, CHUNK, 128), F32),
            pltpu.VMEM((NB, CH, 8, 128), F32),
            pltpu.VMEM((NB, 16, 128), F32),
            pltpu.VMEM((NB, 16, 128), F32),
            pltpu.VMEM((CH, 2, RPZ, 128), F32),
            pltpu.VMEM((512, 128), F32),
            pltpu.VMEM((1024, 512), BF16),
            pltpu.VMEM((1024, 512), BF16),
            pltpu.VMEM((512, 2048), BF16),
            pltpu.VMEM((512, 2048), BF16),
            pltpu.VMEM((1024, 128), BF16),
            pltpu.VMEM((128, 2048), BF16),
            pltpu.VMEM((64, 2, 4, 2, 8, 128), F32),
            pltpu.VMEM((2, 64, 2, 8, 128), F32),
            pltpu.VMEM((2, 2, 64, 2, 8, 128), F32),
            pltpu.VMEM((64, 8, 128), F32),
            pltpu.VMEM((2, 64, 8, 128), F32),
            pltpu.VMEM((8, 8, 8, 128), F32),
            pltpu.VMEM((7, 8, 8, 128), F32),
            pltpu.VMEM((2, 64, 1024), F32),
            dma((2,)),
            dma((NB,)), dma((NB,)), dma((NB,)), dma((NB,)), dma((NB,)), dma((NB,)),
            dma((3,)), dma((3,)), dma((72,)), dma((72,)),
            dma((7,)), dma((7,)), dma((7,)), dma((7,)), dma((8,)), dma((8,)),
        ],
        compiler_params=pltpu.CompilerParams(
            collective_id=0, has_side_effects=True, vmem_limit_bytes=60 * 1024 * 1024),
    )(wavefunctions.reshape(4096, 128), potential.reshape(64, 128), projectors.reshape(72 * 64, 128),
      hamiltonian_correction, delta_s, projector_count)


def solution(mesh):
    placed = (
        P("band", "dom", None, None),
        P("dom", None, None),
        P("dom", None, None, None, None),
        P("dom", None, None),
        P("dom", None, None),
        P("dom"),
    )
    return jax.shard_map(
        on_device, mesh=mesh, in_specs=placed,
        out_specs=(P("band", None), P("band", None)), check_vma=False)
```

```python
import jax
import jax.numpy as jnp
from jax import lax
from jax.experimental import pallas as pl
from jax.experimental.pallas import tpu as pltpu
from jax.sharding import PartitionSpec as P

MESH = pl.DeviceIdType.MESH
F32 = jnp.float32
BF16 = jnp.bfloat16
NB = 16
ND = 16
CH = 8
RPZ = 32
CHUNK = (CH + 1) * RPZ
VOLUME = 1.0 / 131072.0
DZ = (0, 1, 7, 2, 6, 3, 5, 4)
OFFSETS = [(1, 0)] + [(dy, (8 - DZ[p]) % 8) for p in range(1, 8) for dy in (0, 1)]
STAGES = ((0, 5), (5, 7), (7, 8))
START = (0, 25, 49, 64)
HALF = (12, 12, 7)


def block_of(row, col):
    top = max(row, col)
    if top < 5:
        return col * 5 + row
    if top < 7:
        return 25 + col * 2 + row - 5 if col < 5 else 35 + (col - 5) * 7 + row
    return 49 + col if col < 7 else 56 + row


def split(x):
    hi = x.astype(BF16)
    return hi, (x - hi.astype(F32)).astype(BF16)


def dot(a, b):
    return lax.dot_general(a, b, (((1,), (0,)), ((), ())), preferred_element_type=F32)


def dot_exact(a, b):
    return lax.dot_general(a, b, (((1,), (0,)), ((), ())), precision=lax.Precision.HIGHEST,
                           preferred_element_type=F32)


def dot_nt(a, b):
    return lax.dot_general(a, b, (((1,), (1,)), ((), ())), preferred_element_type=F32)


def kernel(psi_in, pot, proj_in, hcor, dels, count, ham, corr,
           psi, proj, SP, M, T, R, RX, CS, CR, VB, AF, AThi, ATlo, Bhi, Blo, ATC, BC, PB,
           F1, F2, G1, G2, ZS, ZR, fin,
           lsem, ssem, rsem, cssem, crsem, xssem, xrsem, pssem, prsem, gssem, grsem,
           zssem, zrsem, fssem, frsem, wssem, wrsem):
    g = lax.axis_index("band")
    d = lax.axis_index("dom")
    ylo, z = g // 8, lax.rem(g, 8)
    xi, yhi, c = d // 4, lax.rem(d // 2, 2), lax.rem(d, 2)
    y = yhi * 2 + ylo
    dprev = lax.rem(d + ND - 1, ND)
    other = d + 1 - 2 * c

    def peer(o):
        dy, dz = OFFSETS[o]
        return lax.rem(ylo + dy, 2) * 8 + lax.rem(z + dz, 8)

    def source(o):
        dy, dz = OFFSETS[o]
        return lax.rem(ylo + dy, 2) * 8 + lax.rem(z - dz + 8, 8)

    def at_y(q):
        return {"band": lax.rem(q, 2) * 8 + z, "dom": xi * 4 + (q // 2) * 2 + c}

    def at_x(q):
        return {"dom": q * 4 + yhi * 2 + c}

    load_psi = pltpu.make_async_copy(psi_in, psi, lsem.at[0])
    load_proj = pltpu.make_async_copy(proj_in, proj, lsem.at[1])
    load_psi.start()
    load_proj.start()

    barrier = pltpu.get_barrier_semaphore()
    for o in range(NB - 1):
        pl.semaphore_signal(barrier, inc=1, device_id={"band": peer(o)}, device_id_type=MESH)
    for k in range(1, ND):
        pl.semaphore_signal(barrier, inc=1, device_id={"dom": lax.rem(d + k, ND)}, device_id_type=MESH)
    pl.semaphore_signal(barrier, inc=1, device_id={"band": (1 - ylo) * 8 + z, "dom": xi * 4 + (1 - yhi) * 2 + c},
                        device_id_type=MESH)

    load_psi.wait()
    for r in range(RPZ):
        xy = (r // 8) * 16 + r % 8
        a = psi[pl.ds(xy, 64, stride=64), :]
        b = psi[pl.ds(xy + 8, 64, stride=64), :]
        T[pl.ds(r, 128, stride=RPZ), :] = jnp.concatenate([a, b], axis=0).T
    T[pl.ds(128 * RPZ, RPZ), :] = T[pl.ds(0, RPZ), :]

    pl.semaphore_wait(barrier, 31)

    def main_copy(o):
        p = peer(o)
        return pltpu.make_async_remote_copy(
            src_ref=T.at[pl.ds(pl.multiple_of(p * (CH * RPZ), CH * RPZ), CHUNK)],
            dst_ref=R.at[g],
            send_sem=ssem.at[o], recv_sem=rsem.at[o],
            device_id={"band": p}, device_id_type=MESH)

    def coef_copy(o):
        p = peer(o)
        return pltpu.make_async_remote_copy(
            src_ref=CS.at[p], dst_ref=CR.at[g],
            send_sem=cssem.at[o], recv_sem=crsem.at[o],
            device_id={"band": p}, device_id_type=MESH)

    def x_copy(o):
        s = source(o) if o < NB - 1 else g
        return pltpu.make_async_remote_copy(
            src_ref=R.at[s].reshape(CH + 1, RPZ, 128).at[pl.ds(0, CH), pl.ds(0, 8)],
            dst_ref=RX.at[s],
            send_sem=xssem.at[o], recv_sem=xrsem.at[o],
            device_id={"dom": dprev}, device_id_type=MESH)

    for o in range(9):
        main_copy(o).start()

    R[g] = T[pl.ds(pl.multiple_of(g * (CH * RPZ), CH * RPZ), CHUNK), :]

    load_proj.wait()
    def project(t, acc):
        for x in range(4):
            xy = x * 16 + t
            p = jnp.concatenate([psi[pl.ds(xy, 64, stride=64), :], psi[pl.ds(xy + 8, 64, stride=64), :]], axis=1)
            q = jnp.concatenate([proj[pl.ds(xy, 72, stride=64), :], proj[pl.ds(xy + 8, 72, stride=64), :]], axis=1)
            phi, plo = split(p)
            qhi, qlo = split(q)
            acc = acc + dot_nt(qhi, phi) + dot_nt(qhi, plo) + dot_nt(qlo, phi)
        return acc

    acc = lax.fori_loop(0, 8, project, jnp.zeros((72, 64), F32))
    craw = jnp.concatenate([acc, jnp.zeros((56, 64), F32)], axis=0)
    x_copy(NB - 1).start()

    line = lax.broadcasted_iota(jnp.int32, (256, 128), 0)
    slot = lax.broadcasted_iota(jnp.int32, (256, 128), 1)
    spot = (line >> 4) * 5 + (line & 15)
    ext = jnp.where((line & 15) < 5, jnp.where(slot == spot, 1.0, 0.0), 0.0)
    srow = lax.broadcasted_iota(jnp.int32, (128, 128), 0)
    scol = lax.broadcasted_iota(jnp.int32, (128, 128), 1)
    SP[...] = jnp.zeros_like(SP)
    for t, ref in ((1, hcor), (2, dels)):
        inside = jnp.where((line & 15) >= 5 * t, jnp.where((line & 15) < 5 * t + 5, 1.0, 0.0), 0.0)

        for a in range(4):
            SP[t - 1, a, 0:18, 0:18] = ref[:, a, :]

        def couple(a, ext):
            s = SP[t - 1, a]
            s = (0.5 / VOLUME) * (s + s.T)
            used_col = jnp.clip(count[a] - slot, 0, 1).astype(F32)
            used_row = jnp.clip(count[a] - srow, 0, 1).astype(F32)
            left = jnp.where(spot - 5 * t == a * 18 + slot, used_col, 0.0) * inside
            right = jnp.where(scol == a * 18 + srow, used_row, 0.0)
            return ext + dot_exact(dot_exact(left, s), right)

        ext = lax.fori_loop(0, 4, couple, ext)
    chi, clo = split(craw)
    ehi, elo = split(ext)
    msg = dot(ehi, chi) + dot(ehi, clo) + dot(elo, chi)
    msg = jnp.concatenate([msg, msg], axis=1)
    CS[...] = msg.reshape(NB, 16, 128)
    CR[g] = CS[g]
    for o in range(NB - 1):
        coef_copy(o).start()

    v = 3.0 + pltpu.roll(pot[...], lax.rem(128 - g * CH, 128), 1)
    for zi in range(CH):
        wide = jnp.broadcast_to(v[:, zi:zi + 1], (64, 128))
        for half in range(2):
            for x in range(4):
                VB[zi, half, x * 8:(x + 1) * 8, :] = wide[x * 16 + half * 8:x * 16 + half * 8 + 8]

    low = lax.broadcasted_iota(jnp.int32, (RPZ, 128), 1) < 64
    low8 = lax.broadcasted_iota(jnp.int32, (8, 128), 1) < 64
    low16 = lax.broadcasted_iota(jnp.int32, (16, 128), 1) < 64
    last = lax.broadcasted_iota(jnp.int32, (8, 128), 0) == 7
    keep = lax.broadcasted_iota(jnp.int32, (16, 128), 0) < 5

    def merge(a, b, mask):
        return jnp.where(mask, a, pltpu.roll(b, 64, 1)), jnp.where(mask, pltpu.roll(a, 64, 1), b)

    def assemble(m, _):
        odd = lax.rem(m, 2)
        dz = odd * ((m + 1) // 2) + (1 - odd) * (8 - m // 2)
        s0 = lax.rem(z + dz, 8)
        s1 = s0 + 8
        rowsm = pl.ds(pl.multiple_of(m * 128, 128), 128)
        cols = pl.ds(pl.multiple_of(m * 256, 256), 128)
        cols2 = pl.ds(pl.multiple_of(m * 256 + 128, 128), 128)

        def column(zi):
            rows = pl.ds(zi * RPZ, RPZ)
            return merge(R[s0, rows, :], R[s1, rows, :], low)

        now = column(0)
        for zi in range(CH):
            nxt = column(zi + 1)
            halo = merge(RX[s0, zi], RX[s1, zi], low8)
            turned = []
            for half in range(2):
                turned.append([pltpu.roll(now[half][x * 8:(x + 1) * 8], 7, 0) for x in range(4)])
            for half in range(2):
                a = now[half]
                ax = jnp.concatenate([a[8:], halo[half]], axis=0)
                ay = jnp.concatenate(
                    [jnp.where(last, turned[1 - half][x], turned[half][x]) for x in range(4)], axis=0)
                h = VB[zi, half] * a - ax - ay - nxt[half]
                rows = pl.ds(half * 256 + zi * RPZ, RPZ)
                AF[rows, :] = a
                hi, lo = split(h)
                Bhi[rows, cols] = hi
                Blo[rows, cols] = lo
                hi, lo = split(a)
                Bhi[rows, cols2] = hi
                Blo[rows, cols2] = lo
            now = nxt
        hi, lo = split(AF[...].T)
        AThi[rowsm, :] = hi
        ATlo[rowsm, :] = lo
        cc, _ = merge(CR[s0], CR[s1], low16)
        chi, clo = split(cc)
        chi, clo = chi.astype(F32), clo.astype(F32)
        zero = jnp.zeros((16, 128), F32)
        pad = jnp.zeros((80, 128), F32)
        ahi = jnp.where(keep, chi, zero)
        alo = jnp.where(keep, clo, zero)
        ATC[rowsm, :] = jnp.concatenate([ahi, ahi, alo, pad], axis=0).T.astype(BF16)
        for t, at in ((1, cols), (2, cols2)):
            bhi = jnp.where(keep, pltpu.roll(chi, 16 - 5 * t, 0), zero)
            blo = jnp.where(keep, pltpu.roll(clo, 16 - 5 * t, 0), zero)
            BC[:, at] = jnp.concatenate([bhi, blo, bhi, pad], axis=0).astype(BF16)
        return 0

    def product(first, n, col, at):
        rows = pl.ds(pl.multiple_of(first * 128, 128), n * 128)
        cols = pl.ds(pl.multiple_of(col * 256, 256), 256)
        a = AThi[rows, :]
        res = dot(a, Bhi[:, cols]) + dot(a, Blo[:, cols]) + dot(ATlo[rows, :], Bhi[:, cols]) \
            + dot(ATC[rows, :], BC[:, cols])
        res = res * VOLUME
        for r in range(n):
            for mat in range(2):
                M[mat * 64 + at + r] = res[r * 128:(r + 1) * 128, mat * 128:(mat + 1) * 128].reshape(2, 4, 2, 8, 128)

    def loop(count_, body):
        def step(t, _):
            body(t)
            return 0
        lax.fori_loop(0, count_, step, 0)

    def even(k, l):
        s = 0.5 * (M[k].reshape(128, 128) + M[l].reshape(128, 128).T)
        M[k] = s.reshape(2, 4, 2, 8, 128)
        M[l] = s.T.reshape(2, 4, 2, 8, 128)

    def products(stage):
        if stage == 0:
            loop(5, lambda t: product(0, 2, t, t * 5))
            loop(5, lambda t: product(2, 2, t, t * 5 + 2))
            loop(5, lambda t: product(4, 1, t, t * 5 + 4))

            def pair(t):
                i, j = t // 5, lax.rem(t, 5)

                @pl.when(i <= j)
                def _():
                    even(j * 5 + i, i * 5 + j)
            loop(25, pair)
        elif stage == 1:
            loop(5, lambda t: product(5, 2, t, 25 + t * 2))
            for i in range(3):
                loop(2, lambda t: product(2 * i, 2, 5 + t, 35 + t * 7 + 2 * i))
            loop(2, lambda t: product(6, 1, 5 + t, 35 + t * 7 + 6))
            loop(10, lambda t: even(35 + (t // 5) * 7 + lax.rem(t, 5), 25 + lax.rem(t, 5) * 2 + t // 5))
            for i, j in ((5, 5), (5, 6), (6, 6)):
                even(block_of(i, j), block_of(j, i))
        else:
            loop(7, lambda t: product(7, 1, t, 49 + t))
            loop(4, lambda t: product(2 * t, 2, 7, 56 + 2 * t))
            loop(7, lambda t: even(56 + t, 49 + t))
            even(63, 63)

    def pair_copy(stage):
        k0, n = START[stage], START[stage + 1] - START[stage]
        return pltpu.make_async_remote_copy(
            src_ref=M.at[pl.ds((1 - c) * 64 + k0, n)], dst_ref=PB.at[pl.ds(k0, n)],
            send_sem=pssem.at[stage], recv_sem=prsem.at[stage],
            device_id={"dom": other}, device_id_type=MESH)

    base = c * 64

    def add_pair(stage):
        pair_copy(stage).wait_recv()

        def body(t):
            M[base + START[stage] + t] = M[base + START[stage] + t] + PB[START[stage] + t]
        loop(START[stage + 1] - START[stage], body)

    class Ring:
        def __init__(self, me, at, piece, first, second, number):
            self.me, self.piece, self.first, self.second = me, piece, first, second
            self.plus, self.minus = at(lax.rem(me + 1, 4)), at(lax.rem(me + 3, 4))
            self.number = number

        def copy(self, k):
            me = self.me
            q, h, buf, way = (
                (me + 2, 0, self.first(0), self.plus),
                (me + 2, 1, self.first(1), self.minus),
                (me + 1, 1, self.second(0, 1), self.plus),
                (me + 3, 0, self.second(1, 0), self.minus),
                (me + 1, 0, self.second(0, 0), self.plus),
                (me + 3, 1, self.second(1, 1), self.minus),
            )[k]
            return pltpu.make_async_remote_copy(
                src_ref=M.at[self.piece(lax.rem(q, 4), h)], dst_ref=buf,
                send_sem=gssem.at[self.number + k], recv_sem=grsem.at[self.number + k],
                device_id=way, device_id_type=MESH)

        def start(self):
            for k in range(4):
                self.copy(k).start()

        def add(self, q, h, *bufs):
            at = self.piece(lax.rem(q, 4), h)
            total = M[at]
            for b in bufs:
                total = total + b[...]
            M[at] = total

        def relay(self):
            self.copy(0).wait_recv()
            self.add(self.me + 1, 0, self.first(0))
            self.copy(4).start()
            self.copy(1).wait_recv()
            self.add(self.me + 3, 1, self.first(1))
            self.copy(5).start()

        def finish(self):
            for k in range(2, 6):
                self.copy(k).wait_recv()
            for h in range(2):
                self.add(self.me, h, self.second(0, h), self.second(1, h))

        def wait_send(self):
            for k in range(6):
                self.copy(k).wait_send()

    rings = []
    full = slice(None)
    for stage in range(3):
        k0, n = START[stage], START[stage + 1] - START[stage]
        na = HALF[stage]
        nb = n - na
        kb = k0 + na
        ha = (na // 2, na - na // 2)
        hb = (nb // 2, nb - nb // 2)

        def ax_piece(q, h, k0=k0, na=na):
            return (pl.ds(base + k0, na), h, q)

        def by_piece(q, h, kb=kb, nb=nb):
            return (pl.ds(base + kb, nb), lax.rem(q, 2), pl.ds(2 * h, 2), q // 2)

        def ay_piece(q, h, k0=k0, ha=ha):
            return (pl.ds(base + k0 + h * ha[0], ha[h]), lax.rem(q, 2), xi, q // 2)

        def bx_piece(q, h, kb=kb, hb=hb):
            return (pl.ds(base + kb + h * hb[0], hb[h]), ylo, q, yhi)

        def wide_first(k, n):
            return lambda h: F1.at[h, pl.ds(k, n)]

        def wide_second(k, n):
            return lambda w, h: F2.at[w, h, pl.ds(k, n)]

        def thin_first(k, hs):
            return lambda h: G1.at[pl.ds(k + h * hs[0], hs[h])]

        def thin_second(k, hs):
            return lambda w, h: G2.at[w, pl.ds(k + h * hs[0], hs[h])]

        rings.append((
            Ring(xi, at_x, ax_piece, wide_first(k0, na), wide_second(k0, na), stage * 24),
            Ring(y, at_y, by_piece, wide_first(kb, nb), wide_second(kb, nb), stage * 24 + 6),
            Ring(y, at_y, ay_piece, thin_first(k0, ha), thin_second(k0, ha), stage * 24 + 12),
            Ring(xi, at_x, bx_piece, thin_first(kb, hb), thin_second(kb, hb), stage * 24 + 18),
        ))

    def arrive(positions):
        for p in positions:
            for o in ((0,) if p == 0 else (2 * p - 1, 2 * p)):
                main_copy(o).wait_recv()
                x_copy(o).start()

    def ready(positions):
        for p in positions:
            for o in ((0, NB - 1) if p == 0 else (2 * p - 1, 2 * p)):
                x_copy(o).wait_recv()
                if o < NB - 1:
                    coef_copy(o).wait_recv()

    def build(stage):
        first, last_ = STAGES[stage]
        lax.fori_loop(first, last_, assemble, 0)
        products(stage)
        pair_copy(stage).start()

    def wide_start(stage):
        add_pair(stage)
        rings[stage][0].start()
        rings[stage][1].start()

    def wide_relay(stage):
        rings[stage][0].relay()
        rings[stage][1].relay()

    def wide_finish(stage):
        rings[stage][0].finish()
        rings[stage][2].start()
        rings[stage][1].finish()
        rings[stage][3].start()

    def thin_relay(stage):
        rings[stage][2].relay()
        rings[stage][3].relay()

    def thin_finish(stage):
        rings[stage][2].finish()
        rings[stage][3].finish()

    arrive(range(0, 4))
    for o in range(9, 13):
        main_copy(o).start()
    arrive(range(4, 5))
    ready(range(0, 5))
    build(0)
    wide_start(0)
    wide_relay(0)
    arrive(range(5, 6))
    for o in range(13, 15):
        main_copy(o).start()
    arrive(range(6, 7))
    wide_finish(0)
    ready(range(5, 7))
    build(1)
    thin_relay(0)
    wide_start(1)
    thin_finish(0)
    wide_relay(1)
    arrive(range(7, 8))
    wide_finish(1)
    ready(range(7, 8))
    build(2)
    thin_relay(1)
    wide_start(2)
    thin_finish(1)
    wide_relay(2)
    wide_finish(2)
    thin_relay(2)
    thin_finish(2)

    for i in range(8):
        for j in range(8):
            ZS[i, lax.rem(z + DZ[j], 8)] = M[base + block_of(i, j), ylo, xi, yhi]

    def z_copy(i):
        return pltpu.make_async_remote_copy(
            src_ref=ZS.at[i], dst_ref=ZR.at[i - 1],
            send_sem=zssem.at[i - 1], recv_sem=zrsem.at[i - 1],
            device_id={"band": ylo * 8 + lax.rem(z + DZ[i], 8)}, device_id_type=MESH)

    for i in range(7, 0, -1):
        z_copy(i).start()
    total = ZS[0]
    for i in range(1, 8):
        z_copy(i).wait_recv()
        total = total + ZR[i - 1]
    rows = pl.ds(pl.multiple_of(xi * 16 + yhi * 8, 8), 8)
    for j in range(4):
        lo, hi = merge(total[2 * j], total[2 * j + 1], low8)
        fin[c, rows, j * 128:(j + 1) * 128] = lo
        fin[c, rows, 512 + j * 128:512 + (j + 1) * 128] = hi

    def gather_copy(k):
        px, ph = lax.rem(xi + k // 2, 4), lax.rem(yhi + k, 2)
        return pltpu.make_async_remote_copy(
            src_ref=fin.at[c, rows], dst_ref=fin.at[c, rows],
            send_sem=fssem.at[k - 1], recv_sem=frsem.at[k - 1],
            device_id={"dom": px * 4 + ph * 2 + c}, device_id_type=MESH)

    def swap_copy(k):
        px, ph = lax.rem(xi - k // 2 + 4, 4), lax.rem(yhi + k, 2)
        part = fin.at[c, pl.ds(pl.multiple_of(px * 16 + ph * 8, 8), 8)]
        return pltpu.make_async_remote_copy(
            src_ref=part, dst_ref=part, send_sem=wssem.at[k], recv_sem=wrsem.at[k],
            device_id={"dom": other}, device_id_type=MESH)

    for k in (5, 4, 7, 6, 3, 2, 1):
        gather_copy(k).start()
    swap_copy(0).start()
    for k in range(1, 8):
        gather_copy(k).wait_recv()
        swap_copy(k).start()
    for k in range(8):
        swap_copy(k).wait_recv()
    ham[...] = fin[0]
    corr[...] = fin[1]

    for stage in range(3):
        pair_copy(stage).wait_send()
        for ring in rings[stage]:
            ring.wait_send()
    for k in range(1, 8):
        z_copy(k).wait_send()
        gather_copy(k).wait_send()
    for k in range(8):
        swap_copy(k).wait_send()
    for o in range(NB - 1):
        main_copy(o).wait_send()
        coef_copy(o).wait_send()
    for o in range(NB):
        x_copy(o).wait_send()


def on_device(wavefunctions, potential, projectors, hamiltonian_correction, delta_s, projector_count):
    vm = pl.BlockSpec(memory_space=pltpu.VMEM)
    hbm = pl.BlockSpec(memory_space=pl.ANY)
    dma = pltpu.SemaphoreType.DMA
    return pl.pallas_call(
        kernel,
        out_shape=(jax.ShapeDtypeStruct((64, 1024), F32), jax.ShapeDtypeStruct((64, 1024), F32)),
        in_specs=[hbm, vm, hbm, vm, vm, pl.BlockSpec(memory_space=pltpu.SMEM)],
        out_specs=(vm, vm),
        scratch_shapes=[
            pltpu.VMEM((4096, 128), F32),
            pltpu.VMEM((4608, 128), F32),
            pltpu.VMEM((2, 4, 128, 128), F32),
            pltpu.VMEM((128, 2, 4, 2, 8, 128), F32),
            pltpu.VMEM((129 * RPZ, 128), F32),
            pltpu.VMEM((NB, CHUNK, 128), F32),
            pltpu.VMEM((NB, CH, 8, 128), F32),
            pltpu.VMEM((NB, 16, 128), F32),
            pltpu.VMEM((NB, 16, 128), F32),
            pltpu.VMEM((CH, 2, RPZ, 128), F32),
            pltpu.VMEM((512, 128), F32),
            pltpu.VMEM((1024, 512), BF16),
            pltpu.VMEM((1024, 512), BF16),
            pltpu.VMEM((512, 2048), BF16),
            pltpu.VMEM((512, 2048), BF16),
            pltpu.VMEM((1024, 128), BF16),
            pltpu.VMEM((128, 2048), BF16),
            pltpu.VMEM((64, 2, 4, 2, 8, 128), F32),
            pltpu.VMEM((2, 64, 2, 8, 128), F32),
            pltpu.VMEM((2, 2, 64, 2, 8, 128), F32),
            pltpu.VMEM((64, 8, 128), F32),
            pltpu.VMEM((2, 64, 8, 128), F32),
            pltpu.VMEM((8, 8, 8, 128), F32),
            pltpu.VMEM((7, 8, 8, 128), F32),
            pltpu.VMEM((2, 64, 1024), F32),
            dma((2,)),
            dma((NB,)), dma((NB,)), dma((NB,)), dma((NB,)), dma((NB,)), dma((NB,)),
            dma((3,)), dma((3,)), dma((72,)), dma((72,)),
            dma((7,)), dma((7,)), dma((7,)), dma((7,)), dma((8,)), dma((8,)),
        ],
        compiler_params=pltpu.CompilerParams(
            collective_id=0, has_side_effects=True, vmem_limit_bytes=60 * 1024 * 1024),
    )(wavefunctions.reshape(4096, 128), potential.reshape(64, 128), projectors.reshape(72 * 64, 128),
      jnp.swapaxes(hamiltonian_correction, 0, 1), jnp.swapaxes(delta_s, 0, 1), projector_count)


def solution(mesh):
    placed = (
        P("band", "dom", None, None),
        P("dom", None, None),
        P("dom", None, None, None, None),
        P("dom", None, None),
        P("dom", None, None),
        P("dom"),
    )
    return jax.shard_map(
        on_device, mesh=mesh, in_specs=placed,
        out_specs=(P("band", None), P("band", None)), check_vma=False)
```

```python
import jax
import jax.numpy as jnp
from jax import lax
from jax.experimental import pallas as pl
from jax.experimental.pallas import tpu as pltpu
from jax.sharding import PartitionSpec as P

MESH = pl.DeviceIdType.MESH
F32 = jnp.float32
BF16 = jnp.bfloat16
NB = 16
ND = 16
CH = 8
RPZ = 32
CHUNK = (CH + 1) * RPZ
VOLUME = 1.0 / 131072.0
DZ = (0, 1, 7, 2, 6, 3, 5, 4)
OFFSETS = [(1, 0)] + [(dy, (8 - DZ[p]) % 8) for p in range(1, 8) for dy in (0, 1)]
STAGES = ((0, 5), (5, 7), (7, 8))
START = (0, 25, 49, 64)
HALF = (12, 12, 7)


def block_of(row, col):
    top = max(row, col)
    if top < 5:
        return col * 5 + row
    if top < 7:
        return 25 + col * 2 + row - 5 if col < 5 else 35 + (col - 5) * 7 + row
    return 49 + col if col < 7 else 56 + row


def split(x):
    hi = x.astype(BF16)
    return hi, (x - hi.astype(F32)).astype(BF16)


def dot(a, b):
    return lax.dot_general(a, b, (((1,), (0,)), ((), ())), preferred_element_type=F32)


def dot_exact(a, b):
    return lax.dot_general(a, b, (((1,), (0,)), ((), ())), precision=lax.Precision.HIGHEST,
                           preferred_element_type=F32)


def dot_nt(a, b):
    return lax.dot_general(a, b, (((1,), (1,)), ((), ())), preferred_element_type=F32)


def kernel(psi_in, pot, proj_in, hcor, dels, count, fin,
           psi, proj, SP, M, T, R, RX, CS, CR, VB, AF, AThi, ATlo, Bhi, Blo, ATC, BC, PB,
           F1, F2, FX, FY, G2, ZS, ZR, TOT,
           lsem, ssem, rsem, cssem, crsem, xssem, xrsem, pssem, prsem, gssem, grsem,
           zssem, zrsem, fssem, frsem, wssem, wrsem):
    g = lax.axis_index("band")
    d = lax.axis_index("dom")
    ylo, z = g // 8, lax.rem(g, 8)
    xi, yhi, c = d // 4, lax.rem(d // 2, 2), lax.rem(d, 2)
    y = yhi * 2 + ylo
    dprev = lax.rem(d + ND - 1, ND)
    other = d + 1 - 2 * c

    def peer(o):
        dy, dz = OFFSETS[o]
        return lax.rem(ylo + dy, 2) * 8 + lax.rem(z + dz, 8)

    def source(o):
        dy, dz = OFFSETS[o]
        return lax.rem(ylo + dy, 2) * 8 + lax.rem(z - dz + 8, 8)

    def at_y(q):
        return {"band": lax.rem(q, 2) * 8 + z, "dom": xi * 4 + (q // 2) * 2 + c}

    def at_x(q):
        return {"dom": q * 4 + yhi * 2 + c}

    load_psi = pltpu.make_async_copy(psi_in, psi, lsem.at[0])
    load_proj = pltpu.make_async_copy(proj_in, proj, lsem.at[1])
    load_psi.start()
    load_proj.start()

    barrier = pltpu.get_barrier_semaphore()
    for o in range(NB - 1):
        pl.semaphore_signal(barrier, inc=1, device_id={"band": peer(o)}, device_id_type=MESH)
    for k in range(1, ND):
        pl.semaphore_signal(barrier, inc=1, device_id={"dom": lax.rem(d + k, ND)}, device_id_type=MESH)
    pl.semaphore_signal(barrier, inc=1, device_id={"band": (1 - ylo) * 8 + z, "dom": xi * 4 + (1 - yhi) * 2 + c},
                        device_id_type=MESH)

    load_psi.wait()
    for r in range(RPZ):
        xy = (r // 8) * 16 + r % 8
        a = psi[pl.ds(xy, 64, stride=64), :]
        b = psi[pl.ds(xy + 8, 64, stride=64), :]
        T[pl.ds(r, 128, stride=RPZ), :] = jnp.concatenate([a, b], axis=0).T
    T[pl.ds(128 * RPZ, RPZ), :] = T[pl.ds(0, RPZ), :]

    pl.semaphore_wait(barrier, 31)

    def main_copy(o):
        p = peer(o)
        return pltpu.make_async_remote_copy(
            src_ref=T.at[pl.ds(pl.multiple_of(p * (CH * RPZ), CH * RPZ), CHUNK)],
            dst_ref=R.at[g],
            send_sem=ssem.at[o], recv_sem=rsem.at[o],
            device_id={"band": p}, device_id_type=MESH)

    def coef_copy(o):
        p = peer(o)
        return pltpu.make_async_remote_copy(
            src_ref=CS.at[p], dst_ref=CR.at[g],
            send_sem=cssem.at[o], recv_sem=crsem.at[o],
            device_id={"band": p}, device_id_type=MESH)

    def x_copy(o):
        s = source(o) if o < NB - 1 else g
        return pltpu.make_async_remote_copy(
            src_ref=R.at[s].reshape(CH + 1, RPZ, 128).at[pl.ds(0, CH), pl.ds(0, 8)],
            dst_ref=RX.at[s],
            send_sem=xssem.at[o], recv_sem=xrsem.at[o],
            device_id={"dom": dprev}, device_id_type=MESH)

    for o in range(9):
        main_copy(o).start()

    R[g] = T[pl.ds(pl.multiple_of(g * (CH * RPZ), CH * RPZ), CHUNK), :]

    load_proj.wait()
    def project(t, acc):
        for x in range(4):
            xy = x * 16 + t
            p = jnp.concatenate([psi[pl.ds(xy, 64, stride=64), :], psi[pl.ds(xy + 8, 64, stride=64), :]], axis=1)
            q = jnp.concatenate([proj[pl.ds(xy, 72, stride=64), :], proj[pl.ds(xy + 8, 72, stride=64), :]], axis=1)
            phi, plo = split(p)
            qhi, qlo = split(q)
            acc = acc + dot_nt(qhi, phi) + dot_nt(qhi, plo) + dot_nt(qlo, phi)
        return acc

    acc = lax.fori_loop(0, 8, project, jnp.zeros((72, 64), F32))
    craw = jnp.concatenate([acc, jnp.zeros((56, 64), F32)], axis=0)
    x_copy(NB - 1).start()

    line = lax.broadcasted_iota(jnp.int32, (256, 128), 0)
    slot = lax.broadcasted_iota(jnp.int32, (256, 128), 1)
    spot = (line >> 4) * 5 + (line & 15)
    ext = jnp.where((line & 15) < 5, jnp.where(slot == spot, 1.0, 0.0), 0.0)
    srow = lax.broadcasted_iota(jnp.int32, (128, 128), 0)
    scol = lax.broadcasted_iota(jnp.int32, (128, 128), 1)
    SP[...] = jnp.zeros_like(SP)
    for t, ref in ((1, hcor), (2, dels)):
        inside = jnp.where((line & 15) >= 5 * t, jnp.where((line & 15) < 5 * t + 5, 1.0, 0.0), 0.0)

        for a in range(4):
            SP[t - 1, a, 0:18, 0:18] = ref[:, a, :]

        def couple(a, ext):
            s = SP[t - 1, a]
            s = (0.5 / VOLUME) * (s + s.T)
            used_col = jnp.clip(count[a] - slot, 0, 1).astype(F32)
            used_row = jnp.clip(count[a] - srow, 0, 1).astype(F32)
            left = jnp.where(spot - 5 * t == a * 18 + slot, used_col, 0.0) * inside
            right = jnp.where(scol == a * 18 + srow, used_row, 0.0)
            return ext + dot_exact(dot_exact(left, s), right)

        ext = lax.fori_loop(0, 4, couple, ext)
    chi, clo = split(craw)
    ehi, elo = split(ext)
    msg = dot(ehi, chi) + dot(ehi, clo) + dot(elo, chi)
    msg = jnp.concatenate([msg, msg], axis=1)
    CS[...] = msg.reshape(NB, 16, 128)
    CR[g] = CS[g]
    for o in range(NB - 1):
        coef_copy(o).start()

    v = 3.0 + pltpu.roll(pot[...], lax.rem(128 - g * CH, 128), 1)
    for zi in range(CH):
        wide = jnp.broadcast_to(v[:, zi:zi + 1], (64, 128))
        for half in range(2):
            for x in range(4):
                VB[zi, half, x * 8:(x + 1) * 8, :] = wide[x * 16 + half * 8:x * 16 + half * 8 + 8]

    low = lax.broadcasted_iota(jnp.int32, (RPZ, 128), 1) < 64
    low8 = lax.broadcasted_iota(jnp.int32, (8, 128), 1) < 64
    low16 = lax.broadcasted_iota(jnp.int32, (16, 128), 1) < 64
    last = lax.broadcasted_iota(jnp.int32, (8, 128), 0) == 7
    keep = lax.broadcasted_iota(jnp.int32, (16, 128), 0) < 5

    def merge(a, b, mask):
        return jnp.where(mask, a, pltpu.roll(b, 64, 1)), jnp.where(mask, pltpu.roll(a, 64, 1), b)

    def assemble(m, _):
        odd = lax.rem(m, 2)
        dz = odd * ((m + 1) // 2) + (1 - odd) * (8 - m // 2)
        s0 = lax.rem(z + dz, 8)
        s1 = s0 + 8
        rowsm = pl.ds(pl.multiple_of(m * 128, 128), 128)
        cols = pl.ds(pl.multiple_of(m * 256, 256), 128)
        cols2 = pl.ds(pl.multiple_of(m * 256 + 128, 128), 128)

        def column(zi):
            rows = pl.ds(zi * RPZ, RPZ)
            return merge(R[s0, rows, :], R[s1, rows, :], low)

        now = column(0)
        for zi in range(CH):
            nxt = column(zi + 1)
            halo = merge(RX[s0, zi], RX[s1, zi], low8)
            turned = []
            for half in range(2):
                turned.append([pltpu.roll(now[half][x * 8:(x + 1) * 8], 7, 0) for x in range(4)])
            for half in range(2):
                a = now[half]
                ax = jnp.concatenate([a[8:], halo[half]], axis=0)
                ay = jnp.concatenate(
                    [jnp.where(last, turned[1 - half][x], turned[half][x]) for x in range(4)], axis=0)
                h = VB[zi, half] * a - ax - ay - nxt[half]
                rows = pl.ds(half * 256 + zi * RPZ, RPZ)
                AF[rows, :] = a
                hi, lo = split(h)
                Bhi[rows, cols] = hi
                Blo[rows, cols] = lo
                hi, lo = split(a)
                Bhi[rows, cols2] = hi
                Blo[rows, cols2] = lo
            now = nxt
        hi, lo = split(AF[...].T)
        AThi[rowsm, :] = hi
        ATlo[rowsm, :] = lo
        cc, _ = merge(CR[s0], CR[s1], low16)
        chi, clo = split(cc)
        chi, clo = chi.astype(F32), clo.astype(F32)
        zero = jnp.zeros((16, 128), F32)
        pad = jnp.zeros((80, 128), F32)
        ahi = jnp.where(keep, chi, zero)
        alo = jnp.where(keep, clo, zero)
        ATC[rowsm, :] = jnp.concatenate([ahi, ahi, alo, pad], axis=0).T.astype(BF16)
        for t, at in ((1, cols), (2, cols2)):
            bhi = jnp.where(keep, pltpu.roll(chi, 16 - 5 * t, 0), zero)
            blo = jnp.where(keep, pltpu.roll(clo, 16 - 5 * t, 0), zero)
            BC[:, at] = jnp.concatenate([bhi, blo, bhi, pad], axis=0).astype(BF16)
        return 0

    def product(first, n, col, at):
        rows = pl.ds(pl.multiple_of(first * 128, 128), n * 128)
        cols = pl.ds(pl.multiple_of(col * 256, 256), 256)
        a = AThi[rows, :]
        res = dot(a, Bhi[:, cols]) + dot(a, Blo[:, cols]) + dot(ATlo[rows, :], Bhi[:, cols]) \
            + dot(ATC[rows, :], BC[:, cols])
        res = res * VOLUME
        for r in range(n):
            for mat in range(2):
                M[mat * 64 + at + r] = res[r * 128:(r + 1) * 128, mat * 128:(mat + 1) * 128].reshape(2, 4, 2, 8, 128)

    def loop(count_, body):
        def step(t, _):
            body(t)
            return 0
        lax.fori_loop(0, count_, step, 0)

    def even(k, l):
        s = 0.5 * (M[k].reshape(128, 128) + M[l].reshape(128, 128).T)
        M[k] = s.reshape(2, 4, 2, 8, 128)
        M[l] = s.T.reshape(2, 4, 2, 8, 128)

    def products(stage):
        if stage == 0:
            loop(5, lambda t: product(0, 2, t, t * 5))
            loop(5, lambda t: product(2, 2, t, t * 5 + 2))
            loop(5, lambda t: product(4, 1, t, t * 5 + 4))

            def pair(t):
                i, j = t // 5, lax.rem(t, 5)

                @pl.when(i <= j)
                def _():
                    even(j * 5 + i, i * 5 + j)
            loop(25, pair)
        elif stage == 1:
            loop(5, lambda t: product(5, 2, t, 25 + t * 2))
            for i in range(3):
                loop(2, lambda t: product(2 * i, 2, 5 + t, 35 + t * 7 + 2 * i))
            loop(2, lambda t: product(6, 1, 5 + t, 35 + t * 7 + 6))
            loop(10, lambda t: even(35 + (t // 5) * 7 + lax.rem(t, 5), 25 + lax.rem(t, 5) * 2 + t // 5))
            for i, j in ((5, 5), (5, 6), (6, 6)):
                even(block_of(i, j), block_of(j, i))
        else:
            loop(7, lambda t: product(7, 1, t, 49 + t))
            loop(4, lambda t: product(2 * t, 2, 7, 56 + 2 * t))
            loop(7, lambda t: even(56 + t, 49 + t))
            even(63, 63)

    def pair_copy(stage):
        k0, n = START[stage], START[stage + 1] - START[stage]
        return pltpu.make_async_remote_copy(
            src_ref=M.at[pl.ds((1 - c) * 64 + k0, n)], dst_ref=PB.at[pl.ds(k0, n)],
            send_sem=pssem.at[stage], recv_sem=prsem.at[stage],
            device_id={"dom": other}, device_id_type=MESH)

    base = c * 64

    def add_pair(stage):
        pair_copy(stage).wait_recv()

        def body(t):
            M[base + START[stage] + t] = M[base + START[stage] + t] + PB[START[stage] + t]
        loop(START[stage + 1] - START[stage], body)

    class Ring:
        def __init__(self, me, at, piece, first, second, number):
            self.me, self.piece, self.first, self.second = me, piece, first, second
            self.plus, self.minus = at(lax.rem(me + 1, 4)), at(lax.rem(me + 3, 4))
            self.number = number

        def copy(self, k):
            me = self.me
            q, h, buf, way = (
                (me + 2, 0, self.first(0), self.plus),
                (me + 2, 1, self.first(1), self.minus),
                (me + 1, 1, self.second(0, 1), self.plus),
                (me + 3, 0, self.second(1, 0), self.minus),
                (me + 1, 0, self.second(0, 0), self.plus),
                (me + 3, 1, self.second(1, 1), self.minus),
            )[k]
            return pltpu.make_async_remote_copy(
                src_ref=M.at[self.piece(lax.rem(q, 4), h)], dst_ref=buf,
                send_sem=gssem.at[self.number + k], recv_sem=grsem.at[self.number + k],
                device_id=way, device_id_type=MESH)

        def start(self):
            for k in range(4):
                self.copy(k).start()

        def add(self, q, h, *bufs):
            at = self.piece(lax.rem(q, 4), h)
            total = M[at]
            for b in bufs:
                total = total + b[...]
            M[at] = total

        def relay(self):
            self.copy(0).wait_recv()
            self.add(self.me + 1, 0, self.first(0))
            self.copy(4).start()
            self.copy(1).wait_recv()
            self.add(self.me + 3, 1, self.first(1))
            self.copy(5).start()

        def finish(self):
            for k in range(2, 6):
                self.copy(k).wait_recv()
            for h in range(2):
                self.add(self.me, h, self.second(0, h), self.second(1, h))

        def wait_send(self):
            for k in range(6):
                self.copy(k).wait_send()

    class Direct:
        def __init__(self, me, at, piece, buf, number):
            self.me, self.at, self.piece, self.buf, self.number = me, at, piece, buf, number

        def copy(self, k):
            q = lax.rem(self.me + k, 4)
            return pltpu.make_async_remote_copy(
                src_ref=M.at[self.piece(q)], dst_ref=self.buf(k - 1),
                send_sem=gssem.at[self.number + k - 1], recv_sem=grsem.at[self.number + k - 1],
                device_id=self.at(q), device_id_type=MESH)

        def start(self):
            for k in (2, 1, 3):
                self.copy(k).start()

        def finish(self):
            at = self.piece(self.me)
            total = M[at]
            for k in (1, 3, 2):
                self.copy(k).wait_recv()
                total = total + self.buf(k - 1)[...]
            M[at] = total

        def wait_send(self):
            for k in range(1, 4):
                self.copy(k).wait_send()

    rings = []
    full = slice(None)
    for stage in range(3):
        k0, n = START[stage], START[stage + 1] - START[stage]
        na = HALF[stage]
        nb = n - na
        kb = k0 + na

        def ax_piece(q, h, k0=k0, na=na):
            return (pl.ds(base + k0, na), h, q)

        def by_piece(q, h, kb=kb, nb=nb):
            return (pl.ds(base + kb, nb), lax.rem(q, 2), pl.ds(2 * h, 2), q // 2)

        def ax_whole(q, k0=k0, na=na):
            return (pl.ds(base + k0, na), full, q)

        def by_whole(q, kb=kb, nb=nb):
            return (pl.ds(base + kb, nb), lax.rem(q, 2), full, q // 2)

        def ay_piece(q, k0=k0, na=na):
            return (pl.ds(base + k0, na), lax.rem(q, 2), xi, q // 2)

        def bx_piece(q, kb=kb, nb=nb):
            return (pl.ds(base + kb, nb), ylo, q, yhi)

        def wide_first(k, n):
            return lambda h: F1.at[h, pl.ds(k, n)]

        def wide_second(k, n):
            return lambda w, h: F2.at[w, h, pl.ds(k, n)]

        def thin(k, n):
            return lambda i: G2.at[i, pl.ds(k, n)]

        number = stage * 24
        if stage < 2:
            wide = (Ring(xi, at_x, ax_piece, wide_first(k0, na), wide_second(k0, na), number),
                    Ring(y, at_y, by_piece, wide_first(kb, nb), wide_second(kb, nb), number + 6))
        else:
            wide = (Direct(xi, at_x, ax_whole, lambda i: FX.at[i], number),
                    Direct(y, at_y, by_whole, lambda i: FY.at[i], number + 6))
        rings.append(wide + (
            Direct(y, at_y, ay_piece, thin(k0, na), number + 12),
            Direct(xi, at_x, bx_piece, thin(kb, nb), number + 18),
        ))

    def arrive(*offsets):
        for o in offsets:
            main_copy(o).wait_recv()
            x_copy(o).start()

    def ready(positions):
        for p in positions:
            for o in ((0, NB - 1) if p == 0 else (2 * p - 1, 2 * p)):
                x_copy(o).wait_recv()
                if o < NB - 1:
                    coef_copy(o).wait_recv()

    def build(stage):
        first, last_ = STAGES[stage]
        lax.fori_loop(first, last_, assemble, 0)
        products(stage)
        pair_copy(stage).start()

    def wide_start(stage):
        add_pair(stage)
        rings[stage][0].start()
        rings[stage][1].start()

    def wide_relay(stage):
        rings[stage][0].relay()
        rings[stage][1].relay()

    def wide_finish(stage):
        rings[stage][0].finish()
        rings[stage][2].start()
        rings[stage][1].finish()
        rings[stage][3].start()

    def thin_finish(stage):
        rings[stage][2].finish()
        rings[stage][3].finish()
        z_send(stage)

    Z_PARTS = (
        [(i, 0, 5) for i in range(5)],
        [(i, 5, 2) for i in range(5)] + [(5, 0, 7), (6, 0, 7)],
        [(7, 0, 8)] + [(i, 7, 1) for i in range(6, -1, -1)],
    )

    def z_copy(stage, i, j, n):
        return pltpu.make_async_remote_copy(
            src_ref=ZS.at[i, pl.ds(j, n)], dst_ref=ZR.at[i - 1, pl.ds(j, n)],
            send_sem=zssem.at[stage * 7 + i - 1], recv_sem=zrsem.at[stage * 7 + i - 1],
            device_id={"band": ylo * 8 + lax.rem(z + DZ[i], 8)}, device_id_type=MESH)

    def z_send(stage):
        for i, j, n in Z_PARTS[stage]:
            for t in range(j, j + n):
                ZS[i, t] = M[base + block_of(i, t), ylo, xi, yhi]
            if i > 0:
                z_copy(stage, i, j, n).start()

    def z_add(stage):
        for i, j, n in sorted(Z_PARTS[stage]):
            if i > 0:
                z_copy(stage, i, j, n).wait_recv()
                for t in range(j, j + n):
                    at = lax.rem(z + 8 - DZ[i] + DZ[t], 8)
                    TOT[at] = TOT[at] + ZR[i - 1, t]

    arrive(0, 1, 2, 3, 4, 5, 7)
    for o in range(9, 13):
        main_copy(o).start()
    arrive(6, 8)
    ready(range(0, 5))
    build(0)
    wide_start(0)
    wide_relay(0)
    arrive(9, 11)
    for o in range(13, 15):
        main_copy(o).start()
    arrive(10, 12)
    wide_finish(0)
    ready(range(5, 7))
    build(1)
    thin_finish(0)
    wide_start(1)
    wide_relay(1)
    arrive(13, 14)
    ready(range(7, 8))
    build(2)
    wide_finish(1)
    wide_start(2)
    thin_finish(1)
    wide_finish(2)
    thin_finish(2)
    for t in range(8):
        TOT[lax.rem(z + DZ[t], 8)] = ZS[0, t]
    for stage in range(3):
        z_add(stage)

    rows = pl.ds(pl.multiple_of(xi * 16 + yhi * 8, 8), 8)
    for j in range(4):
        lo, hi = merge(TOT[2 * j], TOT[2 * j + 1], low8)
        fin[c, rows, j * 128:(j + 1) * 128] = lo
        fin[c, rows, 512 + j * 128:512 + (j + 1) * 128] = hi

    def gather_copy(k):
        px, ph = lax.rem(xi + k // 2, 4), lax.rem(yhi + k, 2)
        return pltpu.make_async_remote_copy(
            src_ref=fin.at[c, rows], dst_ref=fin.at[c, rows],
            send_sem=fssem.at[k - 1], recv_sem=frsem.at[k - 1],
            device_id={"dom": px * 4 + ph * 2 + c}, device_id_type=MESH)

    def swap_copy(k):
        px, ph = lax.rem(xi - k // 2 + 4, 4), lax.rem(yhi + k, 2)
        part = fin.at[c, pl.ds(pl.multiple_of(px * 16 + ph * 8, 8), 8)]
        return pltpu.make_async_remote_copy(
            src_ref=part, dst_ref=part, send_sem=wssem.at[k], recv_sem=wrsem.at[k],
            device_id={"dom": other}, device_id_type=MESH)

    for k in (5, 4, 7, 6, 3, 2, 1):
        gather_copy(k).start()
    swap_copy(0).start()
    for k in range(1, 8):
        gather_copy(k).wait_recv()
        swap_copy(k).start()
    for k in range(8):
        swap_copy(k).wait_recv()

    for stage in range(3):
        pair_copy(stage).wait_send()
        for ring in rings[stage]:
            ring.wait_send()
        for i, j, n in Z_PARTS[stage]:
            if i > 0:
                z_copy(stage, i, j, n).wait_send()
    for k in range(1, 8):
        gather_copy(k).wait_send()
    for k in range(8):
        swap_copy(k).wait_send()
    for o in range(NB - 1):
        main_copy(o).wait_send()
        coef_copy(o).wait_send()
    for o in range(NB):
        x_copy(o).wait_send()


def on_device(wavefunctions, potential, projectors, hamiltonian_correction, delta_s, projector_count):
    vm = pl.BlockSpec(memory_space=pltpu.VMEM)
    hbm = pl.BlockSpec(memory_space=pl.ANY)
    dma = pltpu.SemaphoreType.DMA
    both = pl.pallas_call(
        kernel,
        out_shape=jax.ShapeDtypeStruct((2, 64, 1024), F32),
        in_specs=[hbm, vm, hbm, vm, vm, pl.BlockSpec(memory_space=pltpu.SMEM)],
        out_specs=vm,
        scratch_shapes=[
            pltpu.VMEM((4096, 128), F32),
            pltpu.VMEM((4608, 128), F32),
            pltpu.VMEM((2, 4, 128, 128), F32),
            pltpu.VMEM((128, 2, 4, 2, 8, 128), F32),
            pltpu.VMEM((129 * RPZ, 128), F32),
            pltpu.VMEM((NB, CHUNK, 128), F32),
            pltpu.VMEM((NB, CH, 8, 128), F32),
            pltpu.VMEM((NB, 16, 128), F32),
            pltpu.VMEM((NB, 16, 128), F32),
            pltpu.VMEM((CH, 2, RPZ, 128), F32),
            pltpu.VMEM((512, 128), F32),
            pltpu.VMEM((1024, 512), BF16),
            pltpu.VMEM((1024, 512), BF16),
            pltpu.VMEM((512, 2048), BF16),
            pltpu.VMEM((512, 2048), BF16),
            pltpu.VMEM((1024, 128), BF16),
            pltpu.VMEM((128, 2048), BF16),
            pltpu.VMEM((64, 2, 4, 2, 8, 128), F32),
            pltpu.VMEM((2, 64, 2, 8, 128), F32),
            pltpu.VMEM((2, 2, 64, 2, 8, 128), F32),
            pltpu.VMEM((3, 7, 2, 2, 8, 128), F32),
            pltpu.VMEM((3, 8, 4, 8, 128), F32),
            pltpu.VMEM((3, 64, 8, 128), F32),
            pltpu.VMEM((8, 8, 8, 128), F32),
            pltpu.VMEM((7, 8, 8, 128), F32),
            pltpu.VMEM((8, 8, 128), F32),
            dma((2,)),
            dma((NB,)), dma((NB,)), dma((NB,)), dma((NB,)), dma((NB,)), dma((NB,)),
            dma((3,)), dma((3,)), dma((72,)), dma((72,)),
            dma((21,)), dma((21,)), dma((7,)), dma((7,)), dma((8,)), dma((8,)),
        ],
        compiler_params=pltpu.CompilerParams(
            collective_id=0, has_side_effects=True, vmem_limit_bytes=60 * 1024 * 1024),
    )(wavefunctions.reshape(4096, 128), potential.reshape(64, 128), projectors.reshape(72 * 64, 128),
      jnp.swapaxes(hamiltonian_correction, 0, 1), jnp.swapaxes(delta_s, 0, 1), projector_count)
    return both[0], both[1]


def solution(mesh):
    placed = (
        P("band", "dom", None, None),
        P("dom", None, None),
        P("dom", None, None, None, None),
        P("dom", None, None),
        P("dom", None, None),
        P("dom"),
    )
    return jax.shard_map(
        on_device, mesh=mesh, in_specs=placed,
        out_specs=(P("band", None), P("band", None)), check_vma=False)
```

```python
import jax
import jax.numpy as jnp
from jax import lax
from jax.experimental import pallas as pl
from jax.experimental.pallas import tpu as pltpu
from jax.sharding import PartitionSpec as P

MESH = pl.DeviceIdType.MESH
F32 = jnp.float32
BF16 = jnp.bfloat16
NB = 16
ND = 16
CH = 8
RPZ = 32
CHUNK = (CH + 1) * RPZ
VOLUME = 1.0 / 131072.0
DZ = (0, 1, 7, 2, 6, 3, 5, 4)
OFFSETS = [(1, 0)] + [(dy, (8 - DZ[p]) % 8) for p in range(1, 8) for dy in (0, 1)]
STAGES = ((0, 5), (5, 7), (7, 8))
START = (0, 25, 49, 64)
HALF = (12, 12, 7)


def block_of(row, col):
    top = max(row, col)
    if top < 5:
        return col * 5 + row
    if top < 7:
        return 25 + col * 2 + row - 5 if col < 5 else 35 + (col - 5) * 7 + row
    return 49 + col if col < 7 else 56 + row


def split(x):
    hi = x.astype(BF16)
    return hi, (x - hi.astype(F32)).astype(BF16)


def dot(a, b):
    return lax.dot_general(a, b, (((1,), (0,)), ((), ())), preferred_element_type=F32)


def dot_exact(a, b):
    return lax.dot_general(a, b, (((1,), (0,)), ((), ())), precision=lax.Precision.HIGHEST,
                           preferred_element_type=F32)


def dot_nt(a, b):
    return lax.dot_general(a, b, (((1,), (1,)), ((), ())), preferred_element_type=F32)


def kernel(psi_in, pot, proj_in, hcor, dels, count, fin,
           psi, proj, SP, M, T, R, RX, CS, CR, VB, AF, AThi, ATlo, Bhi, Blo, ATC, BC, PB,
           F1, F2, FX, FY, G2, ZS, ZR, TOT,
           lsem, ssem, rsem, cssem, crsem, xssem, xrsem, pssem, prsem, gssem, grsem,
           zssem, zrsem, fssem, frsem, wssem, wrsem):
    g = lax.axis_index("band")
    d = lax.axis_index("dom")
    ylo, z = g // 8, lax.rem(g, 8)
    xi, yhi, c = d // 4, lax.rem(d // 2, 2), lax.rem(d, 2)
    y = yhi * 2 + ylo
    dprev = lax.rem(d + ND - 1, ND)
    other = d + 1 - 2 * c

    def peer(o):
        dy, dz = OFFSETS[o]
        return lax.rem(ylo + dy, 2) * 8 + lax.rem(z + dz, 8)

    def source(o):
        dy, dz = OFFSETS[o]
        return lax.rem(ylo + dy, 2) * 8 + lax.rem(z - dz + 8, 8)

    def at_y(q):
        return {"band": lax.rem(q, 2) * 8 + z, "dom": xi * 4 + (q // 2) * 2 + c}

    def at_x(q):
        return {"dom": q * 4 + yhi * 2 + c}

    load_psi = pltpu.make_async_copy(psi_in, psi, lsem.at[0])
    load_proj = pltpu.make_async_copy(proj_in, proj, lsem.at[1])
    load_psi.start()
    load_proj.start()

    barrier = pltpu.get_barrier_semaphore()
    for o in range(NB - 1):
        pl.semaphore_signal(barrier, inc=1, device_id={"band": peer(o)}, device_id_type=MESH)
    for k in range(1, ND):
        pl.semaphore_signal(barrier, inc=1, device_id={"dom": lax.rem(d + k, ND)}, device_id_type=MESH)
    pl.semaphore_signal(barrier, inc=1, device_id={"band": (1 - ylo) * 8 + z, "dom": xi * 4 + (1 - yhi) * 2 + c},
                        device_id_type=MESH)

    load_psi.wait()
    for r in range(RPZ):
        xy = (r // 8) * 16 + r % 8
        a = psi[pl.ds(xy, 64, stride=64), :]
        b = psi[pl.ds(xy + 8, 64, stride=64), :]
        T[pl.ds(r, 128, stride=RPZ), :] = jnp.concatenate([a, b], axis=0).T
    T[pl.ds(128 * RPZ, RPZ), :] = T[pl.ds(0, RPZ), :]

    pl.semaphore_wait(barrier, 31)

    def main_copy(o):
        p = peer(o)
        return pltpu.make_async_remote_copy(
            src_ref=T.at[pl.ds(pl.multiple_of(p * (CH * RPZ), CH * RPZ), CHUNK)],
            dst_ref=R.at[g],
            send_sem=ssem.at[o], recv_sem=rsem.at[o],
            device_id={"band": p}, device_id_type=MESH)

    def coef_copy(o):
        p = peer(o)
        return pltpu.make_async_remote_copy(
            src_ref=CS.at[p], dst_ref=CR.at[g],
            send_sem=cssem.at[o], recv_sem=crsem.at[o],
            device_id={"band": p}, device_id_type=MESH)

    def x_copy(o):
        s = source(o) if o < NB - 1 else g
        return pltpu.make_async_remote_copy(
            src_ref=R.at[s].reshape(CH + 1, RPZ, 128).at[pl.ds(0, CH), pl.ds(0, 8)],
            dst_ref=RX.at[s],
            send_sem=xssem.at[o], recv_sem=xrsem.at[o],
            device_id={"dom": dprev}, device_id_type=MESH)

    for o in range(9):
        main_copy(o).start()

    R[g] = T[pl.ds(pl.multiple_of(g * (CH * RPZ), CH * RPZ), CHUNK), :]

    load_proj.wait()
    def project(t, acc):
        for x in range(4):
            xy = x * 16 + t
            p = jnp.concatenate([psi[pl.ds(xy, 64, stride=64), :], psi[pl.ds(xy + 8, 64, stride=64), :]], axis=1)
            q = jnp.concatenate([proj[pl.ds(xy, 72, stride=64), :], proj[pl.ds(xy + 8, 72, stride=64), :]], axis=1)
            phi, plo = split(p)
            qhi, qlo = split(q)
            acc = acc + dot_nt(qhi, phi) + dot_nt(qhi, plo) + dot_nt(qlo, phi)
        return acc

    acc = lax.fori_loop(0, 8, project, jnp.zeros((72, 64), F32))
    craw = jnp.concatenate([acc, jnp.zeros((56, 64), F32)], axis=0)
    x_copy(NB - 1).start()

    line = lax.broadcasted_iota(jnp.int32, (256, 128), 0)
    slot = lax.broadcasted_iota(jnp.int32, (256, 128), 1)
    spot = (line >> 4) * 5 + (line & 15)
    ext = jnp.where((line & 15) < 5, jnp.where(slot == spot, 1.0, 0.0), 0.0)
    srow = lax.broadcasted_iota(jnp.int32, (128, 128), 0)
    scol = lax.broadcasted_iota(jnp.int32, (128, 128), 1)
    SP[...] = jnp.zeros_like(SP)
    for t, ref in ((1, hcor), (2, dels)):
        inside = jnp.where((line & 15) >= 5 * t, jnp.where((line & 15) < 5 * t + 5, 1.0, 0.0), 0.0)

        for a in range(4):
            SP[t - 1, a, 0:18, 0:18] = ref[:, a, :]

        def couple(a, ext):
            s = SP[t - 1, a]
            s = (0.5 / VOLUME) * (s + s.T)
            used_col = jnp.clip(count[a] - slot, 0, 1).astype(F32)
            used_row = jnp.clip(count[a] - srow, 0, 1).astype(F32)
            left = jnp.where(spot - 5 * t == a * 18 + slot, used_col, 0.0) * inside
            right = jnp.where(scol == a * 18 + srow, used_row, 0.0)
            return ext + dot_exact(dot_exact(left, s), right)

        ext = lax.fori_loop(0, 4, couple, ext)
    chi, clo = split(craw)
    ehi, elo = split(ext)
    msg = dot(ehi, chi) + dot(ehi, clo) + dot(elo, chi)
    msg = jnp.concatenate([msg, msg], axis=1)
    CS[...] = msg.reshape(NB, 16, 128)
    CR[g] = CS[g]
    for o in range(NB - 1):
        coef_copy(o).start()

    v = 3.0 + pltpu.roll(pot[...], lax.rem(128 - g * CH, 128), 1)
    for zi in range(CH):
        wide = jnp.broadcast_to(v[:, zi:zi + 1], (64, 128))
        for half in range(2):
            for x in range(4):
                VB[zi, half, x * 8:(x + 1) * 8, :] = wide[x * 16 + half * 8:x * 16 + half * 8 + 8]

    low = lax.broadcasted_iota(jnp.int32, (RPZ, 128), 1) < 64
    low8 = lax.broadcasted_iota(jnp.int32, (8, 128), 1) < 64
    low16 = lax.broadcasted_iota(jnp.int32, (16, 128), 1) < 64
    last = lax.broadcasted_iota(jnp.int32, (8, 128), 0) == 7
    keep = lax.broadcasted_iota(jnp.int32, (16, 128), 0) < 5

    def merge(a, b, mask):
        return jnp.where(mask, a, pltpu.roll(b, 64, 1)), jnp.where(mask, pltpu.roll(a, 64, 1), b)

    def place(m):
        odd = lax.rem(m, 2)
        dz = odd * ((m + 1) // 2) + (1 - odd) * (8 - m // 2)
        s0 = lax.rem(z + dz, 8)
        at = pl.multiple_of(m * 128, 128)
        return s0, s0 + 8, pl.ds(at, 128), pl.ds(pl.multiple_of(1024 + m * 128, 128), 128)

    def column(s0, s1, zi):
        rows = pl.ds(zi * RPZ, RPZ)
        return merge(R[s0, rows, :], R[s1, rows, :], low)

    def assemble_psi(m, _):
        s0, s1, cols, cols2 = place(m)
        for zi in range(CH):
            now = column(s0, s1, zi)
            for half in range(2):
                rows = pl.ds(half * 256 + zi * RPZ, RPZ)
                AF[rows, :] = now[half]
                hi, lo = split(now[half])
                Bhi[rows, cols2] = hi
                Blo[rows, cols2] = lo
        hi, lo = split(AF[...].T)
        AThi[cols, :] = hi
        ATlo[cols, :] = lo
        cc, _ = merge(CR[s0], CR[s1], low16)
        chi, clo = split(cc)
        chi, clo = chi.astype(F32), clo.astype(F32)
        zero = jnp.zeros((16, 128), F32)
        pad = jnp.zeros((80, 128), F32)
        ahi = jnp.where(keep, chi, zero)
        alo = jnp.where(keep, clo, zero)
        ATC[cols, :] = jnp.concatenate([ahi, ahi, alo, pad], axis=0).T.astype(BF16)
        for t, at in ((1, cols), (2, cols2)):
            bhi = jnp.where(keep, pltpu.roll(chi, 16 - 5 * t, 0), zero)
            blo = jnp.where(keep, pltpu.roll(clo, 16 - 5 * t, 0), zero)
            BC[:, at] = jnp.concatenate([bhi, blo, bhi, pad], axis=0).astype(BF16)
        return 0

    def assemble_h(m, _):
        s0, s1, cols, _ = place(m)
        now = column(s0, s1, 0)
        for zi in range(CH):
            nxt = column(s0, s1, zi + 1)
            halo = merge(RX[s0, zi], RX[s1, zi], low8)
            turned = []
            for half in range(2):
                turned.append([pltpu.roll(now[half][x * 8:(x + 1) * 8], 7, 0) for x in range(4)])
            for half in range(2):
                a = now[half]
                ax = jnp.concatenate([a[8:], halo[half]], axis=0)
                ay = jnp.concatenate(
                    [jnp.where(last, turned[1 - half][x], turned[half][x]) for x in range(4)], axis=0)
                h = VB[zi, half] * a - ax - ay - nxt[half]
                rows = pl.ds(half * 256 + zi * RPZ, RPZ)
                hi, lo = split(h)
                Bhi[rows, cols] = hi
                Blo[rows, cols] = lo
            now = nxt
        return 0

    def product(mat, row, n, col, m, at, down, right):
        rows = pl.ds(pl.multiple_of(row * 128, 128), n * 128)
        cols = pl.ds(pl.multiple_of(mat * 1024 + col * 128, 128), m * 128)
        a = AThi[rows, :]
        res = dot(a, Bhi[:, cols]) + dot(a, Blo[:, cols]) + dot(ATlo[rows, :], Bhi[:, cols]) \
            + dot(ATC[rows, :], BC[:, cols])
        res = res * VOLUME
        for r in range(n):
            for k in range(m):
                M[mat * 64 + at + r * down + k * right] = \
                    res[r * 128:(r + 1) * 128, k * 128:(k + 1) * 128].reshape(2, 4, 2, 8, 128)

    def loop(count_, body):
        def step(t, _):
            body(t)
            return 0
        lax.fori_loop(0, count_, step, 0)

    def even(k, l):
        s = 0.5 * (M[k].reshape(128, 128) + M[l].reshape(128, 128).T)
        M[k] = s.reshape(2, 4, 2, 8, 128)
        M[l] = s.T.reshape(2, 4, 2, 8, 128)

    def products(stage, mat):
        if stage == 0:
            loop(4, lambda t: product(mat, (t // 2) * 2, 2, lax.rem(t, 2) * 2, 2,
                                      lax.rem(t, 2) * 10 + (t // 2) * 2, 1, 5))
            loop(2, lambda t: product(mat, 4, 1, 2 * t, 2, 10 * t + 4, 1, 5))
            loop(2, lambda t: product(mat, 2 * t, 2, 4, 1, 20 + 2 * t, 1, 5))
            product(mat, 4, 1, 4, 1, 24, 1, 5)
        elif stage == 1:
            loop(3, lambda t: product(mat, 2 * t, 2, 5, 2, 35 + 2 * t, 1, 7))
            product(mat, 6, 1, 5, 2, 41, 1, 7)
            loop(2, lambda t: product(mat, 5, 2, 2 * t, 2, 25 + 4 * t, 1, 2))
            product(mat, 5, 2, 4, 1, 33, 1, 2)
        else:
            loop(4, lambda t: product(mat, 2 * t, 2, 7, 1, 56 + 2 * t, 1, 1))
            loop(3, lambda t: product(mat, 7, 1, 2 * t, 2, 49 + 2 * t, 1, 1))
            product(mat, 7, 1, 6, 1, 55, 1, 1)

    def evens(stage):
        if stage == 0:
            def pair(t):
                i, j = t // 5, lax.rem(t, 5)

                @pl.when(i <= j)
                def _():
                    even(j * 5 + i, i * 5 + j)
            loop(25, pair)
        elif stage == 1:
            loop(10, lambda t: even(35 + (t // 5) * 7 + lax.rem(t, 5), 25 + lax.rem(t, 5) * 2 + t // 5))
            for i, j in ((5, 5), (5, 6), (6, 6)):
                even(block_of(i, j), block_of(j, i))
        else:
            loop(7, lambda t: even(56 + t, 49 + t))
            even(63, 63)

    def pair_copy(stage):
        k0, n = START[stage], START[stage + 1] - START[stage]
        return pltpu.make_async_remote_copy(
            src_ref=M.at[pl.ds((1 - c) * 64 + k0, n)], dst_ref=PB.at[pl.ds(k0, n)],
            send_sem=pssem.at[stage], recv_sem=prsem.at[stage],
            device_id={"dom": other}, device_id_type=MESH)

    base = c * 64

    def add_pair(stage):
        pair_copy(stage).wait_recv()

        def body(t):
            M[base + START[stage] + t] = M[base + START[stage] + t] + PB[START[stage] + t]
        loop(START[stage + 1] - START[stage], body)

    class Ring:
        def __init__(self, me, at, piece, first, second, number):
            self.me, self.piece, self.first, self.second = me, piece, first, second
            self.plus, self.minus = at(lax.rem(me + 1, 4)), at(lax.rem(me + 3, 4))
            self.number = number

        def copy(self, k):
            me = self.me
            q, h, buf, way = (
                (me + 2, 0, self.first(0), self.plus),
                (me + 2, 1, self.first(1), self.minus),
                (me + 1, 1, self.second(0, 1), self.plus),
                (me + 3, 0, self.second(1, 0), self.minus),
                (me + 1, 0, self.second(0, 0), self.plus),
                (me + 3, 1, self.second(1, 1), self.minus),
            )[k]
            return pltpu.make_async_remote_copy(
                src_ref=M.at[self.piece(lax.rem(q, 4), h)], dst_ref=buf,
                send_sem=gssem.at[self.number + k], recv_sem=grsem.at[self.number + k],
                device_id=way, device_id_type=MESH)

        def start(self):
            for k in range(4):
                self.copy(k).start()

        def add(self, q, h, *bufs):
            at = self.piece(lax.rem(q, 4), h)
            total = M[at]
            for b in bufs:
                total = total + b[...]
            M[at] = total

        def relay(self):
            self.copy(0).wait_recv()
            self.add(self.me + 1, 0, self.first(0))
            self.copy(4).start()
            self.copy(1).wait_recv()
            self.add(self.me + 3, 1, self.first(1))
            self.copy(5).start()

        def finish(self):
            for k in range(2, 6):
                self.copy(k).wait_recv()
            for h in range(2):
                self.add(self.me, h, self.second(0, h), self.second(1, h))

        def wait_send(self):
            for k in range(6):
                self.copy(k).wait_send()

    class Direct:
        def __init__(self, me, at, piece, buf, number):
            self.me, self.at, self.piece, self.buf, self.number = me, at, piece, buf, number

        def copy(self, k):
            q = lax.rem(self.me + k, 4)
            return pltpu.make_async_remote_copy(
                src_ref=M.at[self.piece(q)], dst_ref=self.buf(k - 1),
                send_sem=gssem.at[self.number + k - 1], recv_sem=grsem.at[self.number + k - 1],
                device_id=self.at(q), device_id_type=MESH)

        def start(self):
            for k in (2, 1, 3):
                self.copy(k).start()

        def finish(self):
            at = self.piece(self.me)
            total = M[at]
            for k in (1, 3, 2):
                self.copy(k).wait_recv()
                total = total + self.buf(k - 1)[...]
            M[at] = total

        def wait_send(self):
            for k in range(1, 4):
                self.copy(k).wait_send()

    rings = []
    full = slice(None)
    for stage in range(3):
        k0, n = START[stage], START[stage + 1] - START[stage]
        na = HALF[stage]
        nb = n - na
        kb = k0 + na

        def ax_piece(q, h, k0=k0, na=na):
            return (pl.ds(base + k0, na), h, q)

        def by_piece(q, h, kb=kb, nb=nb):
            return (pl.ds(base + kb, nb), lax.rem(q, 2), pl.ds(2 * h, 2), q // 2)

        def ax_whole(q, k0=k0, na=na):
            return (pl.ds(base + k0, na), full, q)

        def by_whole(q, kb=kb, nb=nb):
            return (pl.ds(base + kb, nb), lax.rem(q, 2), full, q // 2)

        def ay_piece(q, k0=k0, na=na):
            return (pl.ds(base + k0, na), lax.rem(q, 2), xi, q // 2)

        def bx_piece(q, kb=kb, nb=nb):
            return (pl.ds(base + kb, nb), ylo, q, yhi)

        def wide_first(k, n):
            return lambda h: F1.at[h, pl.ds(k, n)]

        def wide_second(k, n):
            return lambda w, h: F2.at[w, h, pl.ds(k, n)]

        def thin(k, n):
            return lambda i: G2.at[i, pl.ds(k, n)]

        number = stage * 24
        if stage < 2:
            wide = (Ring(xi, at_x, ax_piece, wide_first(k0, na), wide_second(k0, na), number),
                    Ring(y, at_y, by_piece, wide_first(kb, nb), wide_second(kb, nb), number + 6))
        else:
            wide = (Direct(xi, at_x, ax_whole, lambda i: FX.at[i], number),
                    Direct(y, at_y, by_whole, lambda i: FY.at[i], number + 6))
        rings.append(wide + (
            Direct(y, at_y, ay_piece, thin(k0, na), number + 12),
            Direct(xi, at_x, bx_piece, thin(kb, nb), number + 18),
        ))

    def arrive(*offsets):
        for o in offsets:
            main_copy(o).wait_recv()
            x_copy(o).start()

    def overlap_part(stage):
        first, last_ = STAGES[stage]
        for o in ((0,) if stage == 0 else ()) + tuple(range(max(1, 2 * first - 1), 2 * last_ - 1)):
            coef_copy(o).wait_recv()
        lax.fori_loop(first, last_, assemble_psi, 0)
        products(stage, 1)

        @pl.when(c == 0)
        def _():
            pair_copy(stage).start()

    def energy_part(stage):
        first, last_ = STAGES[stage]
        for o in ((NB - 1, 0) if stage == 0 else ()) + tuple(range(max(1, 2 * first - 1), 2 * last_ - 1)):
            x_copy(o).wait_recv()
        lax.fori_loop(first, last_, assemble_h, 0)
        products(stage, 0)
        evens(stage)

        @pl.when(c == 1)
        def _():
            pair_copy(stage).start()

    def wide_start(stage):
        add_pair(stage)
        rings[stage][0].start()
        rings[stage][1].start()

    def wide_relay(stage):
        rings[stage][0].relay()
        rings[stage][1].relay()

    def wide_finish(stage):
        rings[stage][0].finish()
        rings[stage][2].start()
        rings[stage][1].finish()
        rings[stage][3].start()

    def thin_finish(stage):
        rings[stage][2].finish()
        rings[stage][3].finish()
        z_send(stage)

    Z_PARTS = (
        [(i, 0, 5) for i in range(5)],
        [(i, 5, 2) for i in range(5)] + [(5, 0, 7), (6, 0, 7)],
        [(7, 0, 8)] + [(i, 7, 1) for i in range(6, -1, -1)],
    )

    def z_copy(stage, i, j, n):
        return pltpu.make_async_remote_copy(
            src_ref=ZS.at[i, pl.ds(j, n)], dst_ref=ZR.at[i - 1, pl.ds(j, n)],
            send_sem=zssem.at[stage * 7 + i - 1], recv_sem=zrsem.at[stage * 7 + i - 1],
            device_id={"band": ylo * 8 + lax.rem(z + DZ[i], 8)}, device_id_type=MESH)

    def z_send(stage):
        for i, j, n in Z_PARTS[stage]:
            for t in range(j, j + n):
                ZS[i, t] = M[base + block_of(i, t), ylo, xi, yhi]
            if i > 0:
                z_copy(stage, i, j, n).start()

    def z_add(stage):
        for i, j, n in sorted(Z_PARTS[stage]):
            if i > 0:
                z_copy(stage, i, j, n).wait_recv()
                for t in range(j, j + n):
                    at = lax.rem(z + 8 - DZ[i] + DZ[t], 8)
                    TOT[at] = TOT[at] + ZR[i - 1, t]

    arrive(0, 1, 2, 3, 4, 5, 7)
    for o in range(9, 13):
        main_copy(o).start()
    arrive(6, 8)
    overlap_part(0)
    for o in range(13, 15):
        main_copy(o).start()
    energy_part(0)
    wide_start(0)
    wide_relay(0)
    arrive(9, 11, 10, 12)
    overlap_part(1)
    wide_finish(0)
    energy_part(1)
    wide_start(1)
    thin_finish(0)
    arrive(13, 14)
    overlap_part(2)
    wide_relay(1)
    energy_part(2)
    wide_finish(1)
    wide_start(2)
    thin_finish(1)
    wide_finish(2)
    thin_finish(2)
    for t in range(8):
        TOT[lax.rem(z + DZ[t], 8)] = ZS[0, t]
    for stage in range(3):
        z_add(stage)

    rows = pl.ds(pl.multiple_of(xi * 16 + yhi * 8, 8), 8)
    for j in range(4):
        lo, hi = merge(TOT[2 * j], TOT[2 * j + 1], low8)
        fin[c, rows, j * 128:(j + 1) * 128] = lo
        fin[c, rows, 512 + j * 128:512 + (j + 1) * 128] = hi

    def gather_copy(k):
        px, ph = lax.rem(xi + k // 2, 4), lax.rem(yhi + k, 2)
        return pltpu.make_async_remote_copy(
            src_ref=fin.at[c, rows], dst_ref=fin.at[c, rows],
            send_sem=fssem.at[k - 1], recv_sem=frsem.at[k - 1],
            device_id={"dom": px * 4 + ph * 2 + c}, device_id_type=MESH)

    def swap_copy(k):
        px, ph = lax.rem(xi - k // 2 + 4, 4), lax.rem(yhi + k, 2)
        part = fin.at[c, pl.ds(pl.multiple_of(px * 16 + ph * 8, 8), 8)]
        return pltpu.make_async_remote_copy(
            src_ref=part, dst_ref=part, send_sem=wssem.at[k], recv_sem=wrsem.at[k],
            device_id={"dom": other}, device_id_type=MESH)

    for k in (5, 4, 7, 6, 3, 2, 1):
        gather_copy(k).start()
    swap_copy(0).start()
    for k in range(1, 8):
        gather_copy(k).wait_recv()
        swap_copy(k).start()
    for k in range(8):
        swap_copy(k).wait_recv()

    for stage in range(3):
        pair_copy(stage).wait_send()
        for ring in rings[stage]:
            ring.wait_send()
        for i, j, n in Z_PARTS[stage]:
            if i > 0:
                z_copy(stage, i, j, n).wait_send()
    for k in range(1, 8):
        gather_copy(k).wait_send()
    for k in range(8):
        swap_copy(k).wait_send()
    for o in range(NB - 1):
        main_copy(o).wait_send()
        coef_copy(o).wait_send()
    for o in range(NB):
        x_copy(o).wait_send()


def on_device(wavefunctions, potential, projectors, hamiltonian_correction, delta_s, projector_count):
    vm = pl.BlockSpec(memory_space=pltpu.VMEM)
    hbm = pl.BlockSpec(memory_space=pl.ANY)
    dma = pltpu.SemaphoreType.DMA
    both = pl.pallas_call(
        kernel,
        out_shape=jax.ShapeDtypeStruct((2, 64, 1024), F32),
        in_specs=[hbm, vm, hbm, vm, vm, pl.BlockSpec(memory_space=pltpu.SMEM)],
        out_specs=vm,
        scratch_shapes=[
            pltpu.VMEM((4096, 128), F32),
            pltpu.VMEM((4608, 128), F32),
            pltpu.VMEM((2, 4, 128, 128), F32),
            pltpu.VMEM((128, 2, 4, 2, 8, 128), F32),
            pltpu.VMEM((129 * RPZ, 128), F32),
            pltpu.VMEM((NB, CHUNK, 128), F32),
            pltpu.VMEM((NB, CH, 8, 128), F32),
            pltpu.VMEM((NB, 16, 128), F32),
            pltpu.VMEM((NB, 16, 128), F32),
            pltpu.VMEM((CH, 2, RPZ, 128), F32),
            pltpu.VMEM((512, 128), F32),
            pltpu.VMEM((1024, 512), BF16),
            pltpu.VMEM((1024, 512), BF16),
            pltpu.VMEM((512, 2048), BF16),
            pltpu.VMEM((512, 2048), BF16),
            pltpu.VMEM((1024, 128), BF16),
            pltpu.VMEM((128, 2048), BF16),
            pltpu.VMEM((64, 2, 4, 2, 8, 128), F32),
            pltpu.VMEM((2, 64, 2, 8, 128), F32),
            pltpu.VMEM((2, 2, 64, 2, 8, 128), F32),
            pltpu.VMEM((3, 7, 2, 2, 8, 128), F32),
            pltpu.VMEM((3, 8, 4, 8, 128), F32),
            pltpu.VMEM((3, 64, 8, 128), F32),
            pltpu.VMEM((8, 8, 8, 128), F32),
            pltpu.VMEM((7, 8, 8, 128), F32),
            pltpu.VMEM((8, 8, 128), F32),
            dma((2,)),
            dma((NB,)), dma((NB,)), dma((NB,)), dma((NB,)), dma((NB,)), dma((NB,)),
            dma((3,)), dma((3,)), dma((72,)), dma((72,)),
            dma((21,)), dma((21,)), dma((7,)), dma((7,)), dma((8,)), dma((8,)),
        ],
        compiler_params=pltpu.CompilerParams(
            collective_id=0, has_side_effects=True, vmem_limit_bytes=60 * 1024 * 1024),
    )(wavefunctions.reshape(4096, 128), potential.reshape(64, 128), projectors.reshape(72 * 64, 128),
      jnp.swapaxes(hamiltonian_correction, 0, 1), jnp.swapaxes(delta_s, 0, 1), projector_count)
    return both[0], both[1]


def solution(mesh):
    placed = (
        P("band", "dom", None, None),
        P("dom", None, None),
        P("dom", None, None, None, None),
        P("dom", None, None),
        P("dom", None, None),
        P("dom"),
    )
    return jax.shard_map(
        on_device, mesh=mesh, in_specs=placed,
        out_specs=(P("band", None), P("band", None)), check_vma=False)
```

```python
import jax
import jax.numpy as jnp
from jax import lax
from jax.experimental import pallas as pl
from jax.experimental.pallas import tpu as pltpu
from jax.sharding import PartitionSpec as P

MESH = pl.DeviceIdType.MESH
F32 = jnp.float32
BF16 = jnp.bfloat16
NB = 16
ND = 16
CH = 8
RPZ = 32
CHUNK = (CH + 1) * RPZ
VOLUME = 1.0 / 131072.0
DZ = (0, 1, 7, 2, 6, 3, 5, 4)
OFFSETS = [(1, 0)] + [(dy, (8 - DZ[p]) % 8) for p in range(1, 8) for dy in (0, 1)]
STAGES = ((0, 5), (5, 7), (7, 8))
START = (0, 25, 49, 64)
HALF = (12, 12, 7)


def block_of(row, col):
    top = max(row, col)
    if top < 5:
        return col * 5 + row
    if top < 7:
        return 25 + col * 2 + row - 5 if col < 5 else 35 + (col - 5) * 7 + row
    return 49 + col if col < 7 else 56 + row


def split(x):
    hi = x.astype(BF16)
    return hi, (x - hi.astype(F32)).astype(BF16)


def dot(a, b):
    return lax.dot_general(a, b, (((1,), (0,)), ((), ())), preferred_element_type=F32)


def dot_exact(a, b):
    return lax.dot_general(a, b, (((1,), (0,)), ((), ())), precision=lax.Precision.HIGHEST,
                           preferred_element_type=F32)


def dot_nt(a, b):
    return lax.dot_general(a, b, (((1,), (1,)), ((), ())), preferred_element_type=F32)


def kernel(psi_in, pot, proj_in, hcor, dels, count, fin,
           psi, proj, SP, M, T, R, RX, CS, CR, VB, AF, AThi, ATlo, Bhi, Blo, ATC, BC, PB,
           F1, F2, FX, FY, G2, ZS, ZR, TOT, HX,
           lsem, ssem, rsem, cssem, crsem, xssem, xrsem, pssem, prsem, gssem, grsem,
           zssem, zrsem, fssem, frsem, wssem, wrsem, hxsem, hsem):
    g = lax.axis_index("band")
    d = lax.axis_index("dom")
    ylo, z = g // 8, lax.rem(g, 8)
    xi, yhi, c = d // 4, lax.rem(d // 2, 2), lax.rem(d, 2)
    y = yhi * 2 + ylo
    dprev = lax.rem(d + ND - 1, ND)
    other = d + 1 - 2 * c

    def peer(o):
        dy, dz = OFFSETS[o]
        return lax.rem(ylo + dy, 2) * 8 + lax.rem(z + dz, 8)

    def source(o):
        dy, dz = OFFSETS[o]
        return lax.rem(ylo + dy, 2) * 8 + lax.rem(z - dz + 8, 8)

    def at_y(q):
        return {"band": lax.rem(q, 2) * 8 + z, "dom": xi * 4 + (q // 2) * 2 + c}

    def at_x(q):
        return {"dom": q * 4 + yhi * 2 + c}

    load_psi = pltpu.make_async_copy(psi_in, psi, lsem.at[0])
    load_proj = pltpu.make_async_copy(proj_in, proj, lsem.at[1])
    load_psi.start()
    load_proj.start()

    barrier = pltpu.get_barrier_semaphore()
    for o in range(NB - 1):
        pl.semaphore_signal(barrier, inc=1, device_id={"band": peer(o)}, device_id_type=MESH)
    for k in range(1, ND):
        pl.semaphore_signal(barrier, inc=1, device_id={"dom": lax.rem(d + k, ND)}, device_id_type=MESH)
    pl.semaphore_signal(barrier, inc=1, device_id={"band": (1 - ylo) * 8 + z, "dom": xi * 4 + (1 - yhi) * 2 + c},
                        device_id_type=MESH)

    load_psi.wait()
    for r in range(RPZ):
        xy = (r // 8) * 16 + r % 8
        a = psi[pl.ds(xy, 64, stride=64), :]
        b = psi[pl.ds(xy + 8, 64, stride=64), :]
        T[pl.ds(r, 128, stride=RPZ), :] = jnp.concatenate([a, b], axis=0).T
    T[pl.ds(128 * RPZ, RPZ), :] = T[pl.ds(0, RPZ), :]

    pl.semaphore_wait(barrier, 31)

    def main_copy(o):
        p = peer(o)
        return pltpu.make_async_remote_copy(
            src_ref=T.at[pl.ds(pl.multiple_of(p * (CH * RPZ), CH * RPZ), CHUNK)],
            dst_ref=R.at[g],
            send_sem=ssem.at[o], recv_sem=rsem.at[o],
            device_id={"band": p}, device_id_type=MESH)

    def coef_copy(o):
        p = peer(o)
        return pltpu.make_async_remote_copy(
            src_ref=CS.at[p], dst_ref=CR.at[g],
            send_sem=cssem.at[o], recv_sem=crsem.at[o],
            device_id={"band": p}, device_id_type=MESH)

    def x_copy(o):
        s = source(o) if o < NB - 1 else g
        return pltpu.make_async_remote_copy(
            src_ref=R.at[s].reshape(CH + 1, RPZ, 128).at[pl.ds(0, CH), pl.ds(0, 8)],
            dst_ref=RX.at[s],
            send_sem=xssem.at[o], recv_sem=xrsem.at[o],
            device_id={"dom": dprev}, device_id_type=MESH)

    home_copy = pltpu.make_async_remote_copy(
        src_ref=T.reshape(129, RPZ, 128).at[pl.ds(0, 128), pl.ds(0, 8)], dst_ref=HX,
        send_sem=hxsem.at[0], recv_sem=hxsem.at[1],
        device_id={"dom": dprev}, device_id_type=MESH)

    def halo_copy(o):
        p = peer(o)
        return pltpu.make_async_remote_copy(
            src_ref=HX.at[pl.ds(pl.multiple_of(p * CH, CH), CH)], dst_ref=RX.at[g],
            send_sem=hsem.at[o], recv_sem=xrsem.at[o],
            device_id={"band": p}, device_id_type=MESH)

    def send_far(*offsets):
        for o in offsets:
            main_copy(o).start()

            @pl.when(c == 1)
            def _():
                halo_copy(o).start()

    for o in range(9):
        main_copy(o).start()

    @pl.when(c == 0)
    def _():
        home_copy.start()

    R[g] = T[pl.ds(pl.multiple_of(g * (CH * RPZ), CH * RPZ), CHUNK), :]

    load_proj.wait()
    def project(t, acc):
        for x in range(4):
            xy = x * 16 + t
            p = jnp.concatenate([psi[pl.ds(xy, 64, stride=64), :], psi[pl.ds(xy + 8, 64, stride=64), :]], axis=1)
            q = jnp.concatenate([proj[pl.ds(xy, 72, stride=64), :], proj[pl.ds(xy + 8, 72, stride=64), :]], axis=1)
            phi, plo = split(p)
            qhi, qlo = split(q)
            acc = acc + dot_nt(qhi, phi) + dot_nt(qhi, plo) + dot_nt(qlo, phi)
        return acc

    acc = lax.fori_loop(0, 8, project, jnp.zeros((72, 64), F32))
    craw = jnp.concatenate([acc, jnp.zeros((56, 64), F32)], axis=0)
    x_copy(NB - 1).start()

    line = lax.broadcasted_iota(jnp.int32, (256, 128), 0)
    slot = lax.broadcasted_iota(jnp.int32, (256, 128), 1)
    spot = (line >> 4) * 5 + (line & 15)
    ext = jnp.where((line & 15) < 5, jnp.where(slot == spot, 1.0, 0.0), 0.0)
    srow = lax.broadcasted_iota(jnp.int32, (128, 128), 0)
    scol = lax.broadcasted_iota(jnp.int32, (128, 128), 1)
    SP[...] = jnp.zeros_like(SP)
    for t, ref in ((1, hcor), (2, dels)):
        inside = jnp.where((line & 15) >= 5 * t, jnp.where((line & 15) < 5 * t + 5, 1.0, 0.0), 0.0)

        for a in range(4):
            SP[t - 1, a, 0:18, 0:18] = ref[:, a, :]

        def couple(a, ext):
            s = SP[t - 1, a]
            s = (0.5 / VOLUME) * (s + s.T)
            used_col = jnp.clip(count[a] - slot, 0, 1).astype(F32)
            used_row = jnp.clip(count[a] - srow, 0, 1).astype(F32)
            left = jnp.where(spot - 5 * t == a * 18 + slot, used_col, 0.0) * inside
            right = jnp.where(scol == a * 18 + srow, used_row, 0.0)
            return ext + dot_exact(dot_exact(left, s), right)

        ext = lax.fori_loop(0, 4, couple, ext)
    chi, clo = split(craw)
    ehi, elo = split(ext)
    msg = dot(ehi, chi) + dot(ehi, clo) + dot(elo, chi)
    msg = jnp.concatenate([msg, msg], axis=1)
    CS[...] = msg.reshape(NB, 16, 128)
    CR[g] = CS[g]
    for o in range(NB - 1):
        coef_copy(o).start()

    v = 3.0 + pltpu.roll(pot[...], lax.rem(128 - g * CH, 128), 1)
    for zi in range(CH):
        wide = jnp.broadcast_to(v[:, zi:zi + 1], (64, 128))
        for half in range(2):
            for x in range(4):
                VB[zi, half, x * 8:(x + 1) * 8, :] = wide[x * 16 + half * 8:x * 16 + half * 8 + 8]

    low = lax.broadcasted_iota(jnp.int32, (RPZ, 128), 1) < 64
    low8 = lax.broadcasted_iota(jnp.int32, (8, 128), 1) < 64
    low16 = lax.broadcasted_iota(jnp.int32, (16, 128), 1) < 64
    last = lax.broadcasted_iota(jnp.int32, (8, 128), 0) == 7
    keep = lax.broadcasted_iota(jnp.int32, (16, 128), 0) < 5

    def merge(a, b, mask):
        return jnp.where(mask, a, pltpu.roll(b, 64, 1)), jnp.where(mask, pltpu.roll(a, 64, 1), b)

    def place(m):
        odd = lax.rem(m, 2)
        dz = odd * ((m + 1) // 2) + (1 - odd) * (8 - m // 2)
        s0 = lax.rem(z + dz, 8)
        at = pl.multiple_of(m * 128, 128)
        return s0, s0 + 8, pl.ds(at, 128), pl.ds(pl.multiple_of(1024 + m * 128, 128), 128)

    def column(s0, s1, zi):
        rows = pl.ds(zi * RPZ, RPZ)
        return merge(R[s0, rows, :], R[s1, rows, :], low)

    def assemble_psi(m, _):
        s0, s1, cols, cols2 = place(m)
        for zi in range(CH):
            now = column(s0, s1, zi)
            for half in range(2):
                rows = pl.ds(half * 256 + zi * RPZ, RPZ)
                AF[rows, :] = now[half]
                hi, lo = split(now[half])
                Bhi[rows, cols2] = hi
                Blo[rows, cols2] = lo
        hi, lo = split(AF[...].T)
        AThi[cols, :] = hi
        ATlo[cols, :] = lo
        cc, _ = merge(CR[s0], CR[s1], low16)
        chi, clo = split(cc)
        chi, clo = chi.astype(F32), clo.astype(F32)
        zero = jnp.zeros((16, 128), F32)
        pad = jnp.zeros((80, 128), F32)
        ahi = jnp.where(keep, chi, zero)
        alo = jnp.where(keep, clo, zero)
        ATC[cols, :] = jnp.concatenate([ahi, ahi, alo, pad], axis=0).T.astype(BF16)
        for t, at in ((1, cols), (2, cols2)):
            bhi = jnp.where(keep, pltpu.roll(chi, 16 - 5 * t, 0), zero)
            blo = jnp.where(keep, pltpu.roll(clo, 16 - 5 * t, 0), zero)
            BC[:, at] = jnp.concatenate([bhi, blo, bhi, pad], axis=0).astype(BF16)
        return 0

    def assemble_h(m, _):
        s0, s1, cols, _ = place(m)
        now = column(s0, s1, 0)
        for zi in range(CH):
            nxt = column(s0, s1, zi + 1)
            halo = merge(RX[s0, zi], RX[s1, zi], low8)
            turned = []
            for half in range(2):
                turned.append([pltpu.roll(now[half][x * 8:(x + 1) * 8], 7, 0) for x in range(4)])
            for half in range(2):
                a = now[half]
                ax = jnp.concatenate([a[8:], halo[half]], axis=0)
                ay = jnp.concatenate(
                    [jnp.where(last, turned[1 - half][x], turned[half][x]) for x in range(4)], axis=0)
                h = VB[zi, half] * a - ax - ay - nxt[half]
                rows = pl.ds(half * 256 + zi * RPZ, RPZ)
                hi, lo = split(h)
                Bhi[rows, cols] = hi
                Blo[rows, cols] = lo
            now = nxt
        return 0

    def product(mat, row, n, col, m, at, down, right):
        rows = pl.ds(pl.multiple_of(row * 128, 128), n * 128)
        cols = pl.ds(pl.multiple_of(mat * 1024 + col * 128, 128), m * 128)
        a = AThi[rows, :]
        res = dot(a, Bhi[:, cols]) + dot(a, Blo[:, cols]) + dot(ATlo[rows, :], Bhi[:, cols]) \
            + dot(ATC[rows, :], BC[:, cols])
        res = res * VOLUME
        for r in range(n):
            for k in range(m):
                M[mat * 64 + at + r * down + k * right] = \
                    res[r * 128:(r + 1) * 128, k * 128:(k + 1) * 128].reshape(2, 4, 2, 8, 128)

    def loop(count_, body):
        def step(t, _):
            body(t)
            return 0
        lax.fori_loop(0, count_, step, 0)

    def even(k, l):
        s = 0.5 * (M[k].reshape(128, 128) + M[l].reshape(128, 128).T)
        M[k] = s.reshape(2, 4, 2, 8, 128)
        M[l] = s.T.reshape(2, 4, 2, 8, 128)

    def products(stage, mat):
        if stage == 0:
            loop(4, lambda t: product(mat, (t // 2) * 2, 2, lax.rem(t, 2) * 2, 2,
                                      lax.rem(t, 2) * 10 + (t // 2) * 2, 1, 5))
            loop(2, lambda t: product(mat, 4, 1, 2 * t, 2, 10 * t + 4, 1, 5))
            loop(2, lambda t: product(mat, 2 * t, 2, 4, 1, 20 + 2 * t, 1, 5))
            product(mat, 4, 1, 4, 1, 24, 1, 5)
        elif stage == 1:
            loop(3, lambda t: product(mat, 2 * t, 2, 5, 2, 35 + 2 * t, 1, 7))
            product(mat, 6, 1, 5, 2, 41, 1, 7)
            loop(2, lambda t: product(mat, 5, 2, 2 * t, 2, 25 + 4 * t, 1, 2))
            product(mat, 5, 2, 4, 1, 33, 1, 2)
        else:
            loop(4, lambda t: product(mat, 2 * t, 2, 7, 1, 56 + 2 * t, 1, 1))
            loop(3, lambda t: product(mat, 7, 1, 2 * t, 2, 49 + 2 * t, 1, 1))
            product(mat, 7, 1, 6, 1, 55, 1, 1)

    def evens(stage):
        if stage == 0:
            def pair(t):
                i, j = t // 5, lax.rem(t, 5)

                @pl.when(i <= j)
                def _():
                    even(j * 5 + i, i * 5 + j)
            loop(25, pair)
        elif stage == 1:
            loop(10, lambda t: even(35 + (t // 5) * 7 + lax.rem(t, 5), 25 + lax.rem(t, 5) * 2 + t // 5))
            for i, j in ((5, 5), (5, 6), (6, 6)):
                even(block_of(i, j), block_of(j, i))
        else:
            loop(7, lambda t: even(56 + t, 49 + t))
            even(63, 63)

    def pair_copy(stage):
        k0, n = START[stage], START[stage + 1] - START[stage]
        return pltpu.make_async_remote_copy(
            src_ref=M.at[pl.ds((1 - c) * 64 + k0, n)], dst_ref=PB.at[pl.ds(k0, n)],
            send_sem=pssem.at[stage], recv_sem=prsem.at[stage],
            device_id={"dom": other}, device_id_type=MESH)

    base = c * 64

    def add_pair(stage):
        pair_copy(stage).wait_recv()

        def body(t):
            M[base + START[stage] + t] = M[base + START[stage] + t] + PB[START[stage] + t]
        loop(START[stage + 1] - START[stage], body)

    class Ring:
        def __init__(self, me, at, piece, first, second, number):
            self.me, self.piece, self.first, self.second = me, piece, first, second
            self.plus, self.minus = at(lax.rem(me + 1, 4)), at(lax.rem(me + 3, 4))
            self.number = number

        def copy(self, k):
            me = self.me
            q, h, buf, way = (
                (me + 2, 0, self.first(0), self.plus),
                (me + 2, 1, self.first(1), self.minus),
                (me + 1, 1, self.second(0, 1), self.plus),
                (me + 3, 0, self.second(1, 0), self.minus),
                (me + 1, 0, self.second(0, 0), self.plus),
                (me + 3, 1, self.second(1, 1), self.minus),
            )[k]
            return pltpu.make_async_remote_copy(
                src_ref=M.at[self.piece(lax.rem(q, 4), h)], dst_ref=buf,
                send_sem=gssem.at[self.number + k], recv_sem=grsem.at[self.number + k],
                device_id=way, device_id_type=MESH)

        def start(self):
            for k in range(4):
                self.copy(k).start()

        def add(self, q, h, *bufs):
            at = self.piece(lax.rem(q, 4), h)
            total = M[at]
            for b in bufs:
                total = total + b[...]
            M[at] = total

        def relay(self):
            self.copy(0).wait_recv()
            self.add(self.me + 1, 0, self.first(0))
            self.copy(4).start()
            self.copy(1).wait_recv()
            self.add(self.me + 3, 1, self.first(1))
            self.copy(5).start()

        def finish(self):
            for k in range(2, 6):
                self.copy(k).wait_recv()
            for h in range(2):
                self.add(self.me, h, self.second(0, h), self.second(1, h))

        def wait_send(self):
            for k in range(6):
                self.copy(k).wait_send()

    class Direct:
        def __init__(self, me, at, piece, buf, number):
            self.me, self.at, self.piece, self.buf, self.number = me, at, piece, buf, number

        def copy(self, k):
            q = lax.rem(self.me + k, 4)
            return pltpu.make_async_remote_copy(
                src_ref=M.at[self.piece(q)], dst_ref=self.buf(k - 1),
                send_sem=gssem.at[self.number + k - 1], recv_sem=grsem.at[self.number + k - 1],
                device_id=self.at(q), device_id_type=MESH)

        def start(self):
            for k in (2, 1, 3):
                self.copy(k).start()

        def finish(self):
            at = self.piece(self.me)
            total = M[at]
            for k in (1, 3, 2):
                self.copy(k).wait_recv()
                total = total + self.buf(k - 1)[...]
            M[at] = total

        def wait_send(self):
            for k in range(1, 4):
                self.copy(k).wait_send()

    rings = []
    full = slice(None)
    for stage in range(3):
        k0, n = START[stage], START[stage + 1] - START[stage]
        na = HALF[stage]
        nb = n - na
        kb = k0 + na

        def ax_piece(q, h, k0=k0, na=na):
            return (pl.ds(base + k0, na), h, q)

        def by_piece(q, h, kb=kb, nb=nb):
            return (pl.ds(base + kb, nb), lax.rem(q, 2), pl.ds(2 * h, 2), q // 2)

        def ax_whole(q, k0=k0, na=na):
            return (pl.ds(base + k0, na), full, q)

        def by_whole(q, kb=kb, nb=nb):
            return (pl.ds(base + kb, nb), lax.rem(q, 2), full, q // 2)

        def ay_piece(q, k0=k0, na=na):
            return (pl.ds(base + k0, na), lax.rem(q, 2), xi, q // 2)

        def bx_piece(q, kb=kb, nb=nb):
            return (pl.ds(base + kb, nb), ylo, q, yhi)

        def wide_first(k, n):
            return lambda h: F1.at[h, pl.ds(k, n)]

        def wide_second(k, n):
            return lambda w, h: F2.at[w, h, pl.ds(k, n)]

        def thin(k, n):
            return lambda i: G2.at[i, pl.ds(k, n)]

        number = stage * 24
        if stage < 2:
            wide = (Ring(xi, at_x, ax_piece, wide_first(k0, na), wide_second(k0, na), number),
                    Ring(y, at_y, by_piece, wide_first(kb, nb), wide_second(kb, nb), number + 6))
        else:
            wide = (Direct(xi, at_x, ax_whole, lambda i: FX.at[i], number),
                    Direct(y, at_y, by_whole, lambda i: FY.at[i], number + 6))
        rings.append(wide + (
            Direct(y, at_y, ay_piece, thin(k0, na), number + 12),
            Direct(xi, at_x, bx_piece, thin(kb, nb), number + 18),
        ))

    def arrive(*offsets):
        for o in offsets:
            main_copy(o).wait_recv()
            if o < 9:
                x_copy(o).start()
            else:
                @pl.when(c == 1)
                def _():
                    x_copy(o).start()

    def overlap_part(stage):
        first, last_ = STAGES[stage]
        for o in ((0,) if stage == 0 else ()) + tuple(range(max(1, 2 * first - 1), 2 * last_ - 1)):
            coef_copy(o).wait_recv()
        lax.fori_loop(first, last_, assemble_psi, 0)
        products(stage, 1)

        @pl.when(c == 0)
        def _():
            pair_copy(stage).start()

    def energy_part(stage):
        first, last_ = STAGES[stage]
        for o in ((NB - 1, 0) if stage == 0 else ()) + tuple(range(max(1, 2 * first - 1), 2 * last_ - 1)):
            x_copy(o).wait_recv()
        lax.fori_loop(first, last_, assemble_h, 0)
        products(stage, 0)
        evens(stage)

        @pl.when(c == 1)
        def _():
            pair_copy(stage).start()

    def wide_start(stage):
        add_pair(stage)
        rings[stage][0].start()
        rings[stage][1].start()

    def wide_relay(stage):
        rings[stage][0].relay()
        rings[stage][1].relay()

    def wide_finish(stage):
        rings[stage][0].finish()
        rings[stage][2].start()
        rings[stage][1].finish()
        rings[stage][3].start()

    def thin_finish(stage):
        rings[stage][2].finish()
        rings[stage][3].finish()
        z_send(stage)

    Z_PARTS = (
        [(i, 0, 5) for i in range(5)],
        [(i, 5, 2) for i in range(5)] + [(5, 0, 7), (6, 0, 7)],
        [(7, 0, 8)] + [(i, 7, 1) for i in range(6, -1, -1)],
    )

    def z_copy(stage, i, j, n):
        return pltpu.make_async_remote_copy(
            src_ref=ZS.at[i, pl.ds(j, n)], dst_ref=ZR.at[i - 1, pl.ds(j, n)],
            send_sem=zssem.at[stage * 7 + i - 1], recv_sem=zrsem.at[stage * 7 + i - 1],
            device_id={"band": ylo * 8 + lax.rem(z + DZ[i], 8)}, device_id_type=MESH)

    def z_send(stage):
        for i, j, n in Z_PARTS[stage]:
            for t in range(j, j + n):
                ZS[i, t] = M[base + block_of(i, t), ylo, xi, yhi]
            if i > 0:
                z_copy(stage, i, j, n).start()

    def z_add(stage):
        for i, j, n in sorted(Z_PARTS[stage]):
            if i > 0:
                z_copy(stage, i, j, n).wait_recv()
                for t in range(j, j + n):
                    at = lax.rem(z + 8 - DZ[i] + DZ[t], 8)
                    TOT[at] = TOT[at] + ZR[i - 1, t]

    arrive(0, 1, 2, 3, 4, 5, 7)

    @pl.when(c == 1)
    def _():
        home_copy.wait_recv()

    send_far(9, 10, 11, 12)
    arrive(6, 8)
    overlap_part(0)
    send_far(13, 14)
    energy_part(0)
    wide_start(0)
    wide_relay(0)
    arrive(9, 11, 10, 12)
    overlap_part(1)
    wide_finish(0)
    energy_part(1)
    wide_start(1)
    thin_finish(0)
    arrive(13, 14)
    overlap_part(2)
    wide_relay(1)
    energy_part(2)
    wide_finish(1)
    wide_start(2)
    thin_finish(1)
    wide_finish(2)
    thin_finish(2)
    for t in range(8):
        TOT[lax.rem(z + DZ[t], 8)] = ZS[0, t]
    for stage in range(3):
        z_add(stage)

    rows = pl.ds(pl.multiple_of(xi * 16 + yhi * 8, 8), 8)
    for j in range(4):
        lo, hi = merge(TOT[2 * j], TOT[2 * j + 1], low8)
        fin[c, rows, j * 128:(j + 1) * 128] = lo
        fin[c, rows, 512 + j * 128:512 + (j + 1) * 128] = hi

    def gather_copy(k):
        px, ph = lax.rem(xi + k // 2, 4), lax.rem(yhi + k, 2)
        return pltpu.make_async_remote_copy(
            src_ref=fin.at[c, rows], dst_ref=fin.at[c, rows],
            send_sem=fssem.at[k - 1], recv_sem=frsem.at[k - 1],
            device_id={"dom": px * 4 + ph * 2 + c}, device_id_type=MESH)

    def swap_copy(k):
        px, ph = lax.rem(xi - k // 2 + 4, 4), lax.rem(yhi + k, 2)
        part = fin.at[c, pl.ds(pl.multiple_of(px * 16 + ph * 8, 8), 8)]
        return pltpu.make_async_remote_copy(
            src_ref=part, dst_ref=part, send_sem=wssem.at[k], recv_sem=wrsem.at[k],
            device_id={"dom": other}, device_id_type=MESH)

    for k in (5, 4, 7, 6, 3, 2, 1):
        gather_copy(k).start()
    swap_copy(0).start()
    for k in range(1, 8):
        gather_copy(k).wait_recv()
        swap_copy(k).start()
    for k in range(8):
        swap_copy(k).wait_recv()

    for stage in range(3):
        pair_copy(stage).wait_send()
        for ring in rings[stage]:
            ring.wait_send()
        for i, j, n in Z_PARTS[stage]:
            if i > 0:
                z_copy(stage, i, j, n).wait_send()
    for k in range(1, 8):
        gather_copy(k).wait_send()
    for k in range(8):
        swap_copy(k).wait_send()
    for o in range(NB - 1):
        main_copy(o).wait_send()
        coef_copy(o).wait_send()
    for o in (*range(9), NB - 1):
        x_copy(o).wait_send()

    @pl.when(c == 0)
    def _():
        home_copy.wait_send()

    @pl.when(c == 1)
    def _():
        for o in range(9, NB - 1):
            x_copy(o).wait_send()
            halo_copy(o).wait_send()


def on_device(wavefunctions, potential, projectors, hamiltonian_correction, delta_s, projector_count):
    vm = pl.BlockSpec(memory_space=pltpu.VMEM)
    hbm = pl.BlockSpec(memory_space=pl.ANY)
    dma = pltpu.SemaphoreType.DMA
    both = pl.pallas_call(
        kernel,
        out_shape=jax.ShapeDtypeStruct((2, 64, 1024), F32),
        in_specs=[hbm, vm, hbm, vm, vm, pl.BlockSpec(memory_space=pltpu.SMEM)],
        out_specs=vm,
        scratch_shapes=[
            pltpu.VMEM((4096, 128), F32),
            pltpu.VMEM((4608, 128), F32),
            pltpu.VMEM((2, 4, 128, 128), F32),
            pltpu.VMEM((128, 2, 4, 2, 8, 128), F32),
            pltpu.VMEM((129 * RPZ, 128), F32),
            pltpu.VMEM((NB, CHUNK, 128), F32),
            pltpu.VMEM((NB, CH, 8, 128), F32),
            pltpu.VMEM((NB, 16, 128), F32),
            pltpu.VMEM((NB, 16, 128), F32),
            pltpu.VMEM((CH, 2, RPZ, 128), F32),
            pltpu.VMEM((512, 128), F32),
            pltpu.VMEM((1024, 512), BF16),
            pltpu.VMEM((1024, 512), BF16),
            pltpu.VMEM((512, 2048), BF16),
            pltpu.VMEM((512, 2048), BF16),
            pltpu.VMEM((1024, 128), BF16),
            pltpu.VMEM((128, 2048), BF16),
            pltpu.VMEM((64, 2, 4, 2, 8, 128), F32),
            pltpu.VMEM((2, 64, 2, 8, 128), F32),
            pltpu.VMEM((2, 2, 64, 2, 8, 128), F32),
            pltpu.VMEM((3, 7, 2, 2, 8, 128), F32),
            pltpu.VMEM((3, 8, 4, 8, 128), F32),
            pltpu.VMEM((3, 64, 8, 128), F32),
            pltpu.VMEM((8, 8, 8, 128), F32),
            pltpu.VMEM((7, 8, 8, 128), F32),
            pltpu.VMEM((8, 8, 128), F32),
            pltpu.VMEM((128, 8, 128), F32),
            dma((2,)),
            dma((NB,)), dma((NB,)), dma((NB,)), dma((NB,)), dma((NB,)), dma((NB,)),
            dma((3,)), dma((3,)), dma((72,)), dma((72,)),
            dma((21,)), dma((21,)), dma((7,)), dma((7,)), dma((8,)), dma((8,)),
            dma((2,)), dma((NB,)),
        ],
        compiler_params=pltpu.CompilerParams(
            collective_id=0, has_side_effects=True, vmem_limit_bytes=60 * 1024 * 1024),
    )(wavefunctions.reshape(4096, 128), potential.reshape(64, 128), projectors.reshape(72 * 64, 128),
      jnp.swapaxes(hamiltonian_correction, 0, 1), jnp.swapaxes(delta_s, 0, 1), projector_count)
    return both[0], both[1]


def solution(mesh):
    placed = (
        P("band", "dom", None, None),
        P("dom", None, None),
        P("dom", None, None, None, None),
        P("dom", None, None),
        P("dom", None, None),
        P("dom"),
    )
    return jax.shard_map(
        on_device, mesh=mesh, in_specs=placed,
        out_specs=(P("band", None), P("band", None)), check_vma=False)
```

```python
import jax
import jax.numpy as jnp
from jax import lax
from jax.experimental import pallas as pl
from jax.experimental.pallas import tpu as pltpu
from jax.sharding import PartitionSpec as P

MESH = pl.DeviceIdType.MESH
F32 = jnp.float32
BF16 = jnp.bfloat16
NB = 16
ND = 16
CH = 8
RPZ = 32
CHUNK = (CH + 1) * RPZ
VOLUME = 1.0 / 131072.0
DZ = (0, 1, 7, 2, 6, 3, 5, 4)
OFFSETS = [(1, 0)] + [(dy, (8 - DZ[p]) % 8) for p in range(1, 8) for dy in (0, 1)]
STAGES = ((0, 5), (5, 7), (7, 8))
START = (0, 25, 49, 64)
HALF = (12, 12, 7)


def block_of(row, col):
    top = max(row, col)
    if top < 5:
        return col * 5 + row
    if top < 7:
        return 25 + col * 2 + row - 5 if col < 5 else 35 + (col - 5) * 7 + row
    return 49 + col if col < 7 else 56 + row


def split(x):
    hi = x.astype(BF16)
    return hi, (x - hi.astype(F32)).astype(BF16)


def dot(a, b):
    return lax.dot_general(a, b, (((1,), (0,)), ((), ())), preferred_element_type=F32)


def dot_exact(a, b):
    return lax.dot_general(a, b, (((1,), (0,)), ((), ())), precision=lax.Precision.HIGHEST,
                           preferred_element_type=F32)


def dot_nt(a, b):
    return lax.dot_general(a, b, (((1,), (1,)), ((), ())), preferred_element_type=F32)


def kernel(psi_in, pot, proj_in, hcor, dels, count, fin,
           psi, proj, SP, M, T, R, RX, CS, CR, VB, AF, AThi, ATlo, Bhi, Blo, ATC, BC, PB,
           F1, F2, FX, FY, G2, ZS, ZR, TOT, HX,
           lsem, ssem, rsem, cssem, crsem, xssem, xrsem, pssem, prsem, gssem, grsem,
           zssem, zrsem, fssem, frsem, wssem, wrsem, hxsem, hsem):
    g = lax.axis_index("band")
    d = lax.axis_index("dom")
    ylo, z = g // 8, lax.rem(g, 8)
    xi, yhi, c = d // 4, lax.rem(d // 2, 2), lax.rem(d, 2)
    y = yhi * 2 + ylo
    dprev = lax.rem(d + ND - 1, ND)
    other = d + 1 - 2 * c

    def peer(o):
        dy, dz = OFFSETS[o]
        return lax.rem(ylo + dy, 2) * 8 + lax.rem(z + dz, 8)

    def source(o):
        dy, dz = OFFSETS[o]
        return lax.rem(ylo + dy, 2) * 8 + lax.rem(z - dz + 8, 8)

    def at_y(q):
        return {"band": lax.rem(q, 2) * 8 + z, "dom": xi * 4 + (q // 2) * 2 + c}

    def at_x(q):
        return {"dom": q * 4 + yhi * 2 + c}

    load_psi = pltpu.make_async_copy(psi_in, psi, lsem.at[0])
    load_proj = pltpu.make_async_copy(proj_in, proj, lsem.at[1])
    load_psi.start()
    load_proj.start()

    barrier = pltpu.get_barrier_semaphore()
    for o in range(NB - 1):
        pl.semaphore_signal(barrier, inc=1, device_id={"band": peer(o)}, device_id_type=MESH)
    for k in range(1, ND):
        pl.semaphore_signal(barrier, inc=1, device_id={"dom": lax.rem(d + k, ND)}, device_id_type=MESH)
    pl.semaphore_signal(barrier, inc=1, device_id={"band": (1 - ylo) * 8 + z, "dom": xi * 4 + (1 - yhi) * 2 + c},
                        device_id_type=MESH)

    load_psi.wait()
    for r in range(RPZ):
        xy = (r // 8) * 16 + r % 8
        a = psi[pl.ds(xy, 64, stride=64), :]
        b = psi[pl.ds(xy + 8, 64, stride=64), :]
        T[pl.ds(r, 128, stride=RPZ), :] = jnp.concatenate([a, b], axis=0).T
    T[pl.ds(128 * RPZ, RPZ), :] = T[pl.ds(0, RPZ), :]

    pl.semaphore_wait(barrier, 31)

    def main_copy(o):
        p = peer(o)
        return pltpu.make_async_remote_copy(
            src_ref=T.at[pl.ds(pl.multiple_of(p * (CH * RPZ), CH * RPZ), CHUNK)],
            dst_ref=R.at[g],
            send_sem=ssem.at[o], recv_sem=rsem.at[o],
            device_id={"band": p}, device_id_type=MESH)

    def coef_copy(o):
        p = peer(o)
        return pltpu.make_async_remote_copy(
            src_ref=CS.at[p], dst_ref=CR.at[g],
            send_sem=cssem.at[o], recv_sem=crsem.at[o],
            device_id={"band": p}, device_id_type=MESH)

    def x_copy(o):
        s = source(o) if o < NB - 1 else g
        return pltpu.make_async_remote_copy(
            src_ref=R.at[s].reshape(CH + 1, RPZ, 128).at[pl.ds(0, CH), pl.ds(0, 8)],
            dst_ref=RX.at[s],
            send_sem=xssem.at[o], recv_sem=xrsem.at[o],
            device_id={"dom": dprev}, device_id_type=MESH)

    home_copy = pltpu.make_async_remote_copy(
        src_ref=T.reshape(129, RPZ, 128).at[pl.ds(0, 128), pl.ds(0, 8)], dst_ref=HX,
        send_sem=hxsem.at[0], recv_sem=hxsem.at[1],
        device_id={"dom": dprev}, device_id_type=MESH)

    def halo_copy(o):
        p = peer(o)
        return pltpu.make_async_remote_copy(
            src_ref=HX.at[pl.ds(pl.multiple_of(p * CH, CH), CH)], dst_ref=RX.at[g],
            send_sem=hsem.at[o], recv_sem=xrsem.at[o],
            device_id={"band": p}, device_id_type=MESH)

    def send_far(*offsets):
        for o in offsets:
            main_copy(o).start()

            @pl.when(c == 1)
            def _():
                halo_copy(o).start()

    for o in range(9):
        main_copy(o).start()

    @pl.when(c == 0)
    def _():
        home_copy.start()

    R[g] = T[pl.ds(pl.multiple_of(g * (CH * RPZ), CH * RPZ), CHUNK), :]

    load_proj.wait()
    def project(t, acc):
        for x in range(4):
            xy = x * 16 + t
            p = jnp.concatenate([psi[pl.ds(xy, 64, stride=64), :], psi[pl.ds(xy + 8, 64, stride=64), :]], axis=1)
            q = jnp.concatenate([proj[pl.ds(xy, 72, stride=64), :], proj[pl.ds(xy + 8, 72, stride=64), :]], axis=1)
            phi, plo = split(p)
            qhi, qlo = split(q)
            acc = acc + dot_nt(qhi, phi) + dot_nt(qhi, plo) + dot_nt(qlo, phi)
        return acc

    acc = lax.fori_loop(0, 8, project, jnp.zeros((72, 64), F32))
    craw = jnp.concatenate([acc, jnp.zeros((56, 64), F32)], axis=0)
    x_copy(NB - 1).start()

    line = lax.broadcasted_iota(jnp.int32, (256, 128), 0)
    slot = lax.broadcasted_iota(jnp.int32, (256, 128), 1)
    spot = (line >> 4) * 5 + (line & 15)
    ext = jnp.where((line & 15) < 5, jnp.where(slot == spot, 1.0, 0.0), 0.0)
    srow = lax.broadcasted_iota(jnp.int32, (128, 128), 0)
    scol = lax.broadcasted_iota(jnp.int32, (128, 128), 1)
    SP[...] = jnp.zeros_like(SP)
    for t, ref in ((1, hcor), (2, dels)):
        inside = jnp.where((line & 15) >= 5 * t, jnp.where((line & 15) < 5 * t + 5, 1.0, 0.0), 0.0)

        for a in range(4):
            SP[t - 1, a, 0:18, 0:18] = ref[:, a, :]

        def couple(a, ext):
            s = SP[t - 1, a]
            s = (0.5 / VOLUME) * (s + s.T)
            used_col = jnp.clip(count[a] - slot, 0, 1).astype(F32)
            used_row = jnp.clip(count[a] - srow, 0, 1).astype(F32)
            left = jnp.where(spot - 5 * t == a * 18 + slot, used_col, 0.0) * inside
            right = jnp.where(scol == a * 18 + srow, used_row, 0.0)
            return ext + dot_exact(dot_exact(left, s), right)

        ext = lax.fori_loop(0, 4, couple, ext)
    chi, clo = split(craw)
    ehi, elo = split(ext)
    msg = dot(ehi, chi) + dot(ehi, clo) + dot(elo, chi)
    msg = jnp.concatenate([msg, msg], axis=1)
    CS[...] = msg.reshape(NB, 16, 128)
    CR[g] = CS[g]
    for o in range(NB - 1):
        coef_copy(o).start()

    v = 3.0 + pltpu.roll(pot[...], lax.rem(128 - g * CH, 128), 1)
    for zi in range(CH):
        wide = jnp.broadcast_to(v[:, zi:zi + 1], (64, 128))
        for half in range(2):
            for x in range(4):
                VB[zi, half, x * 8:(x + 1) * 8, :] = wide[x * 16 + half * 8:x * 16 + half * 8 + 8]

    low = lax.broadcasted_iota(jnp.int32, (RPZ, 128), 1) < 64
    low8 = lax.broadcasted_iota(jnp.int32, (8, 128), 1) < 64
    low16 = lax.broadcasted_iota(jnp.int32, (16, 128), 1) < 64
    last = lax.broadcasted_iota(jnp.int32, (8, 128), 0) == 7
    keep = lax.broadcasted_iota(jnp.int32, (16, 128), 0) < 5

    def merge(a, b, mask):
        return jnp.where(mask, a, pltpu.roll(b, 64, 1)), jnp.where(mask, pltpu.roll(a, 64, 1), b)

    def place(m):
        odd = lax.rem(m, 2)
        dz = odd * ((m + 1) // 2) + (1 - odd) * (8 - m // 2)
        s0 = lax.rem(z + dz, 8)
        at = pl.multiple_of(m * 128, 128)
        return s0, s0 + 8, pl.ds(at, 128), pl.ds(pl.multiple_of(1024 + m * 128, 128), 128)

    def column(s0, s1, zi):
        rows = pl.ds(zi * RPZ, RPZ)
        return merge(R[s0, rows, :], R[s1, rows, :], low)

    def assemble_psi(m, _):
        s0, s1, cols, cols2 = place(m)
        for zi in range(CH):
            now = column(s0, s1, zi)
            for half in range(2):
                rows = pl.ds(half * 256 + zi * RPZ, RPZ)
                AF[rows, :] = now[half]
                hi, lo = split(now[half])
                Bhi[rows, cols2] = hi
                Blo[rows, cols2] = lo
        hi, lo = split(AF[...].T)
        AThi[cols, :] = hi
        ATlo[cols, :] = lo
        cc, _ = merge(CR[s0], CR[s1], low16)
        chi, clo = split(cc)
        chi, clo = chi.astype(F32), clo.astype(F32)
        zero = jnp.zeros((16, 128), F32)
        pad = jnp.zeros((80, 128), F32)
        ahi = jnp.where(keep, chi, zero)
        alo = jnp.where(keep, clo, zero)
        ATC[cols, :] = jnp.concatenate([ahi, ahi, alo, pad], axis=0).T.astype(BF16)
        for t, at in ((1, cols), (2, cols2)):
            bhi = jnp.where(keep, pltpu.roll(chi, 16 - 5 * t, 0), zero)
            blo = jnp.where(keep, pltpu.roll(clo, 16 - 5 * t, 0), zero)
            BC[:, at] = jnp.concatenate([bhi, blo, bhi, pad], axis=0).astype(BF16)
        return 0

    def assemble_h(m, _):
        s0, s1, cols, _ = place(m)
        now = column(s0, s1, 0)
        for zi in range(CH):
            nxt = column(s0, s1, zi + 1)
            halo = merge(RX[s0, zi], RX[s1, zi], low8)
            turned = []
            for half in range(2):
                turned.append([pltpu.roll(now[half][x * 8:(x + 1) * 8], 7, 0) for x in range(4)])
            for half in range(2):
                a = now[half]
                ax = jnp.concatenate([a[8:], halo[half]], axis=0)
                ay = jnp.concatenate(
                    [jnp.where(last, turned[1 - half][x], turned[half][x]) for x in range(4)], axis=0)
                h = VB[zi, half] * a - ax - ay - nxt[half]
                rows = pl.ds(half * 256 + zi * RPZ, RPZ)
                hi, lo = split(h)
                Bhi[rows, cols] = hi
                Blo[rows, cols] = lo
            now = nxt
        return 0

    def product(mat, row, n, col, m, at, down, right):
        rows = pl.ds(pl.multiple_of(row * 128, 128), n * 128)
        cols = pl.ds(pl.multiple_of(mat * 1024 + col * 128, 128), m * 128)
        a = AThi[rows, :]
        res = dot(a, Bhi[:, cols]) + dot(a, Blo[:, cols]) + dot(ATlo[rows, :], Bhi[:, cols]) \
            + dot(ATC[rows, :], BC[:, cols])
        res = res * VOLUME
        for r in range(n):
            for k in range(m):
                M[mat * 64 + at + r * down + k * right] = \
                    res[r * 128:(r + 1) * 128, k * 128:(k + 1) * 128].reshape(2, 4, 2, 8, 128)

    def loop(count_, body):
        def step(t, _):
            body(t)
            return 0
        lax.fori_loop(0, count_, step, 0)

    def even(k, l):
        s = 0.5 * (M[k].reshape(128, 128) + M[l].reshape(128, 128).T)
        M[k] = s.reshape(2, 4, 2, 8, 128)
        M[l] = s.T.reshape(2, 4, 2, 8, 128)

    def products(stage, mat):
        if stage == 0:
            loop(4, lambda t: product(mat, (t // 2) * 2, 2, lax.rem(t, 2) * 2, 2,
                                      lax.rem(t, 2) * 10 + (t // 2) * 2, 1, 5))
            loop(2, lambda t: product(mat, 4, 1, 2 * t, 2, 10 * t + 4, 1, 5))
            loop(2, lambda t: product(mat, 2 * t, 2, 4, 1, 20 + 2 * t, 1, 5))
            product(mat, 4, 1, 4, 1, 24, 1, 5)
        elif stage == 1:
            loop(3, lambda t: product(mat, 2 * t, 2, 5, 2, 35 + 2 * t, 1, 7))
            product(mat, 6, 1, 5, 2, 41, 1, 7)
            loop(2, lambda t: product(mat, 5, 2, 2 * t, 2, 25 + 4 * t, 1, 2))
            product(mat, 5, 2, 4, 1, 33, 1, 2)
        else:
            loop(4, lambda t: product(mat, 2 * t, 2, 7, 1, 56 + 2 * t, 1, 1))
            loop(3, lambda t: product(mat, 7, 1, 2 * t, 2, 49 + 2 * t, 1, 1))
            product(mat, 7, 1, 6, 1, 55, 1, 1)

    def evens(stage):
        if stage == 0:
            def pair(t):
                i, j = t // 5, lax.rem(t, 5)

                @pl.when(i <= j)
                def _():
                    even(j * 5 + i, i * 5 + j)
            loop(25, pair)
        elif stage == 1:
            loop(10, lambda t: even(35 + (t // 5) * 7 + lax.rem(t, 5), 25 + lax.rem(t, 5) * 2 + t // 5))
            for i, j in ((5, 5), (5, 6), (6, 6)):
                even(block_of(i, j), block_of(j, i))
        else:
            loop(7, lambda t: even(56 + t, 49 + t))
            even(63, 63)

    def pair_copy(stage):
        k0, n = START[stage], START[stage + 1] - START[stage]
        return pltpu.make_async_remote_copy(
            src_ref=M.at[pl.ds((1 - c) * 64 + k0, n)], dst_ref=PB.at[pl.ds(k0, n)],
            send_sem=pssem.at[stage], recv_sem=prsem.at[stage],
            device_id={"dom": other}, device_id_type=MESH)

    base = c * 64

    def add_pair(stage):
        pair_copy(stage).wait_recv()

        def body(t):
            M[base + START[stage] + t] = M[base + START[stage] + t] + PB[START[stage] + t]
        loop(START[stage + 1] - START[stage], body)

    class Ring:
        def __init__(self, me, at, piece, first, second, number):
            self.me, self.piece, self.first, self.second = me, piece, first, second
            self.plus, self.minus = at(lax.rem(me + 1, 4)), at(lax.rem(me + 3, 4))
            self.number = number

        def copy(self, k):
            me = self.me
            q, h, buf, way = (
                (me + 2, 0, self.first(0), self.plus),
                (me + 2, 1, self.first(1), self.minus),
                (me + 1, 1, self.second(0, 1), self.plus),
                (me + 3, 0, self.second(1, 0), self.minus),
                (me + 1, 0, self.second(0, 0), self.plus),
                (me + 3, 1, self.second(1, 1), self.minus),
            )[k]
            return pltpu.make_async_remote_copy(
                src_ref=M.at[self.piece(lax.rem(q, 4), h)], dst_ref=buf,
                send_sem=gssem.at[self.number + k], recv_sem=grsem.at[self.number + k],
                device_id=way, device_id_type=MESH)

        def start(self):
            for k in range(4):
                self.copy(k).start()

        def add(self, q, h, *bufs):
            at = self.piece(lax.rem(q, 4), h)
            total = M[at]
            for b in bufs:
                total = total + b[...]
            M[at] = total

        def relay(self):
            self.copy(0).wait_recv()
            self.add(self.me + 1, 0, self.first(0))
            self.copy(4).start()
            self.copy(1).wait_recv()
            self.add(self.me + 3, 1, self.first(1))
            self.copy(5).start()

        def finish(self):
            for k in range(2, 6):
                self.copy(k).wait_recv()
            for h in range(2):
                self.add(self.me, h, self.second(0, h), self.second(1, h))

        def wait_send(self):
            for k in range(6):
                self.copy(k).wait_send()

    class Direct:
        def __init__(self, me, at, piece, buf, number):
            self.me, self.at, self.piece, self.buf, self.number = me, at, piece, buf, number

        def copy(self, k):
            q = lax.rem(self.me + k, 4)
            return pltpu.make_async_remote_copy(
                src_ref=M.at[self.piece(q)], dst_ref=self.buf(k - 1),
                send_sem=gssem.at[self.number + k - 1], recv_sem=grsem.at[self.number + k - 1],
                device_id=self.at(q), device_id_type=MESH)

        def start(self):
            for k in (2, 1, 3):
                self.copy(k).start()

        def finish(self):
            at = self.piece(self.me)
            total = M[at]
            for k in (1, 3, 2):
                self.copy(k).wait_recv()
                total = total + self.buf(k - 1)[...]
            M[at] = total

        def wait_send(self):
            for k in range(1, 4):
                self.copy(k).wait_send()

    rings = []
    full = slice(None)
    for stage in range(3):
        k0, n = START[stage], START[stage + 1] - START[stage]
        na = HALF[stage]
        nb = n - na
        kb = k0 + na

        def ax_piece(q, h, k0=k0, na=na):
            return (pl.ds(base + k0, na), h, q)

        def by_piece(q, h, kb=kb, nb=nb):
            return (pl.ds(base + kb, nb), lax.rem(q, 2), pl.ds(2 * h, 2), q // 2)

        def ax_whole(q, k0=k0, na=na):
            return (pl.ds(base + k0, na), full, q)

        def by_whole(q, kb=kb, nb=nb):
            return (pl.ds(base + kb, nb), lax.rem(q, 2), full, q // 2)

        def ay_piece(q, k0=k0, na=na):
            return (pl.ds(base + k0, na), lax.rem(q, 2), xi, q // 2)

        def bx_piece(q, kb=kb, nb=nb):
            return (pl.ds(base + kb, nb), ylo, q, yhi)

        def wide_first(k, n):
            return lambda h: F1.at[h, pl.ds(k, n)]

        def wide_second(k, n):
            return lambda w, h: F2.at[w, h, pl.ds(k, n)]

        def thin(k, n):
            return lambda i: G2.at[i, pl.ds(k, n)]

        number = stage * 24
        if stage < 2:
            wide = (Ring(xi, at_x, ax_piece, wide_first(k0, na), wide_second(k0, na), number),
                    Ring(y, at_y, by_piece, wide_first(kb, nb), wide_second(kb, nb), number + 6))
        else:
            wide = (Direct(xi, at_x, ax_whole, lambda i: FX.at[i], number),
                    Direct(y, at_y, by_whole, lambda i: FY.at[i], number + 6))
        rings.append(wide + (
            Direct(y, at_y, ay_piece, thin(k0, na), number + 12),
            Direct(xi, at_x, bx_piece, thin(kb, nb), number + 18),
        ))

    def arrive(*offsets):
        for o in offsets:
            main_copy(o).wait_recv()
            if o < 9:
                x_copy(o).start()
            else:
                @pl.when(c == 1)
                def _():
                    x_copy(o).start()

    def overlap_part(stage):
        first, last_ = STAGES[stage]
        for o in ((0,) if stage == 0 else ()) + tuple(range(max(1, 2 * first - 1), 2 * last_ - 1)):
            coef_copy(o).wait_recv()
        lax.fori_loop(first, last_, assemble_psi, 0)
        products(stage, 1)

        @pl.when(c == 0)
        def _():
            pair_copy(stage).start()

    def energy_part(stage):
        first, last_ = STAGES[stage]
        for o in ((NB - 1, 0) if stage == 0 else ()) + tuple(range(max(1, 2 * first - 1), 2 * last_ - 1)):
            x_copy(o).wait_recv()
        lax.fori_loop(first, last_, assemble_h, 0)
        products(stage, 0)
        evens(stage)

        @pl.when(c == 1)
        def _():
            pair_copy(stage).start()

    def wide_start(stage):
        add_pair(stage)
        rings[stage][0].start()
        rings[stage][1].start()

    def wide_relay(stage):
        rings[stage][0].relay()
        rings[stage][1].relay()

    def wide_finish(stage):
        rings[stage][0].finish()
        rings[stage][2].start()
        rings[stage][1].finish()
        rings[stage][3].start()

    def thin_finish(stage):
        rings[stage][2].finish()
        rings[stage][3].finish()
        z_send(stage)

    Z_PARTS = (
        [(i, 0, 5) for i in range(5)],
        [(i, 5, 2) for i in range(5)] + [(5, 0, 7), (6, 0, 7)],
        [(7, 0, 8)] + [(i, 7, 1) for i in range(6, -1, -1)],
    )

    def z_copy(stage, i, j, n):
        return pltpu.make_async_remote_copy(
            src_ref=ZS.at[i, pl.ds(j, n)], dst_ref=ZR.at[i - 1, pl.ds(j, n)],
            send_sem=zssem.at[stage * 7 + i - 1], recv_sem=zrsem.at[stage * 7 + i - 1],
            device_id={"band": ylo * 8 + lax.rem(z + DZ[i], 8)}, device_id_type=MESH)

    def z_send(stage):
        for i, j, n in Z_PARTS[stage]:
            for t in range(j, j + n):
                ZS[i, t] = M[base + block_of(i, t), ylo, xi, yhi]
            if i > 0:
                z_copy(stage, i, j, n).start()

    def z_add(stage):
        for i, j, n in sorted(Z_PARTS[stage]):
            if i > 0:
                z_copy(stage, i, j, n).wait_recv()
                for t in range(j, j + n):
                    at = lax.rem(z + 8 - DZ[i] + DZ[t], 8)
                    TOT[at] = TOT[at] + ZR[i - 1, t]

    arrive(0, 1, 2, 3, 4, 5, 7)

    @pl.when(c == 1)
    def _():
        home_copy.wait_recv()

    send_far(9, 10, 11, 12)
    arrive(6, 8)
    overlap_part(0)
    energy_part(0)
    send_far(13, 14)
    wide_start(0)
    wide_relay(0)
    arrive(9, 11, 10, 12)
    overlap_part(1)
    wide_finish(0)
    energy_part(1)
    wide_start(1)
    thin_finish(0)
    wide_relay(1)
    arrive(13, 14)
    overlap_part(2)
    wide_finish(1)
    energy_part(2)
    wide_start(2)
    thin_finish(1)
    wide_finish(2)
    thin_finish(2)
    for t in range(8):
        TOT[lax.rem(z + DZ[t], 8)] = ZS[0, t]
    for stage in range(3):
        z_add(stage)

    rows = pl.ds(pl.multiple_of(xi * 16 + yhi * 8, 8), 8)
    for j in range(4):
        lo, hi = merge(TOT[2 * j], TOT[2 * j + 1], low8)
        fin[c, rows, j * 128:(j + 1) * 128] = lo
        fin[c, rows, 512 + j * 128:512 + (j + 1) * 128] = hi

    def gather_copy(k):
        px, ph = lax.rem(xi + k // 2, 4), lax.rem(yhi + k, 2)
        return pltpu.make_async_remote_copy(
            src_ref=fin.at[c, rows], dst_ref=fin.at[c, rows],
            send_sem=fssem.at[k - 1], recv_sem=frsem.at[k - 1],
            device_id={"dom": px * 4 + ph * 2 + c}, device_id_type=MESH)

    def swap_copy(k):
        px, ph = lax.rem(xi - k // 2 + 4, 4), lax.rem(yhi + k, 2)
        part = fin.at[c, pl.ds(pl.multiple_of(px * 16 + ph * 8, 8), 8)]
        return pltpu.make_async_remote_copy(
            src_ref=part, dst_ref=part, send_sem=wssem.at[k], recv_sem=wrsem.at[k],
            device_id={"dom": other}, device_id_type=MESH)

    for k in (5, 4, 7, 6, 3, 2, 1):
        gather_copy(k).start()
    swap_copy(0).start()
    for k in range(1, 8):
        gather_copy(k).wait_recv()
        swap_copy(k).start()
    for k in range(8):
        swap_copy(k).wait_recv()

    for stage in range(3):
        pair_copy(stage).wait_send()
        for ring in rings[stage]:
            ring.wait_send()
        for i, j, n in Z_PARTS[stage]:
            if i > 0:
                z_copy(stage, i, j, n).wait_send()
    for k in range(1, 8):
        gather_copy(k).wait_send()
    for k in range(8):
        swap_copy(k).wait_send()
    for o in range(NB - 1):
        main_copy(o).wait_send()
        coef_copy(o).wait_send()
    for o in (*range(9), NB - 1):
        x_copy(o).wait_send()

    @pl.when(c == 0)
    def _():
        home_copy.wait_send()

    @pl.when(c == 1)
    def _():
        for o in range(9, NB - 1):
            x_copy(o).wait_send()
            halo_copy(o).wait_send()


def on_device(wavefunctions, potential, projectors, hamiltonian_correction, delta_s, projector_count):
    vm = pl.BlockSpec(memory_space=pltpu.VMEM)
    hbm = pl.BlockSpec(memory_space=pl.ANY)
    dma = pltpu.SemaphoreType.DMA
    both = pl.pallas_call(
        kernel,
        out_shape=jax.ShapeDtypeStruct((2, 64, 1024), F32),
        in_specs=[hbm, vm, hbm, vm, vm, pl.BlockSpec(memory_space=pltpu.SMEM)],
        out_specs=vm,
        scratch_shapes=[
            pltpu.VMEM((4096, 128), F32),
            pltpu.VMEM((4608, 128), F32),
            pltpu.VMEM((2, 4, 128, 128), F32),
            pltpu.VMEM((128, 2, 4, 2, 8, 128), F32),
            pltpu.VMEM((129 * RPZ, 128), F32),
            pltpu.VMEM((NB, CHUNK, 128), F32),
            pltpu.VMEM((NB, CH, 8, 128), F32),
            pltpu.VMEM((NB, 16, 128), F32),
            pltpu.VMEM((NB, 16, 128), F32),
            pltpu.VMEM((CH, 2, RPZ, 128), F32),
            pltpu.VMEM((512, 128), F32),
            pltpu.VMEM((1024, 512), BF16),
            pltpu.VMEM((1024, 512), BF16),
            pltpu.VMEM((512, 2048), BF16),
            pltpu.VMEM((512, 2048), BF16),
            pltpu.VMEM((1024, 128), BF16),
            pltpu.VMEM((128, 2048), BF16),
            pltpu.VMEM((64, 2, 4, 2, 8, 128), F32),
            pltpu.VMEM((2, 64, 2, 8, 128), F32),
            pltpu.VMEM((2, 2, 64, 2, 8, 128), F32),
            pltpu.VMEM((3, 7, 2, 2, 8, 128), F32),
            pltpu.VMEM((3, 8, 4, 8, 128), F32),
            pltpu.VMEM((3, 64, 8, 128), F32),
            pltpu.VMEM((8, 8, 8, 128), F32),
            pltpu.VMEM((7, 8, 8, 128), F32),
            pltpu.VMEM((8, 8, 128), F32),
            pltpu.VMEM((128, 8, 128), F32),
            dma((2,)),
            dma((NB,)), dma((NB,)), dma((NB,)), dma((NB,)), dma((NB,)), dma((NB,)),
            dma((3,)), dma((3,)), dma((72,)), dma((72,)),
            dma((21,)), dma((21,)), dma((7,)), dma((7,)), dma((8,)), dma((8,)),
            dma((2,)), dma((NB,)),
        ],
        compiler_params=pltpu.CompilerParams(
            collective_id=0, has_side_effects=True, vmem_limit_bytes=60 * 1024 * 1024),
    )(wavefunctions.reshape(4096, 128), potential.reshape(64, 128), projectors.reshape(72 * 64, 128),
      jnp.swapaxes(hamiltonian_correction, 0, 1), jnp.swapaxes(delta_s, 0, 1), projector_count)
    return both[0], both[1]


def solution(mesh):
    placed = (
        P("band", "dom", None, None),
        P("dom", None, None),
        P("dom", None, None, None, None),
        P("dom", None, None),
        P("dom", None, None),
        P("dom"),
    )
    return jax.shard_map(
        on_device, mesh=mesh, in_specs=placed,
        out_specs=(P("band", None), P("band", None)), check_vma=False)
```

```python
import jax
import jax.numpy as jnp
from jax import lax
from jax.experimental import pallas as pl
from jax.experimental.pallas import tpu as pltpu
from jax.sharding import PartitionSpec as P

MESH = pl.DeviceIdType.MESH
F32 = jnp.float32
BF16 = jnp.bfloat16
NB = 16
ND = 16
CH = 8
RPZ = 32
CHUNK = (CH + 1) * RPZ
VOLUME = 1.0 / 131072.0
DZ = (0, 1, 7, 2, 6, 3, 5, 4)
OFFSETS = [(1, 0)] + [(dy, (8 - DZ[p]) % 8) for p in range(1, 8) for dy in (0, 1)]
STAGES = ((0, 5), (5, 7), (7, 8))
START = (0, 25, 49, 64)
HALF = (12, 12, 7)


def block_of(row, col):
    top = max(row, col)
    if top < 5:
        return col * 5 + row
    if top < 7:
        return 25 + col * 2 + row - 5 if col < 5 else 35 + (col - 5) * 7 + row
    return 49 + col if col < 7 else 56 + row


def split(x):
    hi = x.astype(BF16)
    return hi, (x - hi.astype(F32)).astype(BF16)


def dot(a, b):
    return lax.dot_general(a, b, (((1,), (0,)), ((), ())), preferred_element_type=F32)


def dot_exact(a, b):
    return lax.dot_general(a, b, (((1,), (0,)), ((), ())), precision=lax.Precision.HIGHEST,
                           preferred_element_type=F32)


def dot_nt(a, b):
    return lax.dot_general(a, b, (((1,), (1,)), ((), ())), preferred_element_type=F32)


def kernel(psi_in, pot, proj_in, hcor, dels, count, fin,
           psi, proj, SP, M, T, R, RX, CS, CR, VB, AF, AThi, ATlo, Bhi, Blo, ATC, BC, PB,
           F1, F2, FX, FY, G2, ZS, ZR, TOT,
           lsem, ssem, rsem, cssem, crsem, xssem, xrsem, pssem, prsem, gssem, grsem,
           zssem, zrsem, fssem, frsem, wssem, wrsem):
    g = lax.axis_index("band")
    d = lax.axis_index("dom")
    ylo, z = g // 8, lax.rem(g, 8)
    xi, yhi, c = d // 4, lax.rem(d // 2, 2), lax.rem(d, 2)
    y = yhi * 2 + ylo
    dprev = lax.rem(d + ND - 1, ND)
    other = d + 1 - 2 * c

    def peer(o):
        dy, dz = OFFSETS[o]
        return lax.rem(ylo + dy, 2) * 8 + lax.rem(z + dz, 8)

    def source(o):
        dy, dz = OFFSETS[o]
        return lax.rem(ylo + dy, 2) * 8 + lax.rem(z - dz + 8, 8)

    def at_y(q):
        return {"band": lax.rem(q, 2) * 8 + z, "dom": xi * 4 + (q // 2) * 2 + c}

    def at_x(q):
        return {"dom": q * 4 + yhi * 2 + c}

    load_psi = pltpu.make_async_copy(psi_in, psi, lsem.at[0])
    load_proj = pltpu.make_async_copy(proj_in, proj, lsem.at[1])
    load_psi.start()
    load_proj.start()

    barrier = pltpu.get_barrier_semaphore()
    for o in range(NB - 1):
        pl.semaphore_signal(barrier, inc=1, device_id={"band": peer(o)}, device_id_type=MESH)
    for k in range(1, ND):
        pl.semaphore_signal(barrier, inc=1, device_id={"dom": lax.rem(d + k, ND)}, device_id_type=MESH)
    pl.semaphore_signal(barrier, inc=1, device_id={"band": (1 - ylo) * 8 + z, "dom": xi * 4 + (1 - yhi) * 2 + c},
                        device_id_type=MESH)

    load_psi.wait()
    for r in range(RPZ):
        xy = (r // 8) * 16 + r % 8
        a = psi[pl.ds(xy, 64, stride=64), :]
        b = psi[pl.ds(xy + 8, 64, stride=64), :]
        T[pl.ds(r, 128, stride=RPZ), :] = jnp.concatenate([a, b], axis=0).T
    T[pl.ds(128 * RPZ, RPZ), :] = T[pl.ds(0, RPZ), :]

    pl.semaphore_wait(barrier, 31)

    def main_copy(o):
        p = peer(o)
        return pltpu.make_async_remote_copy(
            src_ref=T.at[pl.ds(pl.multiple_of(p * (CH * RPZ), CH * RPZ), CHUNK)],
            dst_ref=R.at[g],
            send_sem=ssem.at[o], recv_sem=rsem.at[o],
            device_id={"band": p}, device_id_type=MESH)

    def coef_copy(o):
        p = peer(o)
        return pltpu.make_async_remote_copy(
            src_ref=CS.at[p], dst_ref=CR.at[g],
            send_sem=cssem.at[o], recv_sem=crsem.at[o],
            device_id={"band": p}, device_id_type=MESH)

    def x_copy(o):
        s = source(o) if o < NB - 1 else g
        return pltpu.make_async_remote_copy(
            src_ref=R.at[s].reshape(CH + 1, RPZ, 128).at[pl.ds(0, CH), pl.ds(0, 8)],
            dst_ref=RX.at[s],
            send_sem=xssem.at[o], recv_sem=xrsem.at[o],
            device_id={"dom": dprev}, device_id_type=MESH)

    for o in range(9):
        main_copy(o).start()

    R[g] = T[pl.ds(pl.multiple_of(g * (CH * RPZ), CH * RPZ), CHUNK), :]

    load_proj.wait()
    def project(t, acc):
        for x in range(4):
            xy = x * 16 + t
            p = jnp.concatenate([psi[pl.ds(xy, 64, stride=64), :], psi[pl.ds(xy + 8, 64, stride=64), :]], axis=1)
            q = jnp.concatenate([proj[pl.ds(xy, 72, stride=64), :], proj[pl.ds(xy + 8, 72, stride=64), :]], axis=1)
            phi, plo = split(p)
            qhi, qlo = split(q)
            acc = acc + dot_nt(qhi, phi) + dot_nt(qhi, plo) + dot_nt(qlo, phi)
        return acc

    acc = lax.fori_loop(0, 8, project, jnp.zeros((72, 64), F32))
    craw = jnp.concatenate([acc, jnp.zeros((56, 64), F32)], axis=0)
    x_copy(NB - 1).start()

    line = lax.broadcasted_iota(jnp.int32, (256, 128), 0)
    slot = lax.broadcasted_iota(jnp.int32, (256, 128), 1)
    spot = (line >> 4) * 5 + (line & 15)
    ext = jnp.where((line & 15) < 5, jnp.where(slot == spot, 1.0, 0.0), 0.0)
    srow = lax.broadcasted_iota(jnp.int32, (128, 128), 0)
    scol = lax.broadcasted_iota(jnp.int32, (128, 128), 1)
    SP[...] = jnp.zeros_like(SP)
    for t, ref in ((1, hcor), (2, dels)):
        inside = jnp.where((line & 15) >= 5 * t, jnp.where((line & 15) < 5 * t + 5, 1.0, 0.0), 0.0)

        for a in range(4):
            SP[t - 1, a, 0:18, 0:18] = ref[:, a, :]

        def couple(a, ext):
            s = SP[t - 1, a]
            s = (0.5 / VOLUME) * (s + s.T)
            used_col = jnp.clip(count[a] - slot, 0, 1).astype(F32)
            used_row = jnp.clip(count[a] - srow, 0, 1).astype(F32)
            left = jnp.where(spot - 5 * t == a * 18 + slot, used_col, 0.0) * inside
            right = jnp.where(scol == a * 18 + srow, used_row, 0.0)
            return ext + dot_exact(dot_exact(left, s), right)

        ext = lax.fori_loop(0, 4, couple, ext)
    chi, clo = split(craw)
    ehi, elo = split(ext)
    msg = dot(ehi, chi) + dot(ehi, clo) + dot(elo, chi)
    msg = jnp.concatenate([msg, msg], axis=1)
    CS[...] = msg.reshape(NB, 16, 128)
    CR[g] = CS[g]
    for o in range(NB - 1):
        coef_copy(o).start()
    for o in (10, 12):
        main_copy(o).start()

    v = 3.0 + pltpu.roll(pot[...], lax.rem(128 - g * CH, 128), 1)
    for zi in range(CH):
        wide = jnp.broadcast_to(v[:, zi:zi + 1], (64, 128))
        for half in range(2):
            for x in range(4):
                VB[zi, half, x * 8:(x + 1) * 8, :] = wide[x * 16 + half * 8:x * 16 + half * 8 + 8]

    low = lax.broadcasted_iota(jnp.int32, (RPZ, 128), 1) < 64
    low8 = lax.broadcasted_iota(jnp.int32, (8, 128), 1) < 64
    low16 = lax.broadcasted_iota(jnp.int32, (16, 128), 1) < 64
    last = lax.broadcasted_iota(jnp.int32, (8, 128), 0) == 7
    keep = lax.broadcasted_iota(jnp.int32, (16, 128), 0) < 5

    def merge(a, b, mask):
        return jnp.where(mask, a, pltpu.roll(b, 64, 1)), jnp.where(mask, pltpu.roll(a, 64, 1), b)

    def place(m):
        odd = lax.rem(m, 2)
        dz = odd * ((m + 1) // 2) + (1 - odd) * (8 - m // 2)
        s0 = lax.rem(z + dz, 8)
        at = pl.multiple_of(m * 128, 128)
        return s0, s0 + 8, pl.ds(at, 128), pl.ds(pl.multiple_of(1024 + m * 128, 128), 128)

    def column(s0, s1, zi):
        rows = pl.ds(zi * RPZ, RPZ)
        return merge(R[s0, rows, :], R[s1, rows, :], low)

    def assemble_psi(m, _):
        s0, s1, cols, cols2 = place(m)
        for zi in range(CH):
            now = column(s0, s1, zi)
            for half in range(2):
                rows = pl.ds(half * 256 + zi * RPZ, RPZ)
                AF[rows, :] = now[half]
                hi, lo = split(now[half])
                Bhi[rows, cols2] = hi
                Blo[rows, cols2] = lo
        hi, lo = split(AF[...].T)
        AThi[cols, :] = hi
        ATlo[cols, :] = lo
        cc, _ = merge(CR[s0], CR[s1], low16)
        chi, clo = split(cc)
        chi, clo = chi.astype(F32), clo.astype(F32)
        zero = jnp.zeros((16, 128), F32)
        pad = jnp.zeros((80, 128), F32)
        ahi = jnp.where(keep, chi, zero)
        alo = jnp.where(keep, clo, zero)
        ATC[cols, :] = jnp.concatenate([ahi, ahi, alo, pad], axis=0).T.astype(BF16)
        for t, at in ((1, cols), (2, cols2)):
            bhi = jnp.where(keep, pltpu.roll(chi, 16 - 5 * t, 0), zero)
            blo = jnp.where(keep, pltpu.roll(clo, 16 - 5 * t, 0), zero)
            BC[:, at] = jnp.concatenate([bhi, blo, bhi, pad], axis=0).astype(BF16)
        return 0

    def assemble_h(m, _):
        s0, s1, cols, _ = place(m)
        now = column(s0, s1, 0)
        for zi in range(CH):
            nxt = column(s0, s1, zi + 1)
            halo = merge(RX[s0, zi], RX[s1, zi], low8)
            turned = []
            for half in range(2):
                turned.append([pltpu.roll(now[half][x * 8:(x + 1) * 8], 7, 0) for x in range(4)])
            for half in range(2):
                a = now[half]
                ax = jnp.concatenate([a[8:], halo[half]], axis=0)
                ay = jnp.concatenate(
                    [jnp.where(last, turned[1 - half][x], turned[half][x]) for x in range(4)], axis=0)
                h = VB[zi, half] * a - ax - ay - nxt[half]
                rows = pl.ds(half * 256 + zi * RPZ, RPZ)
                hi, lo = split(h)
                Bhi[rows, cols] = hi
                Blo[rows, cols] = lo
            now = nxt
        return 0

    def product(mat, row, n, col, m, at, down, right):
        rows = pl.ds(pl.multiple_of(row * 128, 128), n * 128)
        cols = pl.ds(pl.multiple_of(mat * 1024 + col * 128, 128), m * 128)
        a = AThi[rows, :]
        res = dot(a, Bhi[:, cols]) + dot(a, Blo[:, cols]) + dot(ATlo[rows, :], Bhi[:, cols]) \
            + dot(ATC[rows, :], BC[:, cols])
        res = res * VOLUME
        for r in range(n):
            for k in range(m):
                M[mat * 64 + at + r * down + k * right] = \
                    res[r * 128:(r + 1) * 128, k * 128:(k + 1) * 128].reshape(2, 4, 2, 8, 128)

    def loop(count_, body):
        def step(t, _):
            body(t)
            return 0
        lax.fori_loop(0, count_, step, 0)

    def even(k, l):
        s = 0.5 * (M[k].reshape(128, 128) + M[l].reshape(128, 128).T)
        M[k] = s.reshape(2, 4, 2, 8, 128)
        M[l] = s.T.reshape(2, 4, 2, 8, 128)

    def products(stage, mat):
        if stage == 0:
            loop(4, lambda t: product(mat, (t // 2) * 2, 2, lax.rem(t, 2) * 2, 2,
                                      lax.rem(t, 2) * 10 + (t // 2) * 2, 1, 5))
            loop(2, lambda t: product(mat, 4, 1, 2 * t, 2, 10 * t + 4, 1, 5))
            loop(2, lambda t: product(mat, 2 * t, 2, 4, 1, 20 + 2 * t, 1, 5))
            product(mat, 4, 1, 4, 1, 24, 1, 5)
        elif stage == 1:
            loop(3, lambda t: product(mat, 2 * t, 2, 5, 2, 35 + 2 * t, 1, 7))
            product(mat, 6, 1, 5, 2, 41, 1, 7)
            loop(2, lambda t: product(mat, 5, 2, 2 * t, 2, 25 + 4 * t, 1, 2))
            product(mat, 5, 2, 4, 1, 33, 1, 2)
        else:
            loop(4, lambda t: product(mat, 2 * t, 2, 7, 1, 56 + 2 * t, 1, 1))
            loop(3, lambda t: product(mat, 7, 1, 2 * t, 2, 49 + 2 * t, 1, 1))
            product(mat, 7, 1, 6, 1, 55, 1, 1)

    def evens(stage):
        if stage == 0:
            def pair(t):
                i, j = t // 5, lax.rem(t, 5)

                @pl.when(i <= j)
                def _():
                    even(j * 5 + i, i * 5 + j)
            loop(25, pair)
        elif stage == 1:
            loop(10, lambda t: even(35 + (t // 5) * 7 + lax.rem(t, 5), 25 + lax.rem(t, 5) * 2 + t // 5))
            for i, j in ((5, 5), (5, 6), (6, 6)):
                even(block_of(i, j), block_of(j, i))
        else:
            loop(7, lambda t: even(56 + t, 49 + t))
            even(63, 63)

    def pair_copy(stage):
        k0, n = START[stage], START[stage + 1] - START[stage]
        return pltpu.make_async_remote_copy(
            src_ref=M.at[pl.ds((1 - c) * 64 + k0, n)], dst_ref=PB.at[pl.ds(k0, n)],
            send_sem=pssem.at[stage], recv_sem=prsem.at[stage],
            device_id={"dom": other}, device_id_type=MESH)

    base = c * 64

    def add_pair(stage):
        pair_copy(stage).wait_recv()

        def body(t):
            M[base + START[stage] + t] = M[base + START[stage] + t] + PB[START[stage] + t]
        loop(START[stage + 1] - START[stage], body)

    class Ring:
        def __init__(self, me, at, piece, first, second, number):
            self.me, self.piece, self.first, self.second = me, piece, first, second
            self.plus, self.minus = at(lax.rem(me + 1, 4)), at(lax.rem(me + 3, 4))
            self.number = number

        def copy(self, k):
            me = self.me
            q, h, buf, way = (
                (me + 2, 0, self.first(0), self.plus),
                (me + 2, 1, self.first(1), self.minus),
                (me + 1, 1, self.second(0, 1), self.plus),
                (me + 3, 0, self.second(1, 0), self.minus),
                (me + 1, 0, self.second(0, 0), self.plus),
                (me + 3, 1, self.second(1, 1), self.minus),
            )[k]
            return pltpu.make_async_remote_copy(
                src_ref=M.at[self.piece(lax.rem(q, 4), h)], dst_ref=buf,
                send_sem=gssem.at[self.number + k], recv_sem=grsem.at[self.number + k],
                device_id=way, device_id_type=MESH)

        def start(self):
            for k in range(4):
                self.copy(k).start()

        def add(self, q, h, *bufs):
            at = self.piece(lax.rem(q, 4), h)
            total = M[at]
            for b in bufs:
                total = total + b[...]
            M[at] = total

        def relay(self):
            self.copy(0).wait_recv()
            self.add(self.me + 1, 0, self.first(0))
            self.copy(4).start()
            self.copy(1).wait_recv()
            self.add(self.me + 3, 1, self.first(1))
            self.copy(5).start()

        def finish(self):
            for k in range(2, 6):
                self.copy(k).wait_recv()
            for h in range(2):
                self.add(self.me, h, self.second(0, h), self.second(1, h))

        def wait_send(self):
            for k in range(6):
                self.copy(k).wait_send()

    class Direct:
        def __init__(self, me, at, piece, buf, number):
            self.me, self.at, self.piece, self.buf, self.number = me, at, piece, buf, number

        def copy(self, k):
            q = lax.rem(self.me + k, 4)
            return pltpu.make_async_remote_copy(
                src_ref=M.at[self.piece(q)], dst_ref=self.buf(k - 1),
                send_sem=gssem.at[self.number + k - 1], recv_sem=grsem.at[self.number + k - 1],
                device_id=self.at(q), device_id_type=MESH)

        def start(self):
            for k in (2, 1, 3):
                self.copy(k).start()

        def finish(self):
            at = self.piece(self.me)
            total = M[at]
            for k in (1, 3, 2):
                self.copy(k).wait_recv()
                total = total + self.buf(k - 1)[...]
            M[at] = total

        def wait_send(self):
            for k in range(1, 4):
                self.copy(k).wait_send()

    rings = []
    full = slice(None)
    for stage in range(3):
        k0, n = START[stage], START[stage + 1] - START[stage]
        na = HALF[stage]
        nb = n - na
        kb = k0 + na

        def ax_piece(q, h, k0=k0, na=na):
            return (pl.ds(base + k0, na), h, q)

        def by_piece(q, h, kb=kb, nb=nb):
            return (pl.ds(base + kb, nb), lax.rem(q, 2), pl.ds(2 * h, 2), q // 2)

        def ax_whole(q, k0=k0, na=na):
            return (pl.ds(base + k0, na), full, q)

        def by_whole(q, kb=kb, nb=nb):
            return (pl.ds(base + kb, nb), lax.rem(q, 2), full, q // 2)

        def ay_piece(q, k0=k0, na=na):
            return (pl.ds(base + k0, na), lax.rem(q, 2), xi, q // 2)

        def bx_piece(q, kb=kb, nb=nb):
            return (pl.ds(base + kb, nb), ylo, q, yhi)

        def wide_first(k, n):
            return lambda h: F1.at[h, pl.ds(k, n)]

        def wide_second(k, n):
            return lambda w, h: F2.at[w, h, pl.ds(k, n)]

        def thin(k, n):
            return lambda i: G2.at[i, pl.ds(k, n)]

        number = stage * 24
        if stage < 2:
            wide = (Ring(xi, at_x, ax_piece, wide_first(k0, na), wide_second(k0, na), number),
                    Ring(y, at_y, by_piece, wide_first(kb, nb), wide_second(kb, nb), number + 6))
        else:
            wide = (Direct(xi, at_x, ax_whole, lambda i: FX.at[i], number),
                    Direct(y, at_y, by_whole, lambda i: FY.at[i], number + 6))
        rings.append(wide + (
            Direct(y, at_y, ay_piece, thin(k0, na), number + 12),
            Direct(xi, at_x, bx_piece, thin(kb, nb), number + 18),
        ))

    def arrive(*offsets):
        for o in offsets:
            main_copy(o).wait_recv()
            x_copy(o).start()

    def overlap_part(stage):
        first, last_ = STAGES[stage]
        for o in ((0,) if stage == 0 else ()) + tuple(range(max(1, 2 * first - 1), 2 * last_ - 1)):
            coef_copy(o).wait_recv()
        lax.fori_loop(first, last_, assemble_psi, 0)
        products(stage, 1)

        @pl.when(c == 0)
        def _():
            pair_copy(stage).start()

    def energy_part(stage):
        first, last_ = STAGES[stage]
        for o in ((NB - 1, 0) if stage == 0 else ()) + tuple(range(max(1, 2 * first - 1), 2 * last_ - 1)):
            x_copy(o).wait_recv()
        lax.fori_loop(first, last_, assemble_h, 0)
        products(stage, 0)
        evens(stage)

        @pl.when(c == 1)
        def _():
            pair_copy(stage).start()

    def wide_start(stage):
        add_pair(stage)
        rings[stage][0].start()
        rings[stage][1].start()

    def wide_relay(stage):
        rings[stage][0].relay()
        rings[stage][1].relay()

    def wide_finish(stage):
        rings[stage][0].finish()
        rings[stage][2].start()
        rings[stage][1].finish()
        rings[stage][3].start()

    def thin_finish(stage):
        rings[stage][2].finish()
        rings[stage][3].finish()
        z_send(stage)

    Z_PARTS = (
        [(i, 0, 5) for i in range(5)],
        [(i, 5, 2) for i in range(5)] + [(5, 0, 7), (6, 0, 7)],
        [(7, 0, 8)] + [(i, 7, 1) for i in range(6, -1, -1)],
    )

    def z_copy(stage, i, j, n):
        return pltpu.make_async_remote_copy(
            src_ref=ZS.at[i, pl.ds(j, n)], dst_ref=ZR.at[i - 1, pl.ds(j, n)],
            send_sem=zssem.at[stage * 7 + i - 1], recv_sem=zrsem.at[stage * 7 + i - 1],
            device_id={"band": ylo * 8 + lax.rem(z + DZ[i], 8)}, device_id_type=MESH)

    def z_send(stage):
        for i, j, n in Z_PARTS[stage]:
            for t in range(j, j + n):
                ZS[i, t] = M[base + block_of(i, t), ylo, xi, yhi]
            if i > 0:
                z_copy(stage, i, j, n).start()

    def z_add(stage):
        for i, j, n in sorted(Z_PARTS[stage]):
            if i > 0:
                z_copy(stage, i, j, n).wait_recv()
                for t in range(j, j + n):
                    at = lax.rem(z + 8 - DZ[i] + DZ[t], 8)
                    TOT[at] = TOT[at] + ZR[i - 1, t]

    arrive(0, 1, 2, 3, 4, 5, 7)
    for o in (9, 11, 14):
        main_copy(o).start()
    arrive(6, 8)
    overlap_part(0)
    main_copy(13).start()
    energy_part(0)
    wide_start(0)
    wide_relay(0)
    arrive(9, 11, 10, 12)
    overlap_part(1)
    wide_finish(0)
    energy_part(1)
    arrive(13, 14)
    wide_start(1)
    thin_finish(0)
    overlap_part(2)
    wide_relay(1)
    energy_part(2)
    wide_finish(1)
    wide_start(2)
    thin_finish(1)
    wide_finish(2)
    thin_finish(2)
    for t in range(8):
        TOT[lax.rem(z + DZ[t], 8)] = ZS[0, t]
    for stage in range(3):
        z_add(stage)

    rows = pl.ds(pl.multiple_of(xi * 16 + yhi * 8, 8), 8)
    for j in range(4):
        lo, hi = merge(TOT[2 * j], TOT[2 * j + 1], low8)
        fin[c, rows, j * 128:(j + 1) * 128] = lo
        fin[c, rows, 512 + j * 128:512 + (j + 1) * 128] = hi

    def gather_copy(k):
        px, ph = lax.rem(xi + k // 2, 4), lax.rem(yhi + k, 2)
        return pltpu.make_async_remote_copy(
            src_ref=fin.at[c, rows], dst_ref=fin.at[c, rows],
            send_sem=fssem.at[k - 1], recv_sem=frsem.at[k - 1],
            device_id={"dom": px * 4 + ph * 2 + c}, device_id_type=MESH)

    def swap_copy(k):
        px, ph = lax.rem(xi - k // 2 + 4, 4), lax.rem(yhi + k, 2)
        part = fin.at[c, pl.ds(pl.multiple_of(px * 16 + ph * 8, 8), 8)]
        return pltpu.make_async_remote_copy(
            src_ref=part, dst_ref=part, send_sem=wssem.at[k], recv_sem=wrsem.at[k],
            device_id={"dom": other}, device_id_type=MESH)

    for k in (5, 4, 7, 6, 3, 2, 1):
        gather_copy(k).start()
    swap_copy(0).start()
    for k in range(1, 8):
        gather_copy(k).wait_recv()
        swap_copy(k).start()
    for k in range(8):
        swap_copy(k).wait_recv()

    for stage in range(3):
        pair_copy(stage).wait_send()
        for ring in rings[stage]:
            ring.wait_send()
        for i, j, n in Z_PARTS[stage]:
            if i > 0:
                z_copy(stage, i, j, n).wait_send()
    for k in range(1, 8):
        gather_copy(k).wait_send()
    for k in range(8):
        swap_copy(k).wait_send()
    for o in range(NB - 1):
        main_copy(o).wait_send()
        coef_copy(o).wait_send()
    for o in range(NB):
        x_copy(o).wait_send()


def on_device(wavefunctions, potential, projectors, hamiltonian_correction, delta_s, projector_count):
    vm = pl.BlockSpec(memory_space=pltpu.VMEM)
    hbm = pl.BlockSpec(memory_space=pl.ANY)
    dma = pltpu.SemaphoreType.DMA
    both = pl.pallas_call(
        kernel,
        out_shape=jax.ShapeDtypeStruct((2, 64, 1024), F32),
        in_specs=[hbm, vm, hbm, vm, vm, pl.BlockSpec(memory_space=pltpu.SMEM)],
        out_specs=vm,
        scratch_shapes=[
            pltpu.VMEM((4096, 128), F32),
            pltpu.VMEM((4608, 128), F32),
            pltpu.VMEM((2, 4, 128, 128), F32),
            pltpu.VMEM((128, 2, 4, 2, 8, 128), F32),
            pltpu.VMEM((129 * RPZ, 128), F32),
            pltpu.VMEM((NB, CHUNK, 128), F32),
            pltpu.VMEM((NB, CH, 8, 128), F32),
            pltpu.VMEM((NB, 16, 128), F32),
            pltpu.VMEM((NB, 16, 128), F32),
            pltpu.VMEM((CH, 2, RPZ, 128), F32),
            pltpu.VMEM((512, 128), F32),
            pltpu.VMEM((1024, 512), BF16),
            pltpu.VMEM((1024, 512), BF16),
            pltpu.VMEM((512, 2048), BF16),
            pltpu.VMEM((512, 2048), BF16),
            pltpu.VMEM((1024, 128), BF16),
            pltpu.VMEM((128, 2048), BF16),
            pltpu.VMEM((64, 2, 4, 2, 8, 128), F32),
            pltpu.VMEM((2, 64, 2, 8, 128), F32),
            pltpu.VMEM((2, 2, 64, 2, 8, 128), F32),
            pltpu.VMEM((3, 7, 2, 2, 8, 128), F32),
            pltpu.VMEM((3, 8, 4, 8, 128), F32),
            pltpu.VMEM((3, 64, 8, 128), F32),
            pltpu.VMEM((8, 8, 8, 128), F32),
            pltpu.VMEM((7, 8, 8, 128), F32),
            pltpu.VMEM((8, 8, 128), F32),
            dma((2,)),
            dma((NB,)), dma((NB,)), dma((NB,)), dma((NB,)), dma((NB,)), dma((NB,)),
            dma((3,)), dma((3,)), dma((72,)), dma((72,)),
            dma((21,)), dma((21,)), dma((7,)), dma((7,)), dma((8,)), dma((8,)),
        ],
        compiler_params=pltpu.CompilerParams(
            collective_id=0, has_side_effects=True, vmem_limit_bytes=60 * 1024 * 1024),
    )(wavefunctions.reshape(4096, 128), potential.reshape(64, 128), projectors.reshape(72 * 64, 128),
      jnp.swapaxes(hamiltonian_correction, 0, 1), jnp.swapaxes(delta_s, 0, 1), projector_count)
    return both[0], both[1]


def solution(mesh):
    placed = (
        P("band", "dom", None, None),
        P("dom", None, None),
        P("dom", None, None, None, None),
        P("dom", None, None),
        P("dom", None, None),
        P("dom"),
    )
    return jax.shard_map(
        on_device, mesh=mesh, in_specs=placed,
        out_specs=(P("band", None), P("band", None)), check_vma=False)
```

```python
import jax
import jax.numpy as jnp
from jax import lax
from jax.experimental import pallas as pl
from jax.experimental.pallas import tpu as pltpu
from jax.sharding import PartitionSpec as P

MESH = pl.DeviceIdType.MESH
F32 = jnp.float32
BF16 = jnp.bfloat16
NB = 16
ND = 16
CH = 8
RPZ = 32
CHUNK = (CH + 1) * RPZ
VOLUME = 1.0 / 131072.0
DZ = (0, 1, 7, 2, 6, 3, 5, 4)
OFFSETS = [(1, 0)] + [(dy, (8 - DZ[p]) % 8) for p in range(1, 8) for dy in (0, 1)]
STAGES = ((0, 5), (5, 7), (7, 8))
START = (0, 25, 49, 64)
HALF = (12, 12, 7)


def block_of(row, col):
    top = max(row, col)
    if top < 5:
        return col * 5 + row
    if top < 7:
        return 25 + col * 2 + row - 5 if col < 5 else 35 + (col - 5) * 7 + row
    return 49 + col if col < 7 else 56 + row


def split(x):
    hi = x.astype(BF16)
    return hi, (x - hi.astype(F32)).astype(BF16)


def dot(a, b):
    return lax.dot_general(a, b, (((1,), (0,)), ((), ())), preferred_element_type=F32)


def dot_exact(a, b):
    return lax.dot_general(a, b, (((1,), (0,)), ((), ())), precision=lax.Precision.HIGHEST,
                           preferred_element_type=F32)


def dot_nt(a, b):
    return lax.dot_general(a, b, (((1,), (1,)), ((), ())), preferred_element_type=F32)


def kernel(psi_in, pot, proj_in, hcor, dels, count, fin,
           psi, proj, SP, M, T, R, RX, CS, CR, VB, AF, AThi, ATlo, Bhi, Blo, ATC, BC, PB,
           F1, F2, FX, FY, G2, ZS, ZR, TOT,
           lsem, ssem, rsem, cssem, crsem, xssem, xrsem, pssem, prsem, gssem, grsem,
           zssem, zrsem, fssem, frsem, wssem, wrsem):
    g = lax.axis_index("band")
    d = lax.axis_index("dom")
    ylo, z = g // 8, lax.rem(g, 8)
    xi, yhi, c = d // 4, lax.rem(d // 2, 2), lax.rem(d, 2)
    y = yhi * 2 + ylo
    dprev = lax.rem(d + ND - 1, ND)
    other = d + 1 - 2 * c

    def peer(o):
        dy, dz = OFFSETS[o]
        return lax.rem(ylo + dy, 2) * 8 + lax.rem(z + dz, 8)

    def source(o):
        dy, dz = OFFSETS[o]
        return lax.rem(ylo + dy, 2) * 8 + lax.rem(z - dz + 8, 8)

    def at_y(q):
        return {"band": lax.rem(q, 2) * 8 + z, "dom": xi * 4 + (q // 2) * 2 + c}

    def at_x(q):
        return {"dom": q * 4 + yhi * 2 + c}

    load_psi = pltpu.make_async_copy(psi_in, psi, lsem.at[0])
    load_proj = pltpu.make_async_copy(proj_in, proj, lsem.at[1])
    load_psi.start()
    load_proj.start()

    barrier = pltpu.get_barrier_semaphore()
    for o in range(NB - 1):
        pl.semaphore_signal(barrier, inc=1, device_id={"band": peer(o)}, device_id_type=MESH)
    for k in range(1, ND):
        pl.semaphore_signal(barrier, inc=1, device_id={"dom": lax.rem(d + k, ND)}, device_id_type=MESH)
    pl.semaphore_signal(barrier, inc=1, device_id={"band": (1 - ylo) * 8 + z, "dom": xi * 4 + (1 - yhi) * 2 + c},
                        device_id_type=MESH)

    load_psi.wait()
    for r in range(RPZ):
        xy = (r // 8) * 16 + r % 8
        a = psi[pl.ds(xy, 64, stride=64), :]
        b = psi[pl.ds(xy + 8, 64, stride=64), :]
        T[pl.ds(r, 128, stride=RPZ), :] = jnp.concatenate([a, b], axis=0).T
    T[pl.ds(128 * RPZ, RPZ), :] = T[pl.ds(0, RPZ), :]

    pl.semaphore_wait(barrier, 31)

    def main_copy(o):
        p = peer(o)
        return pltpu.make_async_remote_copy(
            src_ref=T.at[pl.ds(pl.multiple_of(p * (CH * RPZ), CH * RPZ), CHUNK)],
            dst_ref=R.at[g],
            send_sem=ssem.at[o], recv_sem=rsem.at[o],
            device_id={"band": p}, device_id_type=MESH)

    def coef_copy(o):
        p = peer(o)
        return pltpu.make_async_remote_copy(
            src_ref=CS.at[p], dst_ref=CR.at[g],
            send_sem=cssem.at[o], recv_sem=crsem.at[o],
            device_id={"band": p}, device_id_type=MESH)

    def x_copy(o):
        s = source(o) if o < NB - 1 else g
        return pltpu.make_async_remote_copy(
            src_ref=R.at[s].reshape(CH + 1, RPZ, 128).at[pl.ds(0, CH), pl.ds(0, 8)],
            dst_ref=RX.at[s],
            send_sem=xssem.at[o], recv_sem=xrsem.at[o],
            device_id={"dom": dprev}, device_id_type=MESH)

    for o in range(9):
        main_copy(o).start()

    R[g] = T[pl.ds(pl.multiple_of(g * (CH * RPZ), CH * RPZ), CHUNK), :]

    load_proj.wait()
    def project(t, acc):
        for x in range(4):
            xy = x * 16 + t
            p = jnp.concatenate([psi[pl.ds(xy, 64, stride=64), :], psi[pl.ds(xy + 8, 64, stride=64), :]], axis=1)
            q = jnp.concatenate([proj[pl.ds(xy, 72, stride=64), :], proj[pl.ds(xy + 8, 72, stride=64), :]], axis=1)
            phi, plo = split(p)
            qhi, qlo = split(q)
            acc = acc + dot_nt(qhi, phi) + dot_nt(qhi, plo) + dot_nt(qlo, phi)
        return acc

    acc = lax.fori_loop(0, 8, project, jnp.zeros((72, 64), F32))
    craw = jnp.concatenate([acc, jnp.zeros((56, 64), F32)], axis=0)
    x_copy(NB - 1).start()

    line = lax.broadcasted_iota(jnp.int32, (256, 128), 0)
    slot = lax.broadcasted_iota(jnp.int32, (256, 128), 1)
    spot = (line >> 4) * 5 + (line & 15)
    ext = jnp.where((line & 15) < 5, jnp.where(slot == spot, 1.0, 0.0), 0.0)
    srow = lax.broadcasted_iota(jnp.int32, (128, 128), 0)
    scol = lax.broadcasted_iota(jnp.int32, (128, 128), 1)
    SP[...] = jnp.zeros_like(SP)
    for t, ref in ((1, hcor), (2, dels)):
        inside = jnp.where((line & 15) >= 5 * t, jnp.where((line & 15) < 5 * t + 5, 1.0, 0.0), 0.0)

        for a in range(4):
            SP[t - 1, a, 0:18, 0:18] = ref[:, a, :]

        def couple(a, ext):
            s = SP[t - 1, a]
            s = (0.5 / VOLUME) * (s + s.T)
            used_col = jnp.clip(count[a] - slot, 0, 1).astype(F32)
            used_row = jnp.clip(count[a] - srow, 0, 1).astype(F32)
            left = jnp.where(spot - 5 * t == a * 18 + slot, used_col, 0.0) * inside
            right = jnp.where(scol == a * 18 + srow, used_row, 0.0)
            return ext + dot_exact(dot_exact(left, s), right)

        ext = lax.fori_loop(0, 4, couple, ext)
    chi, clo = split(craw)
    ehi, elo = split(ext)
    msg = dot(ehi, chi) + dot(ehi, clo) + dot(elo, chi)
    msg = jnp.concatenate([msg, msg], axis=1)
    CS[...] = msg.reshape(NB, 16, 128)
    CR[g] = CS[g]
    for o in range(NB - 1):
        coef_copy(o).start()
    for o in (10, 12):
        main_copy(o).start()

    v = 3.0 + pltpu.roll(pot[...], lax.rem(128 - g * CH, 128), 1)
    for zi in range(CH):
        wide = jnp.broadcast_to(v[:, zi:zi + 1], (64, 128))
        for half in range(2):
            for x in range(4):
                VB[zi, half, x * 8:(x + 1) * 8, :] = wide[x * 16 + half * 8:x * 16 + half * 8 + 8]

    low = lax.broadcasted_iota(jnp.int32, (RPZ, 128), 1) < 64
    low8 = lax.broadcasted_iota(jnp.int32, (8, 128), 1) < 64
    low16 = lax.broadcasted_iota(jnp.int32, (16, 128), 1) < 64
    last = lax.broadcasted_iota(jnp.int32, (8, 128), 0) == 7
    keep = lax.broadcasted_iota(jnp.int32, (16, 128), 0) < 5

    def merge(a, b, mask):
        return jnp.where(mask, a, pltpu.roll(b, 64, 1)), jnp.where(mask, pltpu.roll(a, 64, 1), b)

    def place(m):
        odd = lax.rem(m, 2)
        dz = odd * ((m + 1) // 2) + (1 - odd) * (8 - m // 2)
        s0 = lax.rem(z + dz, 8)
        at = pl.multiple_of(m * 128, 128)
        return s0, s0 + 8, pl.ds(at, 128), pl.ds(pl.multiple_of(1024 + m * 128, 128), 128)

    def column(s0, s1, zi):
        rows = pl.ds(zi * RPZ, RPZ)
        return merge(R[s0, rows, :], R[s1, rows, :], low)

    def assemble_psi(m, _):
        s0, s1, cols, cols2 = place(m)
        for zi in range(CH):
            now = column(s0, s1, zi)
            for half in range(2):
                rows = pl.ds(half * 256 + zi * RPZ, RPZ)
                AF[rows, :] = now[half]
                hi, lo = split(now[half])
                Bhi[rows, cols2] = hi
                Blo[rows, cols2] = lo
        hi, lo = split(AF[...].T)
        AThi[cols, :] = hi
        ATlo[cols, :] = lo
        cc, _ = merge(CR[s0], CR[s1], low16)
        chi, clo = split(cc)
        chi, clo = chi.astype(F32), clo.astype(F32)
        zero = jnp.zeros((16, 128), F32)
        pad = jnp.zeros((80, 128), F32)
        ahi = jnp.where(keep, chi, zero)
        alo = jnp.where(keep, clo, zero)
        ATC[cols, :] = jnp.concatenate([ahi, ahi, alo, pad], axis=0).T.astype(BF16)
        for t, at in ((1, cols), (2, cols2)):
            bhi = jnp.where(keep, pltpu.roll(chi, 16 - 5 * t, 0), zero)
            blo = jnp.where(keep, pltpu.roll(clo, 16 - 5 * t, 0), zero)
            BC[:, at] = jnp.concatenate([bhi, blo, bhi, pad], axis=0).astype(BF16)
        return 0

    def assemble_h(m, _):
        s0, s1, cols, _ = place(m)
        now = column(s0, s1, 0)
        for zi in range(CH):
            nxt = column(s0, s1, zi + 1)
            halo = merge(RX[s0, zi], RX[s1, zi], low8)
            turned = []
            for half in range(2):
                turned.append([pltpu.roll(now[half][x * 8:(x + 1) * 8], 7, 0) for x in range(4)])
            for half in range(2):
                a = now[half]
                ax = jnp.concatenate([a[8:], halo[half]], axis=0)
                ay = jnp.concatenate(
                    [jnp.where(last, turned[1 - half][x], turned[half][x]) for x in range(4)], axis=0)
                h = VB[zi, half] * a - ax - ay - nxt[half]
                rows = pl.ds(half * 256 + zi * RPZ, RPZ)
                hi, lo = split(h)
                Bhi[rows, cols] = hi
                Blo[rows, cols] = lo
            now = nxt
        return 0

    def product(mat, row, n, col, m, at, down, right):
        rows = pl.ds(pl.multiple_of(row * 128, 128), n * 128)
        cols = pl.ds(pl.multiple_of(mat * 1024 + col * 128, 128), m * 128)
        a = AThi[rows, :]
        res = dot(a, Bhi[:, cols]) + dot(a, Blo[:, cols]) + dot(ATlo[rows, :], Bhi[:, cols]) \
            + dot(ATC[rows, :], BC[:, cols])
        res = res * VOLUME
        for r in range(n):
            for k in range(m):
                M[mat * 64 + at + r * down + k * right] = \
                    res[r * 128:(r + 1) * 128, k * 128:(k + 1) * 128].reshape(2, 4, 2, 8, 128)

    def loop(count_, body):
        def step(t, _):
            body(t)
            return 0
        lax.fori_loop(0, count_, step, 0)

    def even(k, l):
        s = 0.5 * (M[k].reshape(128, 128) + M[l].reshape(128, 128).T)
        M[k] = s.reshape(2, 4, 2, 8, 128)
        M[l] = s.T.reshape(2, 4, 2, 8, 128)

    def products(stage, mat):
        if stage == 0:
            loop(4, lambda t: product(mat, (t // 2) * 2, 2, lax.rem(t, 2) * 2, 2,
                                      lax.rem(t, 2) * 10 + (t // 2) * 2, 1, 5))
            loop(2, lambda t: product(mat, 4, 1, 2 * t, 2, 10 * t + 4, 1, 5))
            loop(2, lambda t: product(mat, 2 * t, 2, 4, 1, 20 + 2 * t, 1, 5))
            product(mat, 4, 1, 4, 1, 24, 1, 5)
        elif stage == 1:
            loop(3, lambda t: product(mat, 2 * t, 2, 5, 2, 35 + 2 * t, 1, 7))
            product(mat, 6, 1, 5, 2, 41, 1, 7)
            loop(2, lambda t: product(mat, 5, 2, 2 * t, 2, 25 + 4 * t, 1, 2))
            product(mat, 5, 2, 4, 1, 33, 1, 2)
        else:
            loop(4, lambda t: product(mat, 2 * t, 2, 7, 1, 56 + 2 * t, 1, 1))
            loop(3, lambda t: product(mat, 7, 1, 2 * t, 2, 49 + 2 * t, 1, 1))
            product(mat, 7, 1, 6, 1, 55, 1, 1)

    def evens(stage):
        if stage == 0:
            def pair(t):
                i, j = t // 5, lax.rem(t, 5)

                @pl.when(i <= j)
                def _():
                    even(j * 5 + i, i * 5 + j)
            loop(25, pair)
        elif stage == 1:
            loop(10, lambda t: even(35 + (t // 5) * 7 + lax.rem(t, 5), 25 + lax.rem(t, 5) * 2 + t // 5))
            for i, j in ((5, 5), (5, 6), (6, 6)):
                even(block_of(i, j), block_of(j, i))
        else:
            loop(7, lambda t: even(56 + t, 49 + t))
            even(63, 63)

    def pair_copy(stage):
        k0, n = START[stage], START[stage + 1] - START[stage]
        return pltpu.make_async_remote_copy(
            src_ref=M.at[pl.ds((1 - c) * 64 + k0, n)], dst_ref=PB.at[pl.ds(k0, n)],
            send_sem=pssem.at[stage], recv_sem=prsem.at[stage],
            device_id={"dom": other}, device_id_type=MESH)

    base = c * 64

    def add_pair(stage):
        pair_copy(stage).wait_recv()

        def body(t):
            M[base + START[stage] + t] = M[base + START[stage] + t] + PB[START[stage] + t]
        loop(START[stage + 1] - START[stage], body)

    class Ring:
        def __init__(self, me, at, piece, first, second, number):
            self.me, self.piece, self.first, self.second = me, piece, first, second
            self.plus, self.minus = at(lax.rem(me + 1, 4)), at(lax.rem(me + 3, 4))
            self.number = number

        def copy(self, k):
            me = self.me
            q, h, buf, way = (
                (me + 2, 0, self.first(0), self.plus),
                (me + 2, 1, self.first(1), self.minus),
                (me + 1, 1, self.second(0, 1), self.plus),
                (me + 3, 0, self.second(1, 0), self.minus),
                (me + 1, 0, self.second(0, 0), self.plus),
                (me + 3, 1, self.second(1, 1), self.minus),
            )[k]
            return pltpu.make_async_remote_copy(
                src_ref=M.at[self.piece(lax.rem(q, 4), h)], dst_ref=buf,
                send_sem=gssem.at[self.number + k], recv_sem=grsem.at[self.number + k],
                device_id=way, device_id_type=MESH)

        def start(self):
            for k in range(4):
                self.copy(k).start()

        def add(self, q, h, *bufs):
            at = self.piece(lax.rem(q, 4), h)
            total = M[at]
            for b in bufs:
                total = total + b[...]
            M[at] = total

        def relay(self):
            self.copy(0).wait_recv()
            self.add(self.me + 1, 0, self.first(0))
            self.copy(4).start()
            self.copy(1).wait_recv()
            self.add(self.me + 3, 1, self.first(1))
            self.copy(5).start()

        def finish(self):
            for k in range(2, 6):
                self.copy(k).wait_recv()
            for h in range(2):
                self.add(self.me, h, self.second(0, h), self.second(1, h))

        def wait_send(self):
            for k in range(6):
                self.copy(k).wait_send()

    class Direct:
        def __init__(self, me, at, piece, buf, number):
            self.me, self.at, self.piece, self.buf, self.number = me, at, piece, buf, number

        def copy(self, k):
            q = lax.rem(self.me + k, 4)
            return pltpu.make_async_remote_copy(
                src_ref=M.at[self.piece(q)], dst_ref=self.buf(k - 1),
                send_sem=gssem.at[self.number + k - 1], recv_sem=grsem.at[self.number + k - 1],
                device_id=self.at(q), device_id_type=MESH)

        def start(self):
            for k in (2, 1, 3):
                self.copy(k).start()

        def finish(self):
            at = self.piece(self.me)
            total = M[at]
            for k in (1, 3, 2):
                self.copy(k).wait_recv()
                total = total + self.buf(k - 1)[...]
            M[at] = total

        def wait_send(self):
            for k in range(1, 4):
                self.copy(k).wait_send()

    rings = []
    full = slice(None)
    for stage in range(3):
        k0, n = START[stage], START[stage + 1] - START[stage]
        na = HALF[stage]
        nb = n - na
        kb = k0 + na

        def ax_piece(q, h, k0=k0, na=na):
            return (pl.ds(base + k0, na), h, q)

        def by_piece(q, h, kb=kb, nb=nb):
            return (pl.ds(base + kb, nb), lax.rem(q, 2), pl.ds(2 * h, 2), q // 2)

        def ax_whole(q, k0=k0, na=na):
            return (pl.ds(base + k0, na), full, q)

        def by_whole(q, kb=kb, nb=nb):
            return (pl.ds(base + kb, nb), lax.rem(q, 2), full, q // 2)

        def ay_piece(q, k0=k0, na=na):
            return (pl.ds(base + k0, na), lax.rem(q, 2), xi, q // 2)

        def bx_piece(q, kb=kb, nb=nb):
            return (pl.ds(base + kb, nb), ylo, q, yhi)

        def wide_first(k, n):
            return lambda h: F1.at[h, pl.ds(k, n)]

        def wide_second(k, n):
            return lambda w, h: F2.at[w, h, pl.ds(k, n)]

        def thin(k, n):
            return lambda i: G2.at[i, pl.ds(k, n)]

        number = stage * 24
        if stage < 2:
            wide = (Ring(xi, at_x, ax_piece, wide_first(k0, na), wide_second(k0, na), number),
                    Ring(y, at_y, by_piece, wide_first(kb, nb), wide_second(kb, nb), number + 6))
        else:
            wide = (Direct(xi, at_x, ax_whole, lambda i: FX.at[i], number),
                    Direct(y, at_y, by_whole, lambda i: FY.at[i], number + 6))
        rings.append(wide + (
            Direct(y, at_y, ay_piece, thin(k0, na), number + 12),
            Direct(xi, at_x, bx_piece, thin(kb, nb), number + 18),
        ))

    def arrive(*offsets):
        for o in offsets:
            main_copy(o).wait_recv()
            x_copy(o).start()

    def overlap_part(stage):
        first, last_ = STAGES[stage]
        for o in ((0,) if stage == 0 else ()) + tuple(range(max(1, 2 * first - 1), 2 * last_ - 1)):
            coef_copy(o).wait_recv()
        lax.fori_loop(first, last_, assemble_psi, 0)
        products(stage, 1)

        @pl.when(c == 0)
        def _():
            pair_copy(stage).start()

    def energy_part(stage):
        first, last_ = STAGES[stage]
        for o in ((NB - 1, 0) if stage == 0 else ()) + tuple(range(max(1, 2 * first - 1), 2 * last_ - 1)):
            x_copy(o).wait_recv()
        lax.fori_loop(first, last_, assemble_h, 0)
        products(stage, 0)
        evens(stage)

        @pl.when(c == 1)
        def _():
            pair_copy(stage).start()

    def wide_start(stage):
        add_pair(stage)
        rings[stage][0].start()
        rings[stage][1].start()

    def wide_relay(stage):
        rings[stage][0].relay()
        rings[stage][1].relay()

    def wide_finish(stage):
        rings[stage][0].finish()
        rings[stage][2].start()
        rings[stage][1].finish()
        rings[stage][3].start()

    def thin_finish(stage):
        rings[stage][2].finish()
        rings[stage][3].finish()
        z_send(stage)

    Z_PARTS = (
        [(i, 0, 5) for i in range(5)],
        [(i, 5, 2) for i in range(5)] + [(5, 0, 7), (6, 0, 7)],
        [(7, 0, 8)] + [(i, 7, 1) for i in range(6, -1, -1)],
    )

    def z_copy(stage, i, j, n):
        return pltpu.make_async_remote_copy(
            src_ref=ZS.at[i, pl.ds(j, n)], dst_ref=ZR.at[i - 1, pl.ds(j, n)],
            send_sem=zssem.at[stage * 7 + i - 1], recv_sem=zrsem.at[stage * 7 + i - 1],
            device_id={"band": ylo * 8 + lax.rem(z + DZ[i], 8)}, device_id_type=MESH)

    def z_send(stage):
        for i, j, n in Z_PARTS[stage]:
            for t in range(j, j + n):
                ZS[i, t] = M[base + block_of(i, t), ylo, xi, yhi]
            if i > 0:
                z_copy(stage, i, j, n).start()

    def z_add(stage):
        for i, j, n in sorted(Z_PARTS[stage]):
            if i > 0:
                z_copy(stage, i, j, n).wait_recv()
                for t in range(j, j + n):
                    at = lax.rem(z + 8 - DZ[i] + DZ[t], 8)
                    TOT[at] = TOT[at] + ZR[i - 1, t]

    arrive(0, 1, 2, 3, 4, 5, 7)
    for o in (9, 11, 14):
        main_copy(o).start()
    arrive(6, 8)
    overlap_part(0)
    main_copy(13).start()
    energy_part(0)
    wide_start(0)
    wide_relay(0)
    arrive(9, 11, 10, 12)
    overlap_part(1)
    wide_finish(0)
    energy_part(1)
    arrive(13, 14)
    wide_start(1)
    thin_finish(0)
    overlap_part(2)
    energy_part(2)
    wide_start(2)
    wide_relay(1)
    wide_finish(1)
    wide_finish(2)
    thin_finish(1)
    thin_finish(2)
    for t in range(8):
        TOT[lax.rem(z + DZ[t], 8)] = ZS[0, t]
    for stage in range(3):
        z_add(stage)

    rows = pl.ds(pl.multiple_of(xi * 16 + yhi * 8, 8), 8)
    for j in range(4):
        lo, hi = merge(TOT[2 * j], TOT[2 * j + 1], low8)
        fin[c, rows, j * 128:(j + 1) * 128] = lo
        fin[c, rows, 512 + j * 128:512 + (j + 1) * 128] = hi

    def gather_copy(k):
        px, ph = lax.rem(xi + k // 2, 4), lax.rem(yhi + k, 2)
        return pltpu.make_async_remote_copy(
            src_ref=fin.at[c, rows], dst_ref=fin.at[c, rows],
            send_sem=fssem.at[k - 1], recv_sem=frsem.at[k - 1],
            device_id={"dom": px * 4 + ph * 2 + c}, device_id_type=MESH)

    def swap_copy(k):
        px, ph = lax.rem(xi - k // 2 + 4, 4), lax.rem(yhi + k, 2)
        part = fin.at[c, pl.ds(pl.multiple_of(px * 16 + ph * 8, 8), 8)]
        return pltpu.make_async_remote_copy(
            src_ref=part, dst_ref=part, send_sem=wssem.at[k], recv_sem=wrsem.at[k],
            device_id={"dom": other}, device_id_type=MESH)

    for k in (5, 4, 7, 6, 3, 2, 1):
        gather_copy(k).start()
    swap_copy(0).start()
    for k in range(1, 8):
        gather_copy(k).wait_recv()
        swap_copy(k).start()
    for k in range(8):
        swap_copy(k).wait_recv()

    for stage in range(3):
        pair_copy(stage).wait_send()
        for ring in rings[stage]:
            ring.wait_send()
        for i, j, n in Z_PARTS[stage]:
            if i > 0:
                z_copy(stage, i, j, n).wait_send()
    for k in range(1, 8):
        gather_copy(k).wait_send()
    for k in range(8):
        swap_copy(k).wait_send()
    for o in range(NB - 1):
        main_copy(o).wait_send()
        coef_copy(o).wait_send()
    for o in range(NB):
        x_copy(o).wait_send()


def on_device(wavefunctions, potential, projectors, hamiltonian_correction, delta_s, projector_count):
    vm = pl.BlockSpec(memory_space=pltpu.VMEM)
    hbm = pl.BlockSpec(memory_space=pl.ANY)
    dma = pltpu.SemaphoreType.DMA
    both = pl.pallas_call(
        kernel,
        out_shape=jax.ShapeDtypeStruct((2, 64, 1024), F32),
        in_specs=[hbm, vm, hbm, vm, vm, pl.BlockSpec(memory_space=pltpu.SMEM)],
        out_specs=vm,
        scratch_shapes=[
            pltpu.VMEM((4096, 128), F32),
            pltpu.VMEM((4608, 128), F32),
            pltpu.VMEM((2, 4, 128, 128), F32),
            pltpu.VMEM((128, 2, 4, 2, 8, 128), F32),
            pltpu.VMEM((129 * RPZ, 128), F32),
            pltpu.VMEM((NB, CHUNK, 128), F32),
            pltpu.VMEM((NB, CH, 8, 128), F32),
            pltpu.VMEM((NB, 16, 128), F32),
            pltpu.VMEM((NB, 16, 128), F32),
            pltpu.VMEM((CH, 2, RPZ, 128), F32),
            pltpu.VMEM((512, 128), F32),
            pltpu.VMEM((1024, 512), BF16),
            pltpu.VMEM((1024, 512), BF16),
            pltpu.VMEM((512, 2048), BF16),
            pltpu.VMEM((512, 2048), BF16),
            pltpu.VMEM((1024, 128), BF16),
            pltpu.VMEM((128, 2048), BF16),
            pltpu.VMEM((64, 2, 4, 2, 8, 128), F32),
            pltpu.VMEM((2, 64, 2, 8, 128), F32),
            pltpu.VMEM((2, 2, 64, 2, 8, 128), F32),
            pltpu.VMEM((3, 7, 2, 2, 8, 128), F32),
            pltpu.VMEM((3, 8, 4, 8, 128), F32),
            pltpu.VMEM((3, 64, 8, 128), F32),
            pltpu.VMEM((8, 8, 8, 128), F32),
            pltpu.VMEM((7, 8, 8, 128), F32),
            pltpu.VMEM((8, 8, 128), F32),
            dma((2,)),
            dma((NB,)), dma((NB,)), dma((NB,)), dma((NB,)), dma((NB,)), dma((NB,)),
            dma((3,)), dma((3,)), dma((72,)), dma((72,)),
            dma((21,)), dma((21,)), dma((7,)), dma((7,)), dma((8,)), dma((8,)),
        ],
        compiler_params=pltpu.CompilerParams(
            collective_id=0, has_side_effects=True, vmem_limit_bytes=60 * 1024 * 1024),
    )(wavefunctions.reshape(4096, 128), potential.reshape(64, 128), projectors.reshape(72 * 64, 128),
      jnp.swapaxes(hamiltonian_correction, 0, 1), jnp.swapaxes(delta_s, 0, 1), projector_count)
    return both[0], both[1]


def solution(mesh):
    placed = (
        P("band", "dom", None, None),
        P("dom", None, None),
        P("dom", None, None, None, None),
        P("dom", None, None),
        P("dom", None, None),
        P("dom"),
    )
    return jax.shard_map(
        on_device, mesh=mesh, in_specs=placed,
        out_specs=(P("band", None), P("band", None)), check_vma=False)
```
